128 devices in a mesh: stage: 1, data: 128 (over z, y, x, core).
Axes of the slice: x: 4, y: 4, z: 4, core: 2. Of those that a mesh axis runs over, the one named last changes fastest.
Arguments:
- grad_attn: float32 [128, 1, 1024, 1024], P(('stage', 'data'))
- mom_attn: float32 [1, 1024, 1024], P('stage', 'data')
- master_attn: float32 [1, 1024, 1024], P('stage', 'data')
- grad_up: float32 [128, 1, 1024, 512], P(('stage', 'data'))
- mom_up: float32 [1, 1024, 512], P('stage', 'data')
- master_up: float32 [1, 1024, 512], P('stage', 'data')
- grad_down: float32 [128, 1, 512, 1024], P(('stage', 'data'))
- mom_down: float32 [1, 512, 1024], P('stage', 'data')
- master_down: float32 [1, 512, 1024], P('stage', 'data')
Outputs:
- output 1: float32 [1, 1024, 1024], P('stage', 'data')
- output 2: float32 [1, 1024, 1024], P('stage', 'data')
- output 3: bfloat16 [1, 1024, 1024], P('stage', 'data')
- output 4: float32 [1, 1024, 512], P('stage', 'data')
- output 5: float32 [1, 1024, 512], P('stage', 'data')
- output 6: bfloat16 [1, 1024, 512], P('stage', 'data')
- output 7: float32 [1, 512, 1024], P('stage', 'data')
- output 8: float32 [1, 512, 1024], P('stage', 'data')
- output 9: bfloat16 [1, 512, 1024], P('stage', 'data')
All inputs are finite; a program needn't handle non-finite values.
Results may differ from the reference program's by a relative error of at most 0.00763485.
Values are sent between devices in bfloat16 or wider.
A program may use at most 1 GiB of HBM per device.

```python
import math
import jax
import jax.numpy as jnp
from jax import lax

HIDDEN = 1024
FFN_WIDTH = 512
ATTN_COUNT = 1
EXPERT_COUNT = 1
GROUP_SIZE = 128
NS_STEPS = 5

MOMENTUM = 0.95
LEARN_RATE = 0.25
WEIGHT_DECAY = 0.2
EPSILON = 1e-7
COEF_A = 3.4445
COEF_B = -4.7750
COEF_C = 2.0315
STACK_SHAPES = ((ATTN_COUNT, HIDDEN, HIDDEN), (EXPERT_COUNT, HIDDEN, FFN_WIDTH), (EXPERT_COUNT, FFN_WIDTH, HIDDEN))
STACK_NAMES = ('attn', 'up', 'down')


def draw_grads(key, count, n_rows, n_cols):
    noise = jax.random.normal(key, (GROUP_SIZE, count, n_rows, n_cols), jnp.float32)
    row_owner = jnp.arange(n_rows) // (n_rows // GROUP_SIZE)
    scale = jnp.where(row_owner[None, :] == jnp.arange(GROUP_SIZE)[:, None], 0.8 * GROUP_SIZE, 0.5)
    return noise * scale[:, None, :, None]


def setup_inputs(seed: int = 0, part: int = 0) -> dict:
    base_key = jax.random.fold_in(jax.random.key(seed), part)
    keys = jax.random.split(base_key, 9)
    inputs = {}
    for stack_idx in range(3):
        count, n_rows, n_cols = STACK_SHAPES[stack_idx]
        label = STACK_NAMES[stack_idx]
        inputs['grad_' + label] = draw_grads(keys[3 * stack_idx], count, n_rows, n_cols)
        inputs['mom_' + label] = jax.random.normal(keys[3 * stack_idx + 1], (count, n_rows, n_cols), jnp.float32)
        inputs['master_' + label] = 0.5 * jax.random.normal(keys[3 * stack_idx + 2], (count, n_rows, n_cols), jnp.float32)
    return inputs


def orthogonalize(mom_new):
    n_rows, n_cols = mom_new.shape
    norm = jnp.sqrt(jnp.sum(mom_new * mom_new))
    x_mat = (mom_new / (norm + EPSILON)).astype(jnp.bfloat16)
    if n_rows > n_cols:
        x_mat = x_mat.T
    for _ in range(NS_STEPS):
        gram_mat = jnp.dot(x_mat, x_mat.T, preferred_element_type=jnp.float32).astype(jnp.bfloat16)
        gram_sq = jnp.dot(gram_mat, gram_mat, preferred_element_type=jnp.float32).astype(jnp.bfloat16)
        poly_mat = (COEF_B * gram_mat.astype(jnp.float32) + COEF_C * gram_sq.astype(jnp.float32)).astype(jnp.bfloat16)
        update = jnp.dot(poly_mat, x_mat, preferred_element_type=jnp.float32).astype(jnp.bfloat16)
        x_mat = (COEF_A * x_mat.astype(jnp.float32) + update.astype(jnp.float32)).astype(jnp.bfloat16)
    if n_rows > n_cols:
        x_mat = x_mat.T
    return x_mat


def stack_step(grad_all, mom_old, master_old):
    n_rows, n_cols = mom_old.shape[1], mom_old.shape[2]
    grad_mean = jnp.sum(grad_all, axis=0) / GROUP_SIZE
    mom_new = MOMENTUM * mom_old + grad_mean
    ortho_mat = lax.map(orthogonalize, mom_new)
    scale = 0.2 * math.sqrt(max(n_rows, n_cols))
    master_new = master_old - LEARN_RATE * (scale * ortho_mat.astype(jnp.float32) + WEIGHT_DECAY * master_old)
    return mom_new, master_new, master_new.astype(jnp.bfloat16)


def reference(grad_attn, mom_attn, master_attn, grad_up, mom_up, master_up, grad_down, mom_down, master_down):
    attn_out = stack_step(grad_attn, mom_attn, master_attn)
    up_out = stack_step(grad_up, mom_up, master_up)
    down_out = stack_step(grad_down, mom_down, master_down)
    return (attn_out[0], attn_out[1], attn_out[2], up_out[0], up_out[1], up_out[2], down_out[0], down_out[1], down_out[2])
```

```python
import functools
import math

import jax
import jax.numpy as jnp
from jax import lax
from jax.experimental import pallas as pl
from jax.experimental.pallas import tpu as pltpu
from jax.sharding import PartitionSpec as P

MOMENTUM = 0.95
LEARN_RATE = 0.25
WEIGHT_DECAY = 0.2
EPSILON = 1e-7
COEF_A = 3.4445
COEF_B = -4.7750
COEF_C = 2.0315
NS_STEPS = 5

F32 = jnp.float32
BF16 = jnp.bfloat16

COLS = ((0, 384), (384, 384), (768, 256))
ORDER = ((0, 1, 2), (1, 2, 0), (2, 0, 1))
SIDE = 4
CHIP_ROWS = 16
WIDE = 1024
NARROW = 512
TILE = 256
BLOCK = (SIDE, SIDE, SIDE, CHIP_ROWS, WIDE)
ALL = slice(None)
LO = pl.ds(0, 8)
HI = pl.ds(8, 8)
HALF = (LO, HI)
WEST = pl.ds(0, NARROW)
EAST = pl.ds(NARROW, NARROW)
PIECES = (
    (('up', 0, 384, ALL, 0),),
    (('up', 384, 128, ALL, 384), ('down', 0, TILE, LO, NARROW), ('down', NARROW, TILE, HI, NARROW)),
    (('down', TILE, TILE, LO, 768), ('down', 768, TILE, HI, 768)),
)


def place(ref, fixed, rows, cols):
    return ref.at[region(fixed, rows, cols)]


def region(fixed, rows, cols):
    return tuple(fixed.get(axis, ALL) for axis in range(3)) + (rows, cols)


def coords_of(k):
    return k // (SIDE * SIDE), lax.rem(k // SIDE, SIDE), lax.rem(k, SIDE)


def aligned(start, size):
    return pl.ds(pl.multiple_of(start, size), size)


def kernel(group_size, grad_attn, grad_up, grad_down, mom_attn, mom_up, mom_down, mas_attn, mas_up, mas_down,
           mo_attn, wo_attn, bo_attn, mo_up, wo_up, bo_up, mo_down, wo_down, bo_down,
           own, peer, full, recv0, recv1, recv2, mom_pk, swap_attn, swap_up, swap_down,
           send_attn, send_up, send_down, got_attn, got_up, got_down, x_mat, a_mat, b_mat, turn,
           load_sem, push_sem, pull_sem, rs_send, rs_recv, ag_send, ag_recv, ex_send, ex_recv):
    me = lax.axis_index('data')
    core = lax.rem(me, 2)
    chip = me // 2
    pos = coords_of(chip)
    partner = me + 1 - 2 * core
    recvs = (recv0, recv1, recv2)

    def at_axis(axis, coord):
        coords = list(pos)
        coords[axis] = coord
        return ((coords[0] * SIDE + coords[1]) * SIDE + coords[2]) * 2 + core

    right = [lax.rem(p + 1, SIDE) for p in pos]
    left = [lax.rem(p + 3, SIDE) for p in pos]
    far = [lax.rem(p + 2, SIDE) for p in pos]
    right_dev = [at_axis(a, right[a]) for a in range(3)]
    left_dev = [at_axis(a, left[a]) for a in range(3)]

    def remote(src, dst, send_sem, recv_sem, device):
        return pltpu.make_async_remote_copy(src_ref=src, dst_ref=dst, send_sem=send_sem, recv_sem=recv_sem,
                                            device_id={'data': device}, device_id_type=pl.DeviceIdType.MESH)

    barrier = pltpu.get_barrier_semaphore()
    for device in [partner] + right_dev + left_dev:
        pl.semaphore_signal(barrier, inc=1, device_id={'data': device}, device_id_type=pl.DeviceIdType.MESH)
    pl.semaphore_wait(barrier, 7)

    def turns(color):
        axis = ORDER[color][0]
        return axis, (far[axis], right[axis], left[axis], pos[axis])

    def attn_copy(color, turn_idx, push):
        axis, coords = turns(color)
        cols = pl.ds(*COLS[color])
        src = place(grad_attn, {axis: coords[turn_idx]}, ALL, cols)
        if push:
            dst = place(peer, {axis: coords[turn_idx]}, ALL, cols)
            return remote(src, dst, push_sem.at[color, turn_idx, 0], pull_sem.at[color, turn_idx, 0], partner)
        dst = place(own, {axis: coords[turn_idx]}, ALL, cols)
        return pltpu.make_async_copy(src, dst, load_sem.at[color, turn_idx, 0])

    def expert_copies(color, turn_idx, push):
        axis, coords = turns(color)
        copies = []
        for k, (source, col, width, rows, packed) in enumerate(PIECES[color]):
            src = place(grad_up if source == 'up' else grad_down, {axis: coords[turn_idx]}, ALL, pl.ds(col, width))
            target = peer if push else own
            dst = place(target, {axis: coords[turn_idx]}, rows, pl.ds(packed, width))
            if push:
                copies.append(remote(src, dst, push_sem.at[color, turn_idx, k], pull_sem.at[color, turn_idx, k], partner))
            else:
                copies.append(pltpu.make_async_copy(src, dst, load_sem.at[color, turn_idx, k]))
        return copies

    def mom_copies_from_0():
        return [remote(mom_up, swap_up, ex_send.at[0], ex_recv.at[0], partner),
                remote(mom_down, swap_down, ex_send.at[1], ex_recv.at[1], partner)]

    def mom_copies_from_1():
        return [remote(mom_attn, swap_attn, ex_send.at[0], ex_recv.at[0], partner)]

    @pl.when(core == 0)
    def _():
        for turn_idx in range(SIDE):
            for color in range(3):
                attn_copy(color, turn_idx, False).start()
                for copy in expert_copies(color, turn_idx, True):
                    copy.start()
        for copy in mom_copies_from_0():
            copy.start()

    @pl.when(core == 1)
    def _():
        for turn_idx in range(SIDE):
            for color in range(3):
                for copy in expert_copies(color, turn_idx, False):
                    copy.start()
                attn_copy(color, turn_idx, True).start()
        for copy in mom_copies_from_1():
            copy.start()

    def chip_sum(color, turn_idx):
        @pl.when(core == 0)
        def _():
            attn_copy(color, turn_idx, False).wait()
            attn_copy(color, turn_idx, True).wait_recv()

        @pl.when(core == 1)
        def _():
            for copy in expert_copies(color, turn_idx, False):
                copy.wait()
            for copy in expert_copies(color, turn_idx, True):
                copy.wait_recv()
        axis, coords = turns(color)
        idx = region({axis: coords[turn_idx]}, ALL, pl.ds(*COLS[color]))
        own[idx] = own[idx] + peer[idx]

    def rs_ctx(phase, color):
        order = ORDER[color]
        axis = order[phase]
        fixed = {order[k]: pos[order[k]] for k in range(phase)}
        return axis, fixed, pl.ds(*COLS[color])

    def rs_buf(phase, color, piece):
        col, width = COLS[color]
        lead = (piece,) + (ALL,) * (2 - phase)
        return recvs[phase].at[lead + (ALL, pl.ds(col, width))]

    def rs_copy(phase, color, piece):
        axis, fixed, cols = rs_ctx(phase, color)
        coord, half, device = ((far, 0, right_dev), (far, 1, left_dev), (right, 1, right_dev),
                               (left, 0, left_dev), (right, 0, right_dev), (left, 1, left_dev))[piece]
        src = place(own, {**fixed, axis: coord[axis]}, HALF[half], cols)
        return remote(src, rs_buf(phase, color, piece), rs_send.at[phase, color, piece], rs_recv.at[phase, color, piece],
                      device[axis])

    def rs_add(phase, color, coord, half, pieces):
        axis, fixed, cols = rs_ctx(phase, color)
        idx = region({**fixed, axis: coord[axis]}, HALF[half], cols)
        total = own[idx]
        for piece in pieces:
            col, width = COLS[color]
            lead = (piece,) + (ALL,) * (2 - phase)
            total = total + recvs[phase][lead + (ALL, pl.ds(col, width))]
        own[idx] = total

    def rs_mid(phase, color):
        rs_copy(phase, color, 0).wait_recv()
        rs_add(phase, color, right, 0, (0,))
        rs_copy(phase, color, 4).start()
        rs_copy(phase, color, 1).wait_recv()
        rs_add(phase, color, left, 1, (1,))
        rs_copy(phase, color, 5).start()

    def rs_end(phase, color):
        for piece in (2, 3, 4, 5):
            rs_copy(phase, color, piece).wait_recv()
        rs_add(phase, color, pos, 0, (3, 4))
        rs_add(phase, color, pos, 1, (2, 5))

    for color in range(3):
        chip_sum(color, 0)
        rs_copy(0, color, 0).start()
        rs_copy(0, color, 1).start()
    for color in range(3):
        chip_sum(color, 1)
        rs_copy(0, color, 2).start()
    for color in range(3):
        chip_sum(color, 2)
        rs_copy(0, color, 3).start()
    for color in range(3):
        rs_mid(0, color)
    for color in range(3):
        chip_sum(color, 3)
    for phase in range(3):
        if phase > 0:
            for color in range(3):
                rs_mid(phase, color)
        for color in range(3):
            rs_end(phase, color)
            if phase < 2:
                for piece in range(4):
                    rs_copy(phase + 1, color, piece).start()

    @pl.when(core == 0)
    def _():
        mom_copies_from_1()[0].wait_recv()
        mom_pk[LO] = mom_attn[...]
        mom_pk[HI] = swap_attn[...]

    @pl.when(core == 1)
    def _():
        for copy in mom_copies_from_0():
            copy.wait_recv()
        mom_pk[LO, WEST] = swap_up[...]
        mom_pk[HI, WEST] = mom_up[...]
        for first, cols in ((0, WEST), (8, EAST)):
            mom_pk[pl.ds(first, SIDE), EAST] = swap_down[:, cols]
            mom_pk[pl.ds(first + SIDE, SIDE), EAST] = mom_down[:, cols]

    mine = pos
    mom_new = MOMENTUM * mom_pk[...] + own[mine] * (1.0 / group_size)
    full[mine] = mom_new

    def ag_copy(phase, color, piece):
        order = ORDER[color]
        axis = order[phase]
        fixed = {order[k]: pos[order[k]] for k in range(phase)}
        coord, half, device = ((pos, 0, right_dev), (pos, 1, left_dev), (pos, 1, right_dev), (pos, 0, left_dev),
                               (left, 0, right_dev), (right, 1, left_dev))[piece]
        part = place(full, {**fixed, axis: coord[axis]}, HALF[half], pl.ds(*COLS[color]))
        return remote(part, part, ag_send.at[phase, color, piece], ag_recv.at[phase, color, piece], device[axis])

    def ag_arrive(phase, color, piece):
        order = ORDER[color]
        axis = order[phase]
        fixed = {order[k]: pos[order[k]] for k in range(phase)}
        coord, half = ((left, 0), (right, 1), (left, 1), (right, 0), (far, 0), (far, 1))[piece]
        part = place(full, {**fixed, axis: coord[axis]}, HALF[half], pl.ds(*COLS[color]))
        remote(part, part, ag_send.at[phase, color, piece], ag_recv.at[phase, color, piece], right_dev[axis]).wait_recv()

    for color in range(3):
        for piece in range(4):
            ag_copy(2, color, piece).start()
    for phase in (2, 1, 0):
        for color in range(3):
            ag_arrive(phase, color, 0)
            ag_copy(phase, color, 4).start()
            ag_arrive(phase, color, 1)
            ag_copy(phase, color, 5).start()
        for color in range(3):
            for piece in (2, 3, 4, 5):
                ag_arrive(phase, color, piece)
            if phase > 0:
                for piece in range(4):
                    ag_copy(phase - 1, color, piece).start()

    @pl.when(core == 0)
    def _():
        send_attn[...] = full[mine + (HI, ALL)]
        mo_attn[...] = full[mine + (LO, ALL)]

    @pl.when(core == 1)
    def _():
        send_up[...] = full[mine + (LO, WEST)]
        mo_up[...] = full[mine + (HI, WEST)]
        for rows, cols in ((LO, WEST), (HI, EAST)):
            down = full[mine + (rows, EAST)]
            send_down[:, cols] = down[:SIDE]
            mo_down[:, cols] = down[SIDE:]

    def back_from_0(base, out_attn):
        return [remote(send_attn, out_attn, ex_send.at[base], ex_recv.at[base], partner)]

    def back_from_1(base, out_up, out_down):
        return [remote(send_up, out_up, ex_send.at[base], ex_recv.at[base], partner),
                remote(send_down, out_down, ex_send.at[base + 1], ex_recv.at[base + 1], partner)]

    @pl.when(core == 0)
    def _():
        for copy in back_from_0(2, mo_attn):
            copy.start()

    @pl.when(core == 1)
    def _():
        for copy in back_from_1(2, mo_up, mo_down):
            copy.start()

    def weighted(a_val, q_val):
        return (COEF_B * a_val.astype(F32) + COEF_C * q_val.astype(BF16).astype(F32)).astype(BF16)

    def advance(x_val, y_val):
        return (COEF_A * x_val.astype(F32) + y_val.astype(BF16).astype(F32)).astype(BF16)

    def gram(base, size):
        rows = pl.ds(base, size)

        def body(j, carry):
            off = pl.multiple_of(j * TILE, TILE)
            a_val = lax.dot_general(x_mat[rows, :], x_mat[aligned(base + off, TILE), :], (((1,), (1,)), ((), ())),
                                    preferred_element_type=F32)
            a_mat[rows, pl.ds(off, TILE)] = a_val.astype(BF16)
            return carry
        lax.fori_loop(0, size // TILE, body, 0)

    def poly(base, size):
        rows = pl.ds(base, size)

        def body(j, carry):
            cols = aligned(j * TILE, TILE)
            q_val = jnp.dot(a_mat[rows, 0:size], a_mat[rows, cols], preferred_element_type=F32)
            b_mat[rows, cols] = weighted(a_mat[rows, cols], q_val)
            return carry
        lax.fori_loop(0, size // TILE, body, 0)

    def update(base, size):
        rows = pl.ds(base, size)

        def body(j, carry):
            cols = aligned(j * TILE, TILE)
            y_val = jnp.dot(b_mat[rows, 0:size], x_mat[rows, cols], preferred_element_type=F32)
            x_mat[rows, cols] = advance(x_mat[rows, cols], y_val)
            return carry
        lax.fori_loop(0, 4, body, 0)

    def square_sum(cols):
        def body(k, acc):
            val = full[coords_of(k) + (ALL, cols)]
            return acc + val * val
        acc = lax.fori_loop(0, 64, body, jnp.zeros((16, cols.size), F32))
        return jnp.sum(acc, axis=(0, 1), keepdims=True)

    def inverse(total):
        return 1.0 / (jnp.sqrt(total) + EPSILON)

    @pl.when(core == 0)
    def _():
        scale = inverse(square_sum(pl.ds(0, WIDE)))

        def fill(k, carry):
            val = full[coords_of(k)]
            x_mat[aligned(k * CHIP_ROWS, CHIP_ROWS), :] = (val * scale).astype(BF16)
            return carry
        lax.fori_loop(0, 64, fill, 0)

        def step(_, carry):
            gram(0, WIDE)
            poly(0, WIDE)
            update(0, WIDE)
            return carry
        lax.fori_loop(0, NS_STEPS - 1, step, 0)
        gram(0, WIDE)
        rows = aligned(chip * CHIP_ROWS, CHIP_ROWS)
        a_val = a_mat[rows, :]
        b_val = weighted(a_val, jnp.dot(a_val, a_mat[...], preferred_element_type=F32))
        out = advance(x_mat[rows, :], jnp.dot(b_val, x_mat[...], preferred_element_type=F32)).astype(F32)
        back_from_0(2, mo_attn)[0].wait_send()
        send_attn[...] = out[8:]
        got_attn[...] = out[:8]
        back_from_0(4, got_attn)[0].start()

    @pl.when(core == 1)
    def _():
        scale_up = inverse(square_sum(WEST))
        scale_down = inverse(square_sum(EAST))

        def fill_up(k, carry):
            val = full[k // 2, pl.ds(2 * lax.rem(k, 2), 2), :, :, WEST].reshape(128, NARROW)
            x_mat[WEST, aligned(k * 128, 128)] = jnp.transpose(val * scale_up).astype(BF16)
            return carry
        lax.fori_loop(0, 8, fill_up, 0)

        def fill_down(k, carry):
            z, y, x = coords_of(2 * k)
            val = full[z, y, pl.ds(x, 2), :, EAST] * scale_down
            rows = aligned(NARROW + k * CHIP_ROWS, CHIP_ROWS)
            x_mat[rows, WEST] = val[:, :8].reshape(CHIP_ROWS, NARROW).astype(BF16)
            x_mat[rows, EAST] = val[:, 8:].reshape(CHIP_ROWS, NARROW).astype(BF16)
            return carry
        lax.fori_loop(0, 32, fill_down, 0)

        def matrix(t, carry):
            base = pl.multiple_of(t * NARROW, NARROW)

            def step(_, carry):
                gram(base, NARROW)
                poly(base, NARROW)
                update(base, NARROW)
                return carry
            lax.fori_loop(0, NS_STEPS - 1, step, 0)
            gram(base, NARROW)
            return carry
        lax.fori_loop(0, 2, matrix, 0)
        poly(0, NARROW)
        cols = aligned(chip // 8 * 128, 128)
        out_up = advance(x_mat[WEST, cols], jnp.dot(b_mat[WEST, WEST], x_mat[WEST, cols], preferred_element_type=F32))
        turn[...] = jnp.transpose(out_up.astype(F32))
        rows = aligned(NARROW + chip // 2 * CHIP_ROWS, CHIP_ROWS)
        a_val = a_mat[rows, WEST]
        b_val = weighted(a_val, jnp.dot(a_val, a_mat[EAST, WEST], preferred_element_type=F32))
        both = advance(x_mat[rows, :], jnp.dot(b_val, x_mat[EAST, :], preferred_element_type=F32)).astype(F32)
        out_down = jnp.where(lax.rem(chip, 2) == 0, both[:8], both[8:])
        for copy in back_from_1(2, mo_up, mo_down):
            copy.wait_send()
        first = pl.multiple_of(lax.rem(chip, 8) * CHIP_ROWS, CHIP_ROWS)
        send_up[...] = turn[pl.ds(first, 8), :]
        got_up[...] = turn[pl.ds(first + 8, 8), :]
        send_down[...] = out_down[:SIDE]
        got_down[...] = out_down[SIDE:]
        for copy in back_from_1(4, got_up, got_down):
            copy.start()

    @pl.when(core == 0)
    def _():
        for copy in back_from_1(2, mo_up, mo_down) + back_from_1(4, got_up, got_down):
            copy.wait_recv()

    @pl.when(core == 1)
    def _():
        for copy in back_from_0(2, mo_attn) + back_from_0(4, got_attn):
            copy.wait_recv()

    for mas, got, w_out, b_out in ((mas_attn, got_attn, wo_attn, bo_attn), (mas_up, got_up, wo_up, bo_up),
                                   (mas_down, got_down, wo_down, bo_down)):
        old = mas[...]
        new = old - LEARN_RATE * (0.2 * math.sqrt(WIDE) * got[...] + WEIGHT_DECAY * old)
        w_out[...] = new
        b_out[...] = new.astype(BF16)

    @pl.when(core == 0)
    def _():
        for turn_idx in range(SIDE):
            for color in range(3):
                for copy in expert_copies(color, turn_idx, True):
                    copy.wait_send()
        for copy in mom_copies_from_0() + back_from_0(4, got_attn):
            copy.wait_send()

    @pl.when(core == 1)
    def _():
        for turn_idx in range(SIDE):
            for color in range(3):
                attn_copy(color, turn_idx, True).wait_send()
        for copy in mom_copies_from_1() + back_from_1(4, got_up, got_down):
            copy.wait_send()

    for phase in range(3):
        for color in range(3):
            for piece in range(6):
                rs_copy(phase, color, piece).wait_send()
                ag_copy(phase, color, piece).wait_send()


def solution(mesh):
    group_size = mesh.shape['data']
    grad_spec = P(('stage', 'data'), None, None, None)
    row_spec = P('stage', 'data', None)

    def step_local(grad_attn, mom_attn, mas_attn, grad_up, mom_up, mas_up, grad_down, mom_down, mas_down):
        vmem = pl.BlockSpec(memory_space=pltpu.VMEM)
        hbm = pl.BlockSpec(memory_space=pl.ANY)
        shapes = ((8, WIDE), (8, NARROW), (SIDE, WIDE))
        outs = []
        for shape in shapes:
            outs += [jax.ShapeDtypeStruct(shape, F32), jax.ShapeDtypeStruct(shape, F32), jax.ShapeDtypeStruct(shape, BF16)]
        sem = pltpu.SemaphoreType.DMA
        scratch = [
            *[pltpu.VMEM(BLOCK, F32)] * 3,
            *[pltpu.VMEM((6,) + (SIDE,) * free + (8, WIDE), F32) for free in (2, 1, 0)],
            pltpu.VMEM((CHIP_ROWS, WIDE), F32),
            *[pltpu.VMEM(shape, F32) for shape in shapes * 3],
            *[pltpu.VMEM((WIDE, WIDE), BF16)] * 3,
            pltpu.VMEM((128, NARROW), F32),
            *[sem((3, SIDE, 3))] * 3,
            *[sem((3, 3, 6))] * 4,
            *[sem((6,))] * 2,
        ]
        result = pl.pallas_call(
            functools.partial(kernel, group_size),
            out_shape=outs,
            in_specs=[hbm] * 3 + [vmem] * 6,
            out_specs=[vmem] * 9,
            scratch_shapes=scratch,
            compiler_params=pltpu.CompilerParams(collective_id=0, has_side_effects=True, vmem_limit_bytes=60 * 1024 * 1024),
            name='muon',
        )(grad_attn.reshape(BLOCK), grad_up.reshape(BLOCK[:4] + (NARROW,)), grad_down.reshape(BLOCK[:3] + (8, WIDE)),
          *(v[0] for v in (mom_attn, mom_up, mom_down, mas_attn, mas_up, mas_down)))
        return tuple(r[None] for r in result)

    return jax.shard_map(step_local, mesh=mesh, in_specs=(grad_spec, row_spec, row_spec) * 3, out_specs=(row_spec,) * 9,
                         check_vma=False)
```

```python
import functools
import math

import jax
import jax.numpy as jnp
from jax import lax
from jax.experimental import pallas as pl
from jax.experimental.pallas import tpu as pltpu
from jax.sharding import PartitionSpec as P

MOMENTUM = 0.95
LEARN_RATE = 0.25
WEIGHT_DECAY = 0.2
EPSILON = 1e-7
COEF_A = 3.4445
COEF_B = -4.7750
COEF_C = 2.0315
NS_STEPS = 5

F32 = jnp.float32
BF16 = jnp.bfloat16

COLS = ((0, 384), (384, 384), (768, 256))
ORDER = ((0, 1, 2), (1, 2, 0), (2, 0, 1))
SIDE = 4
CHIP_ROWS = 16
WIDE = 1024
NARROW = 512
TILE = 256
BLOCK = (SIDE, SIDE, SIDE, CHIP_ROWS, WIDE)
ALL = slice(None)
LO = pl.ds(0, 8)
HI = pl.ds(8, 8)
HALF = (LO, HI)
WEST = pl.ds(0, NARROW)
EAST = pl.ds(NARROW, NARROW)
PIECES = (
    (('up', 0, 384, ALL, 0),),
    (('up', 384, 128, ALL, 384), ('down', 0, TILE, LO, NARROW), ('down', NARROW, TILE, HI, NARROW)),
    (('down', TILE, TILE, LO, 768), ('down', 768, TILE, HI, 768)),
)


def place(ref, fixed, rows, cols):
    return ref.at[region(fixed, rows, cols)]


def region(fixed, rows, cols):
    return tuple(fixed.get(axis, ALL) for axis in range(3)) + (rows, cols)


def coords_of(k):
    return k // (SIDE * SIDE), lax.rem(k // SIDE, SIDE), lax.rem(k, SIDE)


def aligned(start, size):
    return pl.ds(pl.multiple_of(start, size), size)


def kernel(group_size, grad_attn, grad_up, grad_down, mom_attn, mom_up, mom_down,
           mo_attn, mo_up, mo_down, got_attn, got_up, got_down,
           own, peer, full, recv0, recv1, recv2, mom_pk, swap_attn, swap_up, swap_down,
           send_attn, send_up, send_down, x_mat, a_mat, b_mat, turn,
           load_sem, push_sem, pull_sem, rs_send, rs_recv, ag_send, ag_recv, ex_send, ex_recv):
    me = lax.axis_index('data')
    core = lax.rem(me, 2)
    chip = me // 2
    pos = coords_of(chip)
    partner = me + 1 - 2 * core
    recvs = (recv0, recv1, recv2)

    def at_axis(axis, coord):
        coords = list(pos)
        coords[axis] = coord
        return ((coords[0] * SIDE + coords[1]) * SIDE + coords[2]) * 2 + core

    right = [lax.rem(p + 1, SIDE) for p in pos]
    left = [lax.rem(p + 3, SIDE) for p in pos]
    far = [lax.rem(p + 2, SIDE) for p in pos]
    right_dev = [at_axis(a, right[a]) for a in range(3)]
    left_dev = [at_axis(a, left[a]) for a in range(3)]

    def remote(src, dst, send_sem, recv_sem, device):
        return pltpu.make_async_remote_copy(src_ref=src, dst_ref=dst, send_sem=send_sem, recv_sem=recv_sem,
                                            device_id={'data': device}, device_id_type=pl.DeviceIdType.MESH)

    barrier = pltpu.get_barrier_semaphore()
    for device in [partner] + right_dev + left_dev:
        pl.semaphore_signal(barrier, inc=1, device_id={'data': device}, device_id_type=pl.DeviceIdType.MESH)
    pl.semaphore_wait(barrier, 7)

    def turns(color):
        axis = ORDER[color][0]
        return axis, (far[axis], right[axis], left[axis], pos[axis])

    def attn_copy(color, turn_idx, push):
        axis, coords = turns(color)
        cols = pl.ds(*COLS[color])
        src = place(grad_attn, {axis: coords[turn_idx]}, ALL, cols)
        if push:
            dst = place(peer, {axis: coords[turn_idx]}, ALL, cols)
            return remote(src, dst, push_sem.at[color, turn_idx, 0], pull_sem.at[color, turn_idx, 0], partner)
        dst = place(own, {axis: coords[turn_idx]}, ALL, cols)
        return pltpu.make_async_copy(src, dst, load_sem.at[color, turn_idx, 0])

    def expert_copies(color, turn_idx, push):
        axis, coords = turns(color)
        copies = []
        for k, (source, col, width, rows, packed) in enumerate(PIECES[color]):
            src = place(grad_up if source == 'up' else grad_down, {axis: coords[turn_idx]}, ALL, pl.ds(col, width))
            target = peer if push else own
            dst = place(target, {axis: coords[turn_idx]}, rows, pl.ds(packed, width))
            if push:
                copies.append(remote(src, dst, push_sem.at[color, turn_idx, k], pull_sem.at[color, turn_idx, k], partner))
            else:
                copies.append(pltpu.make_async_copy(src, dst, load_sem.at[color, turn_idx, k]))
        return copies

    def mom_copies_from_0():
        return [remote(mom_up, swap_up, ex_send.at[0], ex_recv.at[0], partner),
                remote(mom_down, swap_down, ex_send.at[1], ex_recv.at[1], partner)]

    def mom_copies_from_1():
        return [remote(mom_attn, swap_attn, ex_send.at[0], ex_recv.at[0], partner)]

    @pl.when(core == 0)
    def _():
        for turn_idx in range(SIDE):
            for color in range(3):
                attn_copy(color, turn_idx, False).start()
                for copy in expert_copies(color, turn_idx, True):
                    copy.start()
        for copy in mom_copies_from_0():
            copy.start()

    @pl.when(core == 1)
    def _():
        for turn_idx in range(SIDE):
            for color in range(3):
                for copy in expert_copies(color, turn_idx, False):
                    copy.start()
                attn_copy(color, turn_idx, True).start()
        for copy in mom_copies_from_1():
            copy.start()

    def chip_sum(color, turn_idx):
        @pl.when(core == 0)
        def _():
            attn_copy(color, turn_idx, False).wait()
            attn_copy(color, turn_idx, True).wait_recv()

        @pl.when(core == 1)
        def _():
            for copy in expert_copies(color, turn_idx, False):
                copy.wait()
            for copy in expert_copies(color, turn_idx, True):
                copy.wait_recv()
        axis, coords = turns(color)
        idx = region({axis: coords[turn_idx]}, ALL, pl.ds(*COLS[color]))
        own[idx] = own[idx] + peer[idx]

    def rs_ctx(phase, color):
        order = ORDER[color]
        axis = order[phase]
        fixed = {order[k]: pos[order[k]] for k in range(phase)}
        return axis, fixed, pl.ds(*COLS[color])

    def rs_buf(phase, color, piece):
        col, width = COLS[color]
        lead = (piece,) + (ALL,) * (2 - phase)
        return recvs[phase].at[lead + (ALL, pl.ds(col, width))]

    def rs_copy(phase, color, piece):
        axis, fixed, cols = rs_ctx(phase, color)
        coord, half, device = ((far, 0, right_dev), (far, 1, left_dev), (right, 1, right_dev),
                               (left, 0, left_dev), (right, 0, right_dev), (left, 1, left_dev))[piece]
        src = place(own, {**fixed, axis: coord[axis]}, HALF[half], cols)
        return remote(src, rs_buf(phase, color, piece), rs_send.at[phase, color, piece], rs_recv.at[phase, color, piece],
                      device[axis])

    def rs_add(phase, color, coord, half, pieces):
        axis, fixed, cols = rs_ctx(phase, color)
        idx = region({**fixed, axis: coord[axis]}, HALF[half], cols)
        total = own[idx]
        for piece in pieces:
            col, width = COLS[color]
            lead = (piece,) + (ALL,) * (2 - phase)
            total = total + recvs[phase][lead + (ALL, pl.ds(col, width))]
        own[idx] = total

    def rs_mid(phase, color):
        rs_copy(phase, color, 0).wait_recv()
        rs_add(phase, color, right, 0, (0,))
        rs_copy(phase, color, 4).start()
        rs_copy(phase, color, 1).wait_recv()
        rs_add(phase, color, left, 1, (1,))
        rs_copy(phase, color, 5).start()

    def rs_end(phase, color):
        for piece in (2, 3, 4, 5):
            rs_copy(phase, color, piece).wait_recv()
        rs_add(phase, color, pos, 0, (3, 4))
        rs_add(phase, color, pos, 1, (2, 5))

    for color in range(3):
        chip_sum(color, 0)
        rs_copy(0, color, 0).start()
        rs_copy(0, color, 1).start()
    for color in range(3):
        chip_sum(color, 1)
        rs_copy(0, color, 2).start()
    for color in range(3):
        chip_sum(color, 2)
        rs_copy(0, color, 3).start()
    for color in range(3):
        rs_mid(0, color)
    for color in range(3):
        chip_sum(color, 3)
    for phase in range(3):
        if phase > 0:
            for color in range(3):
                rs_mid(phase, color)
        for color in range(3):
            rs_end(phase, color)
            if phase < 2:
                for piece in range(4):
                    rs_copy(phase + 1, color, piece).start()

    @pl.when(core == 0)
    def _():
        mom_copies_from_1()[0].wait_recv()
        mom_pk[LO] = mom_attn[...]
        mom_pk[HI] = swap_attn[...]

    @pl.when(core == 1)
    def _():
        for copy in mom_copies_from_0():
            copy.wait_recv()
        mom_pk[LO, WEST] = swap_up[...]
        mom_pk[HI, WEST] = mom_up[...]
        for first, cols in ((0, WEST), (8, EAST)):
            mom_pk[pl.ds(first, SIDE), EAST] = swap_down[:, cols]
            mom_pk[pl.ds(first + SIDE, SIDE), EAST] = mom_down[:, cols]

    mine = pos
    mom_new = MOMENTUM * mom_pk[...] + own[mine] * (1.0 / group_size)
    full[mine] = mom_new

    def ag_copy(phase, color, piece):
        order = ORDER[color]
        axis = order[phase]
        fixed = {order[k]: pos[order[k]] for k in range(phase)}
        coord, half, device = ((pos, 0, right_dev), (pos, 1, left_dev), (pos, 1, right_dev), (pos, 0, left_dev),
                               (left, 0, right_dev), (right, 1, left_dev))[piece]
        part = place(full, {**fixed, axis: coord[axis]}, HALF[half], pl.ds(*COLS[color]))
        return remote(part, part, ag_send.at[phase, color, piece], ag_recv.at[phase, color, piece], device[axis])

    def ag_arrive(phase, color, piece):
        order = ORDER[color]
        axis = order[phase]
        fixed = {order[k]: pos[order[k]] for k in range(phase)}
        coord, half = ((left, 0), (right, 1), (left, 1), (right, 0), (far, 0), (far, 1))[piece]
        part = place(full, {**fixed, axis: coord[axis]}, HALF[half], pl.ds(*COLS[color]))
        remote(part, part, ag_send.at[phase, color, piece], ag_recv.at[phase, color, piece], right_dev[axis]).wait_recv()

    for color in range(3):
        for piece in range(4):
            ag_copy(2, color, piece).start()
    for phase in (2, 1, 0):
        for color in range(3):
            ag_arrive(phase, color, 0)
            ag_copy(phase, color, 4).start()
            ag_arrive(phase, color, 1)
            ag_copy(phase, color, 5).start()
        for color in range(3):
            for piece in (2, 3, 4, 5):
                ag_arrive(phase, color, piece)
            if phase > 0:
                for piece in range(4):
                    ag_copy(phase - 1, color, piece).start()

    @pl.when(core == 0)
    def _():
        send_attn[...] = full[mine + (HI, ALL)]
        mo_attn[...] = full[mine + (LO, ALL)]

    @pl.when(core == 1)
    def _():
        send_up[...] = full[mine + (LO, WEST)]
        mo_up[...] = full[mine + (HI, WEST)]
        for rows, cols in ((LO, WEST), (HI, EAST)):
            down = full[mine + (rows, EAST)]
            send_down[:, cols] = down[:SIDE]
            mo_down[:, cols] = down[SIDE:]

    def back_from_0(base, out_attn):
        return [remote(send_attn, out_attn, ex_send.at[base], ex_recv.at[base], partner)]

    def back_from_1(base, out_up, out_down):
        return [remote(send_up, out_up, ex_send.at[base], ex_recv.at[base], partner),
                remote(send_down, out_down, ex_send.at[base + 1], ex_recv.at[base + 1], partner)]

    @pl.when(core == 0)
    def _():
        for copy in back_from_0(2, mo_attn):
            copy.start()

    @pl.when(core == 1)
    def _():
        for copy in back_from_1(2, mo_up, mo_down):
            copy.start()

    def weighted(a_val, q_val):
        return (COEF_B * a_val.astype(F32) + COEF_C * q_val.astype(BF16).astype(F32)).astype(BF16)

    def advance(x_val, y_val):
        return (COEF_A * x_val.astype(F32) + y_val.astype(BF16).astype(F32)).astype(BF16)

    def symmetric(out, base, size, block):
        for j in range(0, size, TILE):
            val = block(j)
            out[pl.ds(base + j, size - j), pl.ds(j, TILE)] = val
            if j + TILE < size:
                out[pl.ds(base + j, TILE), pl.ds(j + TILE, size - j - TILE)] = jnp.transpose(val[TILE:])

    def gram(base, size):
        def block(j):
            return lax.dot_general(x_mat[pl.ds(base + j, size - j), :], x_mat[pl.ds(base + j, TILE), :], (((1,), (1,)), ((), ())),
                                   preferred_element_type=F32).astype(BF16)
        symmetric(a_mat, base, size, block)

    def poly(base, size):
        def block(j):
            rows, cols = pl.ds(base + j, size - j), pl.ds(j, TILE)
            q_val = jnp.dot(a_mat[rows, pl.ds(0, size)], a_mat[pl.ds(base, size), cols], preferred_element_type=F32)
            return weighted(a_mat[rows, cols], q_val)
        symmetric(b_mat, base, size, block)

    def update(base, size):
        rows = pl.ds(base, size)
        y_val = jnp.dot(b_mat[rows, pl.ds(0, size)], x_mat[rows, :], preferred_element_type=F32)
        x_mat[rows, :] = advance(x_mat[rows, :], y_val)

    def square_sum(cols):
        def body(k, acc):
            val = full[coords_of(k) + (ALL, cols)]
            return acc + val * val
        acc = lax.fori_loop(0, 64, body, jnp.zeros((16, cols.size), F32))
        return jnp.sum(acc, axis=(0, 1), keepdims=True)

    def inverse(total):
        return 1.0 / (jnp.sqrt(total) + EPSILON)

    @pl.when(core == 0)
    def _():
        scale = inverse(square_sum(pl.ds(0, WIDE)))

        def fill(k, carry):
            val = full[coords_of(k)]
            x_mat[aligned(k * CHIP_ROWS, CHIP_ROWS), :] = (val * scale).astype(BF16)
            return carry
        lax.fori_loop(0, 64, fill, 0)

        def step(_, carry):
            gram(0, WIDE)
            poly(0, WIDE)
            update(0, WIDE)
            return carry
        lax.fori_loop(0, NS_STEPS - 1, step, 0)
        gram(0, WIDE)
        rows = aligned(chip * CHIP_ROWS, CHIP_ROWS)
        a_val = a_mat[rows, :]
        b_val = weighted(a_val, jnp.dot(a_val, a_mat[...], preferred_element_type=F32))
        out = advance(x_mat[rows, :], jnp.dot(b_val, x_mat[...], preferred_element_type=F32)).astype(F32)
        back_from_0(2, mo_attn)[0].wait_send()
        send_attn[...] = out[8:]
        got_attn[...] = out[:8]
        back_from_0(4, got_attn)[0].start()

    @pl.when(core == 1)
    def _():
        scale_up = inverse(square_sum(WEST))
        scale_down = inverse(square_sum(EAST))

        def fill_up(k, carry):
            val = full[k // 2, pl.ds(2 * lax.rem(k, 2), 2), :, :, WEST].reshape(128, NARROW)
            x_mat[WEST, aligned(k * 128, 128)] = jnp.transpose(val * scale_up).astype(BF16)
            return carry
        lax.fori_loop(0, 8, fill_up, 0)

        def fill_down(k, carry):
            z, y, x = coords_of(2 * k)
            val = full[z, y, pl.ds(x, 2), :, EAST] * scale_down
            rows = aligned(NARROW + k * CHIP_ROWS, CHIP_ROWS)
            x_mat[rows, WEST] = val[:, :8].reshape(CHIP_ROWS, NARROW).astype(BF16)
            x_mat[rows, EAST] = val[:, 8:].reshape(CHIP_ROWS, NARROW).astype(BF16)
            return carry
        lax.fori_loop(0, 32, fill_down, 0)

        def step(_, carry):
            for stage in (gram, poly, update):
                stage(0, NARROW)
                stage(NARROW, NARROW)
            return carry
        lax.fori_loop(0, NS_STEPS - 1, step, 0)
        gram(0, NARROW)
        gram(NARROW, NARROW)
        poly(0, NARROW)
        cols = aligned(chip // 8 * 128, 128)
        out_up = advance(x_mat[WEST, cols], jnp.dot(b_mat[WEST, WEST], x_mat[WEST, cols], preferred_element_type=F32))
        turn[...] = jnp.transpose(out_up.astype(F32))
        rows = aligned(NARROW + chip // 2 * CHIP_ROWS, CHIP_ROWS)
        a_val = a_mat[rows, WEST]
        b_val = weighted(a_val, jnp.dot(a_val, a_mat[EAST, WEST], preferred_element_type=F32))
        both = advance(x_mat[rows, :], jnp.dot(b_val, x_mat[EAST, :], preferred_element_type=F32)).astype(F32)
        out_down = jnp.where(lax.rem(chip, 2) == 0, both[:8], both[8:])
        for copy in back_from_1(2, mo_up, mo_down):
            copy.wait_send()
        first = pl.multiple_of(lax.rem(chip, 8) * CHIP_ROWS, CHIP_ROWS)
        send_up[...] = turn[pl.ds(first, 8), :]
        got_up[...] = turn[pl.ds(first + 8, 8), :]
        send_down[...] = out_down[:SIDE]
        got_down[...] = out_down[SIDE:]
        for copy in back_from_1(4, got_up, got_down):
            copy.start()

    @pl.when(core == 0)
    def _():
        for copy in back_from_1(2, mo_up, mo_down) + back_from_1(4, got_up, got_down):
            copy.wait_recv()

    @pl.when(core == 1)
    def _():
        for copy in back_from_0(2, mo_attn) + back_from_0(4, got_attn):
            copy.wait_recv()

    @pl.when(core == 0)
    def _():
        for turn_idx in range(SIDE):
            for color in range(3):
                for copy in expert_copies(color, turn_idx, True):
                    copy.wait_send()
        for copy in mom_copies_from_0() + back_from_0(4, got_attn):
            copy.wait_send()

    @pl.when(core == 1)
    def _():
        for turn_idx in range(SIDE):
            for color in range(3):
                attn_copy(color, turn_idx, True).wait_send()
        for copy in mom_copies_from_1() + back_from_1(4, got_up, got_down):
            copy.wait_send()

    for phase in range(3):
        for color in range(3):
            for piece in range(6):
                rs_copy(phase, color, piece).wait_send()
                ag_copy(phase, color, piece).wait_send()


def finish(*refs):
    for k in range(3):
        mom, out, mas = refs[k], refs[3 + k], refs[6 + k]
        mom_out, mas_out, low_out = refs[9 + 3 * k:12 + 3 * k]
        old = mas[...]
        new = old - LEARN_RATE * (0.2 * math.sqrt(WIDE) * out[...] + WEIGHT_DECAY * old)
        mom_out[...] = mom[...]
        mas_out[...] = new
        low_out[...] = new.astype(BF16)


def solution(mesh):
    group_size = mesh.shape['data']
    grad_spec = P(('stage', 'data'), None, None, None)
    row_spec = P('stage', 'data', None)

    def step_local(grad_attn, mom_attn, mas_attn, grad_up, mom_up, mas_up, grad_down, mom_down, mas_down):
        vmem = pl.BlockSpec(memory_space=pltpu.VMEM)
        hbm = pl.BlockSpec(memory_space=pl.ANY)
        shapes = ((8, WIDE), (8, NARROW), (SIDE, WIDE))
        sem = pltpu.SemaphoreType.DMA
        scratch = [
            *[pltpu.VMEM(BLOCK, F32)] * 3,
            *[pltpu.VMEM((6,) + (SIDE,) * free + (8, WIDE), F32) for free in (2, 1, 0)],
            pltpu.VMEM((CHIP_ROWS, WIDE), F32),
            *[pltpu.VMEM(shape, F32) for shape in shapes * 2],
            *[pltpu.VMEM((WIDE, WIDE), BF16)] * 3,
            pltpu.VMEM((128, NARROW), F32),
            *[sem((3, SIDE, 3))] * 3,
            *[sem((3, 3, 6))] * 4,
            *[sem((6,))] * 2,
        ]
        result = pl.pallas_call(
            functools.partial(kernel, group_size),
            out_shape=[jax.ShapeDtypeStruct(shape, F32) for shape in shapes * 2],
            in_specs=[hbm] * 3 + [vmem] * 3,
            out_specs=[vmem] * 6,
            scratch_shapes=scratch,
            compiler_params=pltpu.CompilerParams(collective_id=0, has_side_effects=True, vmem_limit_bytes=60 * 1024 * 1024),
            name='muon',
        )(grad_attn.reshape(BLOCK), grad_up.reshape(BLOCK[:4] + (NARROW,)), grad_down.reshape(BLOCK[:3] + (8, WIDE)),
          mom_attn[0], mom_up[0], mom_down[0])
        outs = [jax.ShapeDtypeStruct(shape, dtype) for shape in shapes for dtype in (F32, F32, BF16)]
        done = pl.pallas_call(finish, out_shape=outs, in_specs=[vmem] * 9, out_specs=[vmem] * 9, name='finish')(
            *result, mas_attn[0], mas_up[0], mas_down[0])
        return tuple(d[None] for d in done)

    return jax.shard_map(step_local, mesh=mesh, in_specs=(grad_spec, row_spec, row_spec) * 3, out_specs=(row_spec,) * 9,
                         check_vma=False)
```

```python
import functools
import math

import jax
import jax.numpy as jnp
from jax import lax
from jax.experimental import pallas as pl
from jax.experimental.pallas import tpu as pltpu
from jax.sharding import PartitionSpec as P

MOMENTUM = 0.95
LEARN_RATE = 0.25
WEIGHT_DECAY = 0.2
EPSILON = 1e-7
COEF_A = 3.4445
COEF_B = -4.7750
COEF_C = 2.0315
NS_STEPS = 5

F32 = jnp.float32
BF16 = jnp.bfloat16

COLS = ((0, 384), (384, 384), (768, 256))
ORDER = ((0, 1, 2), (1, 2, 0), (2, 0, 1))
ATTN = 1
EXPERT = 0
SIDE = 4
CHIP_ROWS = 16
WIDE = 1024
NARROW = 512
TILE = 256
BLOCK = (SIDE, SIDE, SIDE, CHIP_ROWS, WIDE)
ALL = slice(None)
LO = pl.ds(0, 8)
HI = pl.ds(8, 8)
HALF = (LO, HI)
WEST = pl.ds(0, NARROW)
EAST = pl.ds(NARROW, NARROW)
PIECES = (
    (('up', 0, 384, ALL, 0),),
    (('up', 384, 128, ALL, 384), ('down', 0, TILE, LO, NARROW), ('down', NARROW, TILE, HI, NARROW)),
    (('down', TILE, TILE, LO, 768), ('down', 768, TILE, HI, 768)),
)


def place(ref, fixed, rows, cols):
    return ref.at[region(fixed, rows, cols)]


def region(fixed, rows, cols):
    return tuple(fixed.get(axis, ALL) for axis in range(3)) + (rows, cols)


def coords_of(k):
    return k // (SIDE * SIDE), lax.rem(k // SIDE, SIDE), lax.rem(k, SIDE)


def aligned(start, size):
    return pl.ds(pl.multiple_of(start, size), size)


def kernel(group_size, grad_attn, grad_up, grad_down, mom_attn, mom_up, mom_down,
           mo_attn, mo_up, mo_down, got_attn, got_up, got_down,
           own, peer, full, recv0, recv1, recv2, mom_pk, swap_attn, swap_up, swap_down, keep_attn, keep_up, keep_down,
           send_attn, send_up, send_down, x_mat, a_mat, b_mat, turn, x_all, norms, scales,
           load_sem, push_sem, pull_sem, rs_send, rs_recv, ag_send, ag_recv, ex_send, ex_recv, keep_sem, norm_send, norm_recv, gate):
    me = lax.axis_index('data')
    core = lax.rem(me, 2)
    chip = me // 2
    pos = coords_of(chip)
    partner = me + 1 - 2 * core
    recvs = (recv0, recv1, recv2)

    def at_axis(axis, coord):
        coords = list(pos)
        coords[axis] = coord
        return ((coords[0] * SIDE + coords[1]) * SIDE + coords[2]) * 2 + core

    right = [lax.rem(p + 1, SIDE) for p in pos]
    left = [lax.rem(p + 3, SIDE) for p in pos]
    far = [lax.rem(p + 2, SIDE) for p in pos]
    right_dev = [at_axis(a, right[a]) for a in range(3)]
    left_dev = [at_axis(a, left[a]) for a in range(3)]
    far_dev = [at_axis(a, far[a]) for a in range(3)]

    def remote(src, dst, send_sem, recv_sem, device):
        return pltpu.make_async_remote_copy(src_ref=src, dst_ref=dst, send_sem=send_sem, recv_sem=recv_sem,
                                            device_id={'data': device}, device_id_type=pl.DeviceIdType.MESH)

    def turns(color):
        axis = ORDER[color][0]
        return axis, (far[axis], right[axis], left[axis], pos[axis])

    def attn_copy(color, turn_idx, push):
        axis, coords = turns(color)
        cols = pl.ds(*COLS[color])
        src = place(grad_attn, {axis: coords[turn_idx]}, ALL, cols)
        if push:
            dst = place(peer, {axis: coords[turn_idx]}, ALL, cols)
            return remote(src, dst, push_sem.at[color, turn_idx, 0], pull_sem.at[color, turn_idx, 0], partner)
        dst = place(own, {axis: coords[turn_idx]}, ALL, cols)
        return pltpu.make_async_copy(src, dst, load_sem.at[color, turn_idx, 0])

    def expert_copies(color, turn_idx, push):
        axis, coords = turns(color)
        copies = []
        for k, (source, col, width, rows, packed) in enumerate(PIECES[color]):
            src = place(grad_up if source == 'up' else grad_down, {axis: coords[turn_idx]}, ALL, pl.ds(col, width))
            target = peer if push else own
            dst = place(target, {axis: coords[turn_idx]}, rows, pl.ds(packed, width))
            if push:
                copies.append(remote(src, dst, push_sem.at[color, turn_idx, k], pull_sem.at[color, turn_idx, k], partner))
            else:
                copies.append(pltpu.make_async_copy(src, dst, load_sem.at[color, turn_idx, k]))
        return copies

    def mom_from_attn():
        return [remote(mom_up, swap_up, ex_send.at[0], ex_recv.at[0], partner),
                remote(mom_down, swap_down, ex_send.at[1], ex_recv.at[1], partner)]

    def mom_from_expert():
        return [remote(mom_attn, swap_attn, ex_send.at[0], ex_recv.at[0], partner)]

    def keep_copies(role):
        pairs = ((mom_attn, keep_attn),) if role == ATTN else ((mom_up, keep_up), (mom_down, keep_down))
        return [pltpu.make_async_copy(src, dst, keep_sem.at[k]) for k, (src, dst) in enumerate(pairs)]

    barrier = pltpu.get_barrier_semaphore()
    for device in [partner] + right_dev + left_dev + far_dev:
        pl.semaphore_signal(barrier, inc=1, device_id={'data': device}, device_id_type=pl.DeviceIdType.MESH)

    @pl.when(core == ATTN)
    def _():
        for turn_idx in range(SIDE):
            for color in range(3):
                attn_copy(color, turn_idx, False).start()
        for copy in keep_copies(ATTN):
            copy.start()

    with jax.named_scope('barrier'):
        pl.semaphore_wait(barrier, 10)

    @pl.when(core == ATTN)
    def _():
        for copy in mom_from_attn():
            copy.start()
        for turn_idx in range(SIDE):
            for color in range(3):
                for copy in expert_copies(color, turn_idx, True):
                    copy.start()

    @pl.when(core == EXPERT)
    def _():
        for turn_idx in range(SIDE):
            for color in range(3):
                attn_copy(color, turn_idx, True).start()
        for copy in mom_from_expert():
            copy.start()
        for copy in keep_copies(EXPERT):
            copy.start()
        for turn_idx in range(SIDE):
            for color in range(3):
                for copy in expert_copies(color, turn_idx, False):
                    copy.start()
        with jax.named_scope('gate'):
            pl.semaphore_wait(gate, 1)

    def open_gate():
        @pl.when(core == ATTN)
        def _():
            pl.semaphore_signal(gate, inc=1, device_id={'data': partner}, device_id_type=pl.DeviceIdType.MESH)

    def chip_sum(color, turn_idx):
        @pl.when(core == ATTN)
        def _():
            attn_copy(color, turn_idx, False).wait()
            attn_copy(color, turn_idx, True).wait_recv()

        @pl.when(core == EXPERT)
        def _():
            for copy in expert_copies(color, turn_idx, False):
                copy.wait()
            for copy in expert_copies(color, turn_idx, True):
                copy.wait_recv()
        axis, coords = turns(color)
        idx = region({axis: coords[turn_idx]}, ALL, pl.ds(*COLS[color]))
        own[idx] = own[idx] + peer[idx]

    PAIRED = ((far, 0, right_dev), (far, 1, left_dev), (right, 1, right_dev), (left, 0, left_dev), (right, 0, right_dev), (left, 1, left_dev))
    DIRECT = ((far, far_dev), (right, right_dev), (left, left_dev))

    def ctx(phase, color):
        order = ORDER[color]
        return order[phase], {order[k]: pos[order[k]] for k in range(phase)}, pl.ds(*COLS[color])

    def rs_slot(phase, color, piece):
        return (piece,) + (ALL,) * (2 - phase) + (ALL, pl.ds(*COLS[color]))

    def rs_copy(phase, color, piece):
        axis, fixed, cols = ctx(phase, color)
        if phase < 2:
            coord, half, device = PAIRED[piece]
            rows = HALF[half]
        else:
            coord, device = DIRECT[piece]
            rows = ALL
        src = place(own, {**fixed, axis: coord[axis]}, rows, cols)
        return remote(src, recvs[phase].at[rs_slot(phase, color, piece)], rs_send.at[phase, color, piece],
                      rs_recv.at[phase, color, piece], device[axis])

    def rs_add(phase, color, coord, rows, pieces):
        axis, fixed, cols = ctx(phase, color)
        idx = region({**fixed, axis: coord[axis]}, rows, cols)
        total = own[idx]
        for piece in pieces:
            total = total + recvs[phase][rs_slot(phase, color, piece)]
        own[idx] = total

    def rs_mid(phase, color):
        rs_copy(phase, color, 0).wait_recv()
        rs_add(phase, color, right, LO, (0,))
        rs_copy(phase, color, 4).start()
        rs_copy(phase, color, 1).wait_recv()
        rs_add(phase, color, left, HI, (1,))
        rs_copy(phase, color, 5).start()

    def rs_end(phase, color):
        for piece in (2, 3, 4, 5):
            rs_copy(phase, color, piece).wait_recv()
        rs_add(phase, color, pos, LO, (3, 4))
        rs_add(phase, color, pos, HI, (2, 5))

    with jax.named_scope('rs0_load'):
        for color in range(3):
            chip_sum(color, 0)
            rs_copy(0, color, 0).start()
            rs_copy(0, color, 1).start()
        open_gate()
        for turn_idx in (1, 2):
            for color in range(3):
                chip_sum(color, turn_idx)
                rs_copy(0, color, turn_idx + 1).start()
    with jax.named_scope('rs0_mid'):
        for color in range(3):
            rs_mid(0, color)
        for color in range(3):
            chip_sum(color, 3)
    with jax.named_scope('rs0_end'):
        for color in range(3):
            rs_end(0, color)
            for piece in range(4):
                rs_copy(1, color, piece).start()
    with jax.named_scope('rs1_mid'):
        for color in range(3):
            rs_mid(1, color)
    with jax.named_scope('rs1_end'):
        for color in range(3):
            rs_end(1, color)
            for piece in range(3):
                rs_copy(2, color, piece).start()
    with jax.named_scope('rs2'):
        for color in range(3):
            for piece in range(3):
                rs_copy(2, color, piece).wait_recv()
            rs_add(2, color, pos, ALL, range(3))

    @pl.when(core == ATTN)
    def _():
        mom_from_expert()[0].wait_recv()
        keep_copies(ATTN)[0].wait()
        mom_pk[LO] = swap_attn[...]
        mom_pk[HI] = keep_attn[...]

    @pl.when(core == EXPERT)
    def _():
        for copy in mom_from_attn():
            copy.wait_recv()
        for copy in keep_copies(EXPERT):
            copy.wait()
        mom_pk[LO, WEST] = keep_up[...]
        mom_pk[HI, WEST] = swap_up[...]
        for first, cols in ((0, WEST), (8, EAST)):
            mom_pk[pl.ds(first, SIDE), EAST] = keep_down[:, cols]
            mom_pk[pl.ds(first + SIDE, SIDE), EAST] = swap_down[:, cols]

    mine = pos
    mom_new = MOMENTUM * mom_pk[...] + own[mine] * (1.0 / group_size)
    full[mine] = mom_new

    AG_SEND = ((pos, 0, right_dev), (pos, 1, left_dev), (pos, 1, right_dev), (pos, 0, left_dev), (left, 0, right_dev), (right, 1, left_dev))
    AG_LAND = ((left, 0), (right, 1), (left, 1), (right, 0), (far, 0), (far, 1))
    AG_DIRECT = (far, left, right)

    def ag_part(phase, color, coord, rows):
        axis, fixed, cols = ctx(phase, color)
        return place(full, {**fixed, axis: coord[axis]}, rows, cols)

    def ag_half(phase, color, coord, half):
        if phase == 1:
            return ag_part(phase, color, coord, HALF[half])
        axis, second, _ = ORDER[color]
        return place(x_all, {axis: coord[axis], second: pl.ds(2 * half, 2)}, ALL, pl.ds(*COLS[color]))

    def ag_remote(part, phase, color, piece, device):
        return remote(part, part, ag_send.at[phase, color, piece], ag_recv.at[phase, color, piece], device[ORDER[color][phase]])

    def ag_copy(phase, color, piece):
        if phase < 2:
            coord, half, device = AG_SEND[piece]
            return ag_remote(ag_half(phase, color, coord, half), phase, color, piece, device)
        return ag_remote(ag_part(phase, color, pos, ALL), phase, color, piece, DIRECT[piece][1])

    def ag_arrive(phase, color, piece):
        if phase < 2:
            coord, half = AG_LAND[piece]
            part = ag_half(phase, color, coord, half)
        else:
            part = ag_part(phase, color, AG_DIRECT[piece], ALL)
        ag_remote(part, phase, color, piece, right_dev).wait_recv()

    def drain_push():
        @pl.when(core == ATTN)
        def _():
            for turn_idx in range(SIDE):
                for color in range(3):
                    for copy in expert_copies(color, turn_idx, True):
                        copy.wait_send()
            for copy in mom_from_attn():
                copy.wait_send()

        @pl.when(core == EXPERT)
        def _():
            for turn_idx in range(SIDE):
                for color in range(3):
                    attn_copy(color, turn_idx, True).wait_send()
            for copy in mom_from_expert():
                copy.wait_send()

    with jax.named_scope('ag2'):
        for color in range(3):
            for piece in range(3):
                ag_copy(2, color, piece).start()
        drain_push()
        for color in range(3):
            for piece in range(3):
                ag_arrive(2, color, piece)
            for piece in range(4):
                ag_copy(1, color, piece).start()
    def drain(phase, make):
        for color in range(3):
            for piece in range(6 if phase < 2 else 3):
                make(phase, color, piece).wait_send()

    def ag_mid(phase):
        for color in range(3):
            ag_arrive(phase, color, 0)
            ag_copy(phase, color, 4).start()
            ag_arrive(phase, color, 1)
            ag_copy(phase, color, 5).start()

    def norm_copy(color, piece):
        axis = ORDER[color][0]
        part = norms.at[color, pos[axis]]
        return remote(part, part, norm_send.at[color, piece], norm_recv.at[color, piece], DIRECT[piece][1][axis])

    def norm_arrive(color, piece):
        axis = ORDER[color][0]
        part = norms.at[color, AG_DIRECT[piece][axis]]
        remote(part, part, norm_send.at[color, piece], norm_recv.at[color, piece], right_dev[axis]).wait_recv()

    def square_tile(plane, cols):
        val = full[plane + (ALL, cols)].reshape(32, 8, cols.size)
        val = jnp.sum(val * val, axis=0)
        return sum(val[:, k:k + 128] for k in range(0, cols.size, 128))

    def norm_start(color):
        axis = ORDER[color][0]
        plane = region({axis: pos[axis]}, ALL, ALL)[:3]
        first, width = COLS[color]
        west = max(0, min(NARROW - first, width))
        for side, (start, size) in enumerate(((first, west), (first + west, width - west))):
            val = square_tile(plane, pl.ds(start, size)) if size else jnp.zeros((8, 128), F32)
            norms[color, pos[axis], side] = val
        for piece in range(3):
            norm_copy(color, piece).start()

    drain(1, rs_copy)
    drain(2, ag_copy)
    with jax.named_scope('ag1_mid'):
        ag_mid(1)
    with jax.named_scope('ag1_end'):
        for color in range(3):
            for piece in (2, 3, 4, 5):
                ag_arrive(1, color, piece)
            norm_start(color)
    drain(0, rs_copy)
    drain(2, rs_copy)
    drain(1, ag_copy)
    with jax.named_scope('norm'):
        for color in range(3):
            for piece in range(3):
                norm_arrive(color, piece)
        tiles = [norms[color, j] for color in range(3) for j in range(SIDE)]
        total = jnp.sum(sum(tiles), axis=(1, 2), keepdims=True)
        west, east = total[0], total[1]
        both = west + east
        west = jnp.where(core == ATTN, both, west)
        east = jnp.where(core == ATTN, both, east)
        lane = lax.broadcasted_iota(jnp.int32, (1, WIDE), 1)
        norm = jnp.sqrt(jnp.where(lane < NARROW, west, east))
        scales[...] = 1.0 / (norm + EPSILON)
    with jax.named_scope('ag0_start'):
        for color in range(3):
            axis, cols = ORDER[color][0], pl.ds(*COLS[color])
            idx = region({axis: pos[axis]}, ALL, cols)
            x_all[idx] = (full[idx] * scales[:, cols]).astype(BF16)
            for piece in range(4):
                ag_copy(0, color, piece).start()
    with jax.named_scope('ag0_mid'):
        ag_mid(0)
    with jax.named_scope('ag0_end'):
        for color in range(3):
            for piece in (2, 3, 4, 5):
                ag_arrive(0, color, piece)
    for color in range(3):
        for piece in range(3):
            norm_copy(color, piece).wait_send()
    drain(0, ag_copy)

    @pl.when(core == ATTN)
    def _():
        send_attn[...] = full[mine + (LO, ALL)]
        mo_attn[...] = full[mine + (HI, ALL)]

    @pl.when(core == EXPERT)
    def _():
        send_up[...] = full[mine + (HI, WEST)]
        mo_up[...] = full[mine + (LO, WEST)]
        for rows, cols in ((LO, WEST), (HI, EAST)):
            down = full[mine + (rows, EAST)]
            send_down[:, cols] = down[SIDE:]
            mo_down[:, cols] = down[:SIDE]

    def back_from_attn(base, out_attn):
        return [remote(send_attn, out_attn, ex_send.at[base], ex_recv.at[base], partner)]

    def back_from_expert(base, out_up, out_down):
        return [remote(send_up, out_up, ex_send.at[base], ex_recv.at[base], partner),
                remote(send_down, out_down, ex_send.at[base + 1], ex_recv.at[base + 1], partner)]

    @pl.when(core == ATTN)
    def _():
        for copy in back_from_attn(2, mo_attn):
            copy.start()

    @pl.when(core == EXPERT)
    def _():
        for copy in back_from_expert(2, mo_up, mo_down):
            copy.start()

    def weighted(a_val, q_val):
        return (COEF_B * a_val.astype(F32) + COEF_C * q_val.astype(BF16).astype(F32)).astype(BF16)

    def advance(x_val, y_val):
        return (COEF_A * x_val.astype(F32) + y_val.astype(BF16).astype(F32)).astype(BF16)

    def symmetric(out, base, size, block):
        for j in range(0, size, TILE):
            val = block(j)
            out[pl.ds(base + j, size - j), pl.ds(j, TILE)] = val
            if j + TILE < size:
                out[pl.ds(base + j, TILE), pl.ds(j + TILE, size - j - TILE)] = jnp.transpose(val[TILE:])

    def gram(base, size):
        def block(j):
            return lax.dot_general(x_mat[pl.ds(base + j, size - j), :], x_mat[pl.ds(base + j, TILE), :], (((1,), (1,)), ((), ())),
                                   preferred_element_type=F32).astype(BF16)
        symmetric(a_mat, base, size, block)

    def poly(base, size):
        def block(j):
            rows, cols = pl.ds(base + j, size - j), pl.ds(j, TILE)
            q_val = jnp.dot(a_mat[rows, pl.ds(0, size)], a_mat[pl.ds(base, size), cols], preferred_element_type=F32)
            return weighted(a_mat[rows, cols], q_val)
        symmetric(b_mat, base, size, block)

    def update(base, size):
        rows = pl.ds(base, size)
        y_val = jnp.dot(b_mat[rows, pl.ds(0, size)], x_mat[rows, :], preferred_element_type=F32)
        x_mat[rows, :] = advance(x_mat[rows, :], y_val)

    @pl.when(core == ATTN)
    def _():
        with jax.named_scope('fill'):
            x_mat[...] = x_all[...].reshape(WIDE, WIDE)

        def step(_, carry):
            gram(0, WIDE)
            poly(0, WIDE)
            update(0, WIDE)
            return carry
        with jax.named_scope('steps'):
            lax.fori_loop(0, NS_STEPS - 1, step, 0)
            gram(0, WIDE)
        rows = aligned(chip * CHIP_ROWS, CHIP_ROWS)
        a_val = a_mat[rows, :]
        b_val = weighted(a_val, jnp.dot(a_val, a_mat[...], preferred_element_type=F32))
        out = advance(x_mat[rows, :], jnp.dot(b_val, x_mat[...], preferred_element_type=F32)).astype(F32)
        back_from_attn(2, mo_attn)[0].wait_send()
        send_attn[...] = out[:8]
        got_attn[...] = out[8:]
        back_from_attn(4, got_attn)[0].start()

    @pl.when(core == EXPERT)
    def _():
        with jax.named_scope('fill'):
            def fill_up(k, carry):
                val = x_all[k // 2, pl.ds(2 * lax.rem(k, 2), 2), :, :, WEST].reshape(128, NARROW)
                x_mat[WEST, aligned(k * 128, 128)] = jnp.transpose(val)
                return carry
            lax.fori_loop(0, 8, fill_up, 0)

            def fill_down(k, carry):
                z, y, x = coords_of(2 * k)
                val = x_all[z, y, pl.ds(x, 2), :, EAST].astype(F32)
                rows = aligned(NARROW + k * CHIP_ROWS, CHIP_ROWS)
                x_mat[rows, WEST] = val[:, :8].reshape(CHIP_ROWS, NARROW).astype(BF16)
                x_mat[rows, EAST] = val[:, 8:].reshape(CHIP_ROWS, NARROW).astype(BF16)
                return carry
            lax.fori_loop(0, 32, fill_down, 0)

        def step(_, carry):
            for stage in (gram, poly, update):
                stage(0, NARROW)
                stage(NARROW, NARROW)
            return carry
        with jax.named_scope('steps'):
            lax.fori_loop(0, NS_STEPS - 1, step, 0)
            gram(0, NARROW)
            gram(NARROW, NARROW)
        poly(0, NARROW)
        cols = aligned(chip // 8 * 128, 128)
        out_up = advance(x_mat[WEST, cols], jnp.dot(b_mat[WEST, WEST], x_mat[WEST, cols], preferred_element_type=F32))
        turn[...] = jnp.transpose(out_up.astype(F32))
        rows = aligned(NARROW + chip // 2 * CHIP_ROWS, CHIP_ROWS)
        a_val = a_mat[rows, WEST]
        b_val = weighted(a_val, jnp.dot(a_val, a_mat[EAST, WEST], preferred_element_type=F32))
        both = advance(x_mat[rows, :], jnp.dot(b_val, x_mat[EAST, :], preferred_element_type=F32)).astype(F32)
        out_down = jnp.where(lax.rem(chip, 2) == 0, both[:8], both[8:])
        for copy in back_from_expert(2, mo_up, mo_down):
            copy.wait_send()
        first = pl.multiple_of(lax.rem(chip, 8) * CHIP_ROWS, CHIP_ROWS)
        send_up[...] = turn[pl.ds(first + 8, 8), :]
        got_up[...] = turn[pl.ds(first, 8), :]
        send_down[...] = out_down[SIDE:]
        got_down[...] = out_down[:SIDE]
        for copy in back_from_expert(4, got_up, got_down):
            copy.start()

    @pl.when(core == ATTN)
    def _():
        for copy in back_from_expert(2, mo_up, mo_down) + back_from_expert(4, got_up, got_down):
            copy.wait_recv()

    @pl.when(core == EXPERT)
    def _():
        for copy in back_from_attn(2, mo_attn) + back_from_attn(4, got_attn):
            copy.wait_recv()

    @pl.when(core == ATTN)
    def _():
        for copy in back_from_attn(4, got_attn):
            copy.wait_send()

    @pl.when(core == EXPERT)
    def _():
        for copy in back_from_expert(4, got_up, got_down):
            copy.wait_send()


def finish(*refs):
    for k in range(3):
        mom, out, mas = refs[k], refs[3 + k], refs[6 + k]
        mom_out, mas_out, low_out = refs[9 + 3 * k:12 + 3 * k]
        old = mas[...]
        new = old - LEARN_RATE * (0.2 * math.sqrt(WIDE) * out[...] + WEIGHT_DECAY * old)
        mom_out[...] = mom[...]
        mas_out[...] = new
        low_out[...] = new.astype(BF16)


def solution(mesh):
    group_size = mesh.shape['data']
    grad_spec = P(('stage', 'data'), None, None, None)
    row_spec = P('stage', 'data', None)

    def step_local(grad_attn, mom_attn, mas_attn, grad_up, mom_up, mas_up, grad_down, mom_down, mas_down):
        vmem = pl.BlockSpec(memory_space=pltpu.VMEM)
        hbm = pl.BlockSpec(memory_space=pl.ANY)
        shapes = ((8, WIDE), (8, NARROW), (SIDE, WIDE))
        sem = pltpu.SemaphoreType.DMA
        scratch = [
            *[pltpu.VMEM(BLOCK, F32)] * 3,
            *[pltpu.VMEM((6,) + (SIDE,) * free + (8, WIDE), F32) for free in (2, 1)],
            pltpu.VMEM((3, CHIP_ROWS, WIDE), F32),
            pltpu.VMEM((CHIP_ROWS, WIDE), F32),
            *[pltpu.VMEM(shape, F32) for shape in shapes * 3],
            *[pltpu.VMEM((WIDE, WIDE), BF16)] * 3,
            pltpu.VMEM((128, NARROW), F32),
            pltpu.VMEM(BLOCK, BF16), pltpu.VMEM((3, SIDE, 2, 8, 128), F32), pltpu.VMEM((1, WIDE), F32),
            *[sem((3, SIDE, 3))] * 3,
            *[sem((3, 3, 6))] * 4,
            *[sem((6,))] * 2,
            sem((2,)),
            *[sem((3, 3))] * 2,
            pltpu.SemaphoreType.REGULAR,
        ]
        result = pl.pallas_call(
            functools.partial(kernel, group_size),
            out_shape=[jax.ShapeDtypeStruct(shape, F32) for shape in shapes * 2],
            in_specs=[hbm] * 6,
            out_specs=[vmem] * 6,
            scratch_shapes=scratch,
            compiler_params=pltpu.CompilerParams(collective_id=0, has_side_effects=True, vmem_limit_bytes=60 * 1024 * 1024),
            name='muon',
        )(grad_attn.reshape(BLOCK), grad_up.reshape(BLOCK[:4] + (NARROW,)), grad_down.reshape(BLOCK[:3] + (8, WIDE)),
          mom_attn[0], mom_up[0], mom_down[0])
        outs = [jax.ShapeDtypeStruct(shape, dtype) for shape in shapes for dtype in (F32, F32, BF16)]
        done = pl.pallas_call(finish, out_shape=outs, in_specs=[vmem] * 9, out_specs=[vmem] * 9, name='finish')(
            *result, mas_attn[0], mas_up[0], mas_down[0])
        return tuple(d[None] for d in done)

    return jax.shard_map(step_local, mesh=mesh, in_specs=(grad_spec, row_spec, row_spec) * 3, out_specs=(row_spec,) * 9,
                         check_vma=False)
```

```python
import functools
import math

import jax
import jax.numpy as jnp
from jax import lax
from jax.experimental import pallas as pl
from jax.experimental.pallas import tpu as pltpu
from jax.sharding import PartitionSpec as P

MOMENTUM = 0.95
LEARN_RATE = 0.25
WEIGHT_DECAY = 0.2
EPSILON = 1e-7
COEF_A = 3.4445
COEF_B = -4.7750
COEF_C = 2.0315
NS_STEPS = 5

F32 = jnp.float32
BF16 = jnp.bfloat16

COLS = ((0, 384), (384, 384), (768, 256))
ORDER = ((0, 1, 2), (1, 2, 0), (2, 0, 1))
ATTN = 1
EXPERT = 0
SIDE = 4
CHIP_ROWS = 16
WIDE = 1024
NARROW = 512
TILE = 256
BLOCK = (SIDE, SIDE, SIDE, CHIP_ROWS, WIDE)
ALL = slice(None)
LO = pl.ds(0, 8)
HI = pl.ds(8, 8)
HALF = (LO, HI)
WEST = pl.ds(0, NARROW)
EAST = pl.ds(NARROW, NARROW)
PIECES = (
    (('up', 0, 384, ALL, 0),),
    (('up', 384, 128, ALL, 384), ('down', 0, TILE, LO, NARROW), ('down', NARROW, TILE, HI, NARROW)),
    (('down', TILE, TILE, LO, 768), ('down', 768, TILE, HI, 768)),
)


def place(ref, fixed, rows, cols):
    return ref.at[region(fixed, rows, cols)]


def region(fixed, rows, cols):
    return tuple(fixed.get(axis, ALL) for axis in range(3)) + (rows, cols)


def coords_of(k):
    return k // (SIDE * SIDE), lax.rem(k // SIDE, SIDE), lax.rem(k, SIDE)


def aligned(start, size):
    return pl.ds(pl.multiple_of(start, size), size)


def kernel(group_size, grad_attn, grad_up, grad_down, mom_attn, mom_up, mom_down,
           mo_attn, mo_up, mo_down, got_attn, got_up, got_down,
           own, peer, full, recv0, recv1, recv2, mom_pk, swap_attn, swap_up, swap_down, keep_attn, keep_up, keep_down,
           send_down, stay_down, out_pk, x_mat, a_mat, b_mat, turn, x_all, norms, scales,
           load_sem, push_sem, pull_sem, rs_send, rs_recv, ag_send, ag_recv, ex_send, ex_recv, back_send, back_recv, stay_sem, keep_sem, norm_send, norm_recv, gate):
    me = lax.axis_index('data')
    core = lax.rem(me, 2)
    chip = me // 2
    pos = coords_of(chip)
    partner = me + 1 - 2 * core
    recvs = (recv0, recv1, recv2)

    def at_axis(axis, coord):
        coords = list(pos)
        coords[axis] = coord
        return ((coords[0] * SIDE + coords[1]) * SIDE + coords[2]) * 2 + core

    right = [lax.rem(p + 1, SIDE) for p in pos]
    left = [lax.rem(p + 3, SIDE) for p in pos]
    far = [lax.rem(p + 2, SIDE) for p in pos]
    right_dev = [at_axis(a, right[a]) for a in range(3)]
    left_dev = [at_axis(a, left[a]) for a in range(3)]
    far_dev = [at_axis(a, far[a]) for a in range(3)]

    def remote(src, dst, send_sem, recv_sem, device):
        return pltpu.make_async_remote_copy(src_ref=src, dst_ref=dst, send_sem=send_sem, recv_sem=recv_sem,
                                            device_id={'data': device}, device_id_type=pl.DeviceIdType.MESH)

    def arrived(part, sem):
        remote(part, part, sem, sem, partner).wait_recv()

    def departed(part, sem):
        remote(part, part, sem, sem, partner).wait_send()

    def turns(color):
        axis = ORDER[color][0]
        return axis, (far[axis], right[axis], left[axis], pos[axis])

    def attn_copy(color, turn_idx, push):
        axis, coords = turns(color)
        cols = pl.ds(*COLS[color])
        src = place(grad_attn, {axis: coords[turn_idx]}, ALL, cols)
        if push:
            dst = place(peer, {axis: coords[turn_idx]}, ALL, cols)
            return remote(src, dst, push_sem, pull_sem.at[color, turn_idx], partner)
        dst = place(own, {axis: coords[turn_idx]}, ALL, cols)
        return pltpu.make_async_copy(src, dst, load_sem.at[color, turn_idx])

    def expert_copies(color, turn_idx, push):
        axis, coords = turns(color)
        copies = []
        for source, col, width, rows, packed in PIECES[color]:
            src = place(grad_up if source == 'up' else grad_down, {axis: coords[turn_idx]}, ALL, pl.ds(col, width))
            target = peer if push else own
            dst = place(target, {axis: coords[turn_idx]}, rows, pl.ds(packed, width))
            if push:
                copies.append(remote(src, dst, push_sem, pull_sem.at[color, turn_idx], partner))
            else:
                copies.append(pltpu.make_async_copy(src, dst, load_sem.at[color, turn_idx]))
        return copies

    def mom_from_attn():
        return [remote(mom_up, swap_up, ex_send.at[0], ex_recv.at[0], partner),
                remote(mom_down, swap_down, ex_send.at[1], ex_recv.at[1], partner)]

    def mom_from_expert():
        return [remote(mom_attn, swap_attn, ex_send.at[0], ex_recv.at[0], partner)]

    def keep_copies(role):
        pairs = ((mom_attn, keep_attn),) if role == ATTN else ((mom_up, keep_up), (mom_down, keep_down))
        return [pltpu.make_async_copy(src, dst, keep_sem.at[k]) for k, (src, dst) in enumerate(pairs)]

    barrier = pltpu.get_barrier_semaphore()
    for device in [partner] + right_dev + left_dev:
        pl.semaphore_signal(barrier, inc=1, device_id={'data': device}, device_id_type=pl.DeviceIdType.MESH)

    @pl.when(core == ATTN)
    def _():
        for turn_idx in range(SIDE):
            for color in range(3):
                attn_copy(color, turn_idx, False).start()
        for copy in keep_copies(ATTN):
            copy.start()

    with jax.named_scope('barrier'):
        pl.semaphore_wait(barrier, 7)

    @pl.when(core == ATTN)
    def _():
        for copy in mom_from_attn():
            copy.start()
        for turn_idx in range(SIDE):
            for color in range(3):
                for copy in expert_copies(color, turn_idx, True):
                    copy.start()

    @pl.when(core == EXPERT)
    def _():
        for turn_idx in range(SIDE):
            for color in range(3):
                attn_copy(color, turn_idx, True).start()
        for copy in mom_from_expert():
            copy.start()
        for copy in keep_copies(EXPERT):
            copy.start()
        for turn_idx in range(SIDE):
            for color in range(3):
                for copy in expert_copies(color, turn_idx, False):
                    copy.start()
        with jax.named_scope('gate'):
            pl.semaphore_wait(gate, 1)

    def open_gate():
        @pl.when(core == ATTN)
        def _():
            pl.semaphore_signal(gate, inc=1, device_id={'data': partner}, device_id_type=pl.DeviceIdType.MESH)

    def chip_sum(color, turn_idx):
        axis, coords = turns(color)
        idx = region({axis: coords[turn_idx]}, ALL, pl.ds(*COLS[color]))
        pltpu.make_async_copy(own.at[idx], own.at[idx], load_sem.at[color, turn_idx]).wait()
        arrived(peer.at[idx], pull_sem.at[color, turn_idx])
        own[idx] = own[idx] + peer[idx]

    PAIRED = ((far, 0, right_dev), (far, 1, left_dev), (right, 1, right_dev), (left, 0, left_dev), (right, 0, right_dev), (left, 1, left_dev))
    DIRECT = ((far, far_dev), (right, right_dev), (left, left_dev))

    def ctx(phase, color):
        order = ORDER[color]
        return order[phase], {order[k]: pos[order[k]] for k in range(phase)}, pl.ds(*COLS[color])

    def rs_slot(phase, color, piece):
        return (piece,) + (ALL,) * (2 - phase) + (ALL, pl.ds(*COLS[color]))

    def rs_copy(phase, color, piece):
        axis, fixed, cols = ctx(phase, color)
        if phase < 2:
            coord, half, device = PAIRED[piece]
            rows = HALF[half]
        else:
            coord, device = DIRECT[piece]
            rows = ALL
        src = place(own, {**fixed, axis: coord[axis]}, rows, cols)
        return remote(src, recvs[phase].at[rs_slot(phase, color, piece)], rs_send.at[phase], recv_sem(rs_recv, phase, color, piece),
                      device[axis])

    def recv_sem(sems, phase, color, piece):
        return sems.at[phase, color, min(piece, 2) if phase < 2 else 0]

    def rs_arrive(phase, color, pieces):
        first = pieces[0]
        slot = rs_slot(phase, color, pl.ds(first, len(pieces)))
        arrived(recvs[phase].at[slot], recv_sem(rs_recv, phase, color, first))

    def rs_add(phase, color, coord, rows, pieces):
        axis, fixed, cols = ctx(phase, color)
        idx = region({**fixed, axis: coord[axis]}, rows, cols)
        total = own[idx]
        for piece in pieces:
            total = total + recvs[phase][rs_slot(phase, color, piece)]
        own[idx] = total

    def rs_mid(phase, color):
        rs_arrive(phase, color, (0,))
        rs_add(phase, color, right, LO, (0,))
        rs_copy(phase, color, 4).start()
        rs_arrive(phase, color, (1,))
        rs_add(phase, color, left, HI, (1,))
        rs_copy(phase, color, 5).start()

    def rs_end(phase, color):
        rs_arrive(phase, color, (2, 3, 4, 5))
        rs_add(phase, color, pos, LO, (3, 4))
        rs_add(phase, color, pos, HI, (2, 5))

    with jax.named_scope('rs0_load'):
        for color in range(3):
            chip_sum(color, 0)
            rs_copy(0, color, 0).start()
            rs_copy(0, color, 1).start()
        open_gate()
        for turn_idx in (1, 2):
            for color in range(3):
                chip_sum(color, turn_idx)
                rs_copy(0, color, turn_idx + 1).start()
    with jax.named_scope('rs0_mid'):
        for color in range(3):
            rs_mid(0, color)
        for color in range(3):
            chip_sum(color, 3)
    with jax.named_scope('rs0_end'):
        for color in range(3):
            rs_end(0, color)
            for piece in range(4):
                rs_copy(1, color, piece).start()
    with jax.named_scope('rs1_mid'):
        for color in range(3):
            rs_mid(1, color)
    with jax.named_scope('rs1_end'):
        for color in range(3):
            rs_end(1, color)
            for piece in range(3):
                rs_copy(2, color, piece).start()
    with jax.named_scope('rs2'):
        for color in range(3):
            rs_arrive(2, color, (0, 1, 2))
            rs_add(2, color, pos, ALL, range(3))

    @pl.when(core == ATTN)
    def _():
        mom_from_expert()[0].wait_recv()
        keep_copies(ATTN)[0].wait()
        mom_pk[LO] = swap_attn[...]
        mom_pk[HI] = keep_attn[...]

    @pl.when(core == EXPERT)
    def _():
        for copy in mom_from_attn():
            copy.wait_recv()
        for copy in keep_copies(EXPERT):
            copy.wait()
        mom_pk[LO, WEST] = keep_up[...]
        mom_pk[HI, WEST] = swap_up[...]
        for first, cols in ((0, WEST), (8, EAST)):
            mom_pk[pl.ds(first, SIDE), EAST] = keep_down[:, cols]
            mom_pk[pl.ds(first + SIDE, SIDE), EAST] = swap_down[:, cols]

    mine = pos
    mom_new = MOMENTUM * mom_pk[...] + own[mine] * (1.0 / group_size)
    full[mine] = mom_new

    AG_SEND = ((pos, 0, right_dev), (pos, 1, left_dev), (pos, 1, right_dev), (pos, 0, left_dev), (left, 0, right_dev), (right, 1, left_dev))
    AG_LAND = ((left, 0), (right, 1), (left, 1), (right, 0), (far, 0), (far, 1))
    AG_DIRECT = (far, left, right)

    def ag_part(phase, color, coord, rows):
        axis, fixed, cols = ctx(phase, color)
        return place(full, {**fixed, axis: coord[axis]}, rows, cols)

    def ag_half(phase, color, coord, half):
        if phase == 1:
            return ag_part(phase, color, coord, HALF[half])
        axis, second, _ = ORDER[color]
        return place(x_all, {axis: coord[axis], second: pl.ds(2 * half, 2)}, ALL, pl.ds(*COLS[color]))

    def ag_remote(part, phase, color, piece, device):
        return remote(part, part, ag_send.at[phase], recv_sem(ag_recv, phase, color, piece), device[ORDER[color][phase]])

    def ag_copy(phase, color, piece):
        if phase < 2:
            coord, half, device = AG_SEND[piece]
            return ag_remote(ag_half(phase, color, coord, half), phase, color, piece, device)
        return ag_remote(ag_part(phase, color, pos, ALL), phase, color, piece, DIRECT[piece][1])

    def ag_arrive(phase, color, piece):
        sem = recv_sem(ag_recv, phase, color, piece)
        if phase == 2:
            arrived(ag_part(phase, color, [pl.ds(0, 3)] * 3, ALL), sem)
        elif piece < 2:
            coord, half = AG_LAND[piece]
            arrived(ag_half(phase, color, coord, half), sem)
        elif phase == 1:
            arrived(ag_part(phase, color, [pl.ds(0, 2)] * 3, ALL), sem)
        else:
            arrived(place(x_all, {ORDER[color][0]: pl.ds(0, 2)}, ALL, pl.ds(*COLS[color])), sem)

    def drain_push():
        departed(peer, push_sem)

        @pl.when(core == ATTN)
        def _():
            for copy in mom_from_attn():
                copy.wait_send()

        @pl.when(core == EXPERT)
        def _():
            for copy in mom_from_expert():
                copy.wait_send()

    with jax.named_scope('ag2'):
        for color in range(3):
            for piece in range(3):
                ag_copy(2, color, piece).start()
        drain_push()
        for color in range(3):
            ag_arrive(2, color, 0)
            for piece in range(4):
                ag_copy(1, color, piece).start()
    def rs_drain(phase):
        departed(recvs[phase], rs_send.at[phase])

    def ag_drain(phase):
        departed((x_all.at[pl.ds(0, 3)], full.at[0, pl.ds(0, 3)], full.at[0, 0, pl.ds(0, 3)])[phase], ag_send.at[phase])

    def ag_mid(phase):
        for color in range(3):
            ag_arrive(phase, color, 0)
            ag_copy(phase, color, 4).start()
            ag_arrive(phase, color, 1)
            ag_copy(phase, color, 5).start()

    def norm_copy(level, color, piece):
        axis = ORDER[color][level]
        part = norms.at[level, color, pos[axis]]
        return remote(part, part, norm_send.at[level], norm_recv.at[level, color], DIRECT[piece][1][axis])

    def norm_sum(level, color):
        arrived(norms.at[level, color, pl.ds(0, 3)], norm_recv.at[level, color])
        return sum(norms[level, color, j] for j in range(SIDE))

    def norm_send_all(level, color):
        for piece in range(3):
            norm_copy(level, color, piece).start()

    def square_tile(line, cols):
        val = full[line + (ALL, cols)].reshape(8, 8, cols.size)
        val = jnp.sum(val * val, axis=0)
        return sum(val[:, k:k + 128] for k in range(0, cols.size, 128))

    def norm_start(color):
        first_axis, second_axis, _ = ORDER[color]
        line = region({first_axis: pos[first_axis], second_axis: pos[second_axis]}, ALL, ALL)[:3]
        first, width = COLS[color]
        west = max(0, min(NARROW - first, width))
        for side, (start, size) in enumerate(((first, west), (first + west, width - west))):
            val = square_tile(line, pl.ds(start, size)) if size else jnp.zeros((8, 128), F32)
            norms[1, color, pos[second_axis], side] = val
        norm_send_all(1, color)

    def result_copies(role, which):
        if role == ATTN:
            source = (full.at[mine], out_pk)[which]
            pairs = ((source.at[HI], source.at[LO], (mo_attn, got_attn)[which]),)
        else:
            first = pl.multiple_of(lax.rem(chip, 8) * CHIP_ROWS, CHIP_ROWS)
            ups = ((full.at[mine + (LO, WEST)], full.at[mine + (HI, WEST)]), (turn.at[pl.ds(first, 8)], turn.at[pl.ds(first + 8, 8)]))[which]
            pairs = (ups + ((mo_up, got_up)[which],), (stay_down.at[which], send_down.at[which], (mo_down, got_down)[which]))
        stay = [pltpu.make_async_copy(pair[0], pair[2], stay_sem.at[which, k]) for k, pair in enumerate(pairs)]
        away = [remote(pair[1], pair[2], back_send.at[which, k], back_recv.at[which, k], partner) for k, pair in enumerate(pairs)]
        return stay, away

    def result_start(role, which):
        stay, away = result_copies(role, which)
        for copy in away + stay:
            copy.start()

    with jax.named_scope('ag1_start'):
        for color in range(3):
            norm_start(color)

        @pl.when(core == ATTN)
        def _():
            result_start(ATTN, 0)

        @pl.when(core == EXPERT)
        def _():
            for rows, cols in ((LO, WEST), (HI, EAST)):
                down = full[mine + (rows, EAST)]
                send_down[0, :, cols] = down[SIDE:]
                stay_down[0, :, cols] = down[:SIDE]
            result_start(EXPERT, 0)
        rs_drain(1)
        ag_drain(2)
    with jax.named_scope('ag1_mid'):
        ag_mid(1)
        for color in range(3):
            norms[0, color, pos[ORDER[color][0]]] = norm_sum(1, color)
            norm_send_all(0, color)
        rs_drain(0)
        rs_drain(2)
    with jax.named_scope('ag1_end'):
        for color in range(3):
            ag_arrive(1, color, 2)
    with jax.named_scope('norm'):
        total = jnp.sum(norm_sum(0, 0) + norm_sum(0, 1) + norm_sum(0, 2), axis=(1, 2), keepdims=True)
        west, east = total[0], total[1]
        both = west + east
        west = jnp.where(core == ATTN, both, west)
        east = jnp.where(core == ATTN, both, east)
        lane = lax.broadcasted_iota(jnp.int32, (1, WIDE), 1)
        norm = jnp.sqrt(jnp.where(lane < NARROW, west, east))
        scales[...] = 1.0 / (norm + EPSILON)
    with jax.named_scope('ag0_start'):
        for color in range(3):
            axis, cols = ORDER[color][0], pl.ds(*COLS[color])
            idx = region({axis: pos[axis]}, ALL, cols)
            x_all[idx] = (full[idx] * scales[:, cols]).astype(BF16)
            for piece in range(4):
                ag_copy(0, color, piece).start()
    with jax.named_scope('ag0_mid'):
        ag_mid(0)
    with jax.named_scope('ag0_end'):
        for color in range(3):
            ag_arrive(0, color, 2)
    for level in range(2):
        departed(norms.at[level, :, pl.ds(0, 3)], norm_send.at[level])
    ag_drain(1)
    ag_drain(0)

    def weighted(a_val, q_val):
        return (COEF_B * a_val.astype(F32) + COEF_C * q_val.astype(BF16).astype(F32)).astype(BF16)

    def advance(x_val, y_val):
        return (COEF_A * x_val.astype(F32) + y_val.astype(BF16).astype(F32)).astype(BF16)

    def symmetric(out, base, size, block):
        for j in range(0, size, TILE):
            val = block(j)
            out[pl.ds(base + j, size - j), pl.ds(j, TILE)] = val
            if j + TILE < size:
                out[pl.ds(base + j, TILE), pl.ds(j + TILE, size - j - TILE)] = jnp.transpose(val[TILE:])

    def gram(base, size):
        def block(j):
            return lax.dot_general(x_mat[pl.ds(base + j, size - j), :], x_mat[pl.ds(base + j, TILE), :], (((1,), (1,)), ((), ())),
                                   preferred_element_type=F32).astype(BF16)
        symmetric(a_mat, base, size, block)

    def poly(base, size):
        def block(j):
            rows, cols = pl.ds(base + j, size - j), pl.ds(j, TILE)
            q_val = jnp.dot(a_mat[rows, pl.ds(0, size)], a_mat[pl.ds(base, size), cols], preferred_element_type=F32)
            return weighted(a_mat[rows, cols], q_val)
        symmetric(b_mat, base, size, block)

    def update(base, size):
        rows = pl.ds(base, size)
        y_val = jnp.dot(b_mat[rows, pl.ds(0, size)], x_mat[rows, :], preferred_element_type=F32)
        x_mat[rows, :] = advance(x_mat[rows, :], y_val)

    @pl.when(core == ATTN)
    def _():
        with jax.named_scope('fill'):
            x_mat[...] = x_all[...].reshape(WIDE, WIDE)

        def step(_, carry):
            gram(0, WIDE)
            poly(0, WIDE)
            update(0, WIDE)
            return carry
        with jax.named_scope('steps'):
            lax.fori_loop(0, NS_STEPS - 1, step, 0)
            gram(0, WIDE)
        with jax.named_scope('last'):
            rows = aligned(chip * CHIP_ROWS, CHIP_ROWS)
            a_val = a_mat[rows, :]
            b_val = weighted(a_val, jnp.dot(a_val, a_mat[...], preferred_element_type=F32))
            out = advance(x_mat[rows, :], jnp.dot(b_val, x_mat[...], preferred_element_type=F32)).astype(F32)
            out_pk[...] = out
            result_start(ATTN, 1)

    @pl.when(core == EXPERT)
    def _():
        with jax.named_scope('fill'):
            def fill_up(k, carry):
                val = x_all[k // 2, pl.ds(2 * lax.rem(k, 2), 2), :, :, WEST].reshape(128, NARROW)
                x_mat[WEST, aligned(k * 128, 128)] = jnp.transpose(val)
                return carry
            lax.fori_loop(0, 8, fill_up, 0)

            def fill_down(k, carry):
                z, y, x = coords_of(2 * k)
                val = x_all[z, y, pl.ds(x, 2), :, EAST].astype(F32)
                rows = aligned(NARROW + k * CHIP_ROWS, CHIP_ROWS)
                x_mat[rows, WEST] = val[:, :8].reshape(CHIP_ROWS, NARROW).astype(BF16)
                x_mat[rows, EAST] = val[:, 8:].reshape(CHIP_ROWS, NARROW).astype(BF16)
                return carry
            lax.fori_loop(0, 32, fill_down, 0)

        def step(_, carry):
            for stage in (gram, poly, update):
                stage(0, NARROW)
                stage(NARROW, NARROW)
            return carry
        with jax.named_scope('steps'):
            lax.fori_loop(0, NS_STEPS - 1, step, 0)
            gram(0, NARROW)
            gram(NARROW, NARROW)
        with jax.named_scope('last'):
            poly(0, NARROW)
            cols = aligned(chip // 8 * 128, 128)
            out_up = advance(x_mat[WEST, cols], jnp.dot(b_mat[WEST, WEST], x_mat[WEST, cols], preferred_element_type=F32))
            turn[...] = jnp.transpose(out_up.astype(F32))
            rows = aligned(NARROW + chip // 2 * CHIP_ROWS, CHIP_ROWS)
            a_val = a_mat[rows, WEST]
            b_val = weighted(a_val, jnp.dot(a_val, a_mat[EAST, WEST], preferred_element_type=F32))
            both = advance(x_mat[rows, :], jnp.dot(b_val, x_mat[EAST, :], preferred_element_type=F32)).astype(F32)
            out_down = jnp.where(lax.rem(chip, 2) == 0, both[:8], both[8:])
            send_down[1] = out_down[SIDE:]
            stay_down[1] = out_down[:SIDE]
            result_start(EXPERT, 1)

    with jax.named_scope('swap'):
        for role, other in ((ATTN, EXPERT), (EXPERT, ATTN)):
            @pl.when(core == role)
            def _(role=role, other=other):
                for which in range(2):
                    stay, away = result_copies(role, which)
                    for copy in stay:
                        copy.wait()
                    for copy in away:
                        copy.wait_send()
                    for copy in result_copies(other, which)[1]:
                        copy.wait_recv()


def finish(*refs):
    for k in range(3):
        mom, out, mas = refs[k], refs[3 + k], refs[6 + k]
        mom_out, mas_out, low_out = refs[9 + 3 * k:12 + 3 * k]
        old = mas[...]
        new = old - LEARN_RATE * (0.2 * math.sqrt(WIDE) * out[...] + WEIGHT_DECAY * old)
        mom_out[...] = mom[...]
        mas_out[...] = new
        low_out[...] = new.astype(BF16)


def solution(mesh):
    group_size = mesh.shape['data']
    grad_spec = P(('stage', 'data'), None, None, None)
    row_spec = P('stage', 'data', None)

    def step_local(grad_attn, mom_attn, mas_attn, grad_up, mom_up, mas_up, grad_down, mom_down, mas_down):
        vmem = pl.BlockSpec(memory_space=pltpu.VMEM)
        hbm = pl.BlockSpec(memory_space=pl.ANY)
        shapes = ((8, WIDE), (8, NARROW), (SIDE, WIDE))
        sem = pltpu.SemaphoreType.DMA
        scratch = [
            *[pltpu.VMEM(BLOCK, F32)] * 3,
            *[pltpu.VMEM((6,) + (SIDE,) * free + (8, WIDE), F32) for free in (2, 1)],
            pltpu.VMEM((3, CHIP_ROWS, WIDE), F32),
            pltpu.VMEM((CHIP_ROWS, WIDE), F32),
            *[pltpu.VMEM(shape, F32) for shape in shapes * 2],
            *[pltpu.VMEM((2, SIDE, WIDE), F32)] * 2,
            pltpu.VMEM((CHIP_ROWS, WIDE), F32),
            *[pltpu.VMEM((WIDE, WIDE), BF16)] * 3,
            pltpu.VMEM((128, NARROW), F32),
            pltpu.VMEM(BLOCK, BF16), pltpu.VMEM((2, 3, SIDE, 2, 8, 128), F32), pltpu.VMEM((1, WIDE), F32),
            sem((3, SIDE)), sem, sem((3, SIDE)),
            sem((3,)), sem((3, 3, 3)), sem((3,)), sem((3, 3, 3)),
            *[sem((2,))] * 2,
            *[sem((2, 2))] * 3,
            sem((2,)),
            sem((2,)), sem((2, 3)),
            pltpu.SemaphoreType.REGULAR,
        ]
        result = pl.pallas_call(
            functools.partial(kernel, group_size),
            out_shape=[jax.ShapeDtypeStruct(shape, F32) for shape in shapes * 2],
            in_specs=[hbm] * 6,
            out_specs=[hbm] * 6,
            scratch_shapes=scratch,
            compiler_params=pltpu.CompilerParams(collective_id=0, has_side_effects=True, vmem_limit_bytes=60 * 1024 * 1024),
            name='muon',
        )(grad_attn.reshape(BLOCK), grad_up.reshape(BLOCK[:4] + (NARROW,)), grad_down.reshape(BLOCK[:3] + (8, WIDE)),
          mom_attn[0], mom_up[0], mom_down[0])
        outs = [jax.ShapeDtypeStruct(shape, dtype) for shape in shapes for dtype in (F32, F32, BF16)]
        done = pl.pallas_call(finish, out_shape=outs, in_specs=[vmem] * 9, out_specs=[vmem] * 9, name='finish')(
            *result, mas_attn[0], mas_up[0], mas_down[0])
        return tuple(d[None] for d in done)

    return jax.shard_map(step_local, mesh=mesh, in_specs=(grad_spec, row_spec, row_spec) * 3, out_specs=(row_spec,) * 9,
                         check_vma=False)
```

```python
import functools
import math

import jax
import jax.numpy as jnp
from jax import lax
from jax.experimental import pallas as pl
from jax.experimental.pallas import tpu as pltpu
from jax.sharding import PartitionSpec as P

MOMENTUM = 0.95
LEARN_RATE = 0.25
WEIGHT_DECAY = 0.2
EPSILON = 1e-7
COEF_A = 3.4445
COEF_B = -4.7750
COEF_C = 2.0315
NS_STEPS = 5

F32 = jnp.float32
BF16 = jnp.bfloat16

COLS = ((0, 384), (384, 384), (768, 256))
ORDER = ((0, 1, 2), (1, 2, 0), (2, 0, 1))
ATTN = 1
EXPERT = 0
SIDE = 4
CHIP_ROWS = 16
WIDE = 1024
NARROW = 512
TILE = 256
BLOCK = (SIDE, SIDE, SIDE, CHIP_ROWS, WIDE)
ALL = slice(None)
LO = pl.ds(0, 8)
HI = pl.ds(8, 8)
HALF = (LO, HI)
WEST = pl.ds(0, NARROW)
EAST = pl.ds(NARROW, NARROW)
PIECES = (
    (('up', 0, 384, ALL, 0),),
    (('up', 384, 128, ALL, 384), ('down', 0, TILE, LO, NARROW), ('down', NARROW, TILE, HI, NARROW)),
    (('down', TILE, TILE, LO, 768), ('down', 768, TILE, HI, 768)),
)


def place(ref, fixed, rows, cols):
    return ref.at[region(fixed, rows, cols)]


def region(fixed, rows, cols):
    return tuple(fixed.get(axis, ALL) for axis in range(3)) + (rows, cols)


def coords_of(k):
    return k // (SIDE * SIDE), lax.rem(k // SIDE, SIDE), lax.rem(k, SIDE)


def aligned(start, size):
    return pl.ds(pl.multiple_of(start, size), size)


def kernel(group_size, grad_attn, grad_up, grad_down, mom_attn, mom_up, mom_down,
           mo_attn, mo_up, mo_down, got_attn, got_up, got_down,
           own, peer, full, recv0, recv1, recv2, mom_pk, swap_attn, swap_up, swap_down, keep_attn, keep_up, keep_down,
           send_down, stay_down, out_pk, x_mat, a_mat, b_mat, turn, x_all, norms, scales,
           load_sem, push_sem, pull_sem, rs_send, rs_recv, ag_send, ag_recv, ex_send, ex_recv, back_send, back_recv, stay_sem, keep_sem, norm_send, norm_recv, gate):
    me = lax.axis_index('data')
    core = lax.rem(me, 2)
    chip = me // 2
    pos = coords_of(chip)
    partner = me + 1 - 2 * core
    recvs = (recv0, recv1, recv2)

    def at_axis(axis, coord):
        coords = list(pos)
        coords[axis] = coord
        return ((coords[0] * SIDE + coords[1]) * SIDE + coords[2]) * 2 + core

    right = [lax.rem(p + 1, SIDE) for p in pos]
    left = [lax.rem(p + 3, SIDE) for p in pos]
    far = [lax.rem(p + 2, SIDE) for p in pos]
    right_dev = [at_axis(a, right[a]) for a in range(3)]
    left_dev = [at_axis(a, left[a]) for a in range(3)]
    far_dev = [at_axis(a, far[a]) for a in range(3)]

    def remote(src, dst, send_sem, recv_sem, device):
        return pltpu.make_async_remote_copy(src_ref=src, dst_ref=dst, send_sem=send_sem, recv_sem=recv_sem,
                                            device_id={'data': device}, device_id_type=pl.DeviceIdType.MESH)

    def arrived(part, sem):
        remote(part, part, sem, sem, partner).wait_recv()

    def departed(part, sem):
        remote(part, part, sem, sem, partner).wait_send()

    def turns(color):
        axis = ORDER[color][0]
        return axis, (far[axis], right[axis], left[axis], pos[axis])

    PARTS = ((0, 0), (0, 1), (1, None), (2, None), (3, None))

    def attn_copy(color, part, push):
        turn_idx, half = PARTS[part]
        rows = ALL if half is None else HALF[half]
        axis, coords = turns(color)
        cols = pl.ds(*COLS[color])
        src = place(grad_attn, {axis: coords[turn_idx]}, rows, cols)
        if push:
            dst = place(peer, {axis: coords[turn_idx]}, rows, cols)
            return remote(src, dst, push_sem, pull_sem.at[color, part], partner)
        dst = place(own, {axis: coords[turn_idx]}, rows, cols)
        return pltpu.make_async_copy(src, dst, load_sem.at[color, part])

    def expert_copies(color, part, push):
        turn_idx, half = PARTS[part]
        axis, coords = turns(color)
        copies = []
        for source, col, width, rows, packed in PIECES[color]:
            from_rows = ALL
            if half is not None and source == 'up':
                from_rows = rows = HALF[half]
            elif half is not None and rows is not HALF[half]:
                continue
            src = place(grad_up if source == 'up' else grad_down, {axis: coords[turn_idx]}, from_rows, pl.ds(col, width))
            target = peer if push else own
            dst = place(target, {axis: coords[turn_idx]}, rows, pl.ds(packed, width))
            if push:
                copies.append(remote(src, dst, push_sem, pull_sem.at[color, part], partner))
            else:
                copies.append(pltpu.make_async_copy(src, dst, load_sem.at[color, part]))
        return copies

    def mom_from_attn():
        return [remote(mom_up, swap_up, ex_send.at[0], ex_recv.at[0], partner),
                remote(mom_down, swap_down, ex_send.at[1], ex_recv.at[1], partner)]

    def mom_from_expert():
        return [remote(mom_attn, swap_attn, ex_send.at[0], ex_recv.at[0], partner)]

    def keep_copies(role):
        pairs = ((mom_attn, keep_attn),) if role == ATTN else ((mom_up, keep_up), (mom_down, keep_down))
        return [pltpu.make_async_copy(src, dst, keep_sem.at[k]) for k, (src, dst) in enumerate(pairs)]

    barrier = pltpu.get_barrier_semaphore()
    for device in [partner] + right_dev + left_dev:
        pl.semaphore_signal(barrier, inc=1, device_id={'data': device}, device_id_type=pl.DeviceIdType.MESH)

    @pl.when(core == ATTN)
    def _():
        for part in range(len(PARTS)):
            for color in range(3):
                attn_copy(color, part, False).start()
        for copy in keep_copies(ATTN):
            copy.start()

    with jax.named_scope('barrier'):
        pl.semaphore_wait(barrier, 7)

    @pl.when(core == ATTN)
    def _():
        for copy in mom_from_attn():
            copy.start()
        for part in range(len(PARTS)):
            for color in range(3):
                for copy in expert_copies(color, part, True):
                    copy.start()

    @pl.when(core == EXPERT)
    def _():
        for part in range(len(PARTS)):
            for color in range(3):
                attn_copy(color, part, True).start()
        for copy in mom_from_expert():
            copy.start()
        for copy in keep_copies(EXPERT):
            copy.start()
        for part in range(len(PARTS)):
            for color in range(3):
                for copy in expert_copies(color, part, False):
                    copy.start()
        with jax.named_scope('gate'):
            pl.semaphore_wait(gate, 1)

    def open_gate():
        @pl.when(core == ATTN)
        def _():
            pl.semaphore_signal(gate, inc=1, device_id={'data': partner}, device_id_type=pl.DeviceIdType.MESH)

    def chip_sum(color, part):
        axis, coords = turns(color)
        turn_idx, half = PARTS[part]
        idx = region({axis: coords[turn_idx]}, ALL if half is None else HALF[half], pl.ds(*COLS[color]))
        pltpu.make_async_copy(own.at[idx], own.at[idx], load_sem.at[color, part]).wait()
        arrived(peer.at[idx], pull_sem.at[color, part])
        own[idx] = own[idx] + peer[idx]

    PAIRED = ((far, 0, right_dev), (far, 1, left_dev), (right, 1, right_dev), (left, 0, left_dev), (right, 0, right_dev), (left, 1, left_dev))
    DIRECT = ((far, far_dev), (right, right_dev), (left, left_dev))

    def ctx(phase, color):
        order = ORDER[color]
        return order[phase], {order[k]: pos[order[k]] for k in range(phase)}, pl.ds(*COLS[color])

    def rs_slot(phase, color, piece, sub=None):
        free = [ALL] * (2 - phase)
        if sub is not None:
            free[0] = pl.ds(2 * sub, 2)
        return (piece, *free, ALL, pl.ds(*COLS[color]))

    def recv_sem(sems, phase, color, piece, sub):
        return sems.at[phase, color, 4 if phase == 2 or piece > 1 else 2 * piece + (sub or 0)]

    def rs_region(phase, color, coord, rows, sub):
        axis, fixed, cols = ctx(phase, color)
        fixed = {**fixed, axis: coord[axis]}
        if sub is not None:
            fixed[min(k for k in range(3) if k != axis)] = pl.ds(2 * sub, 2)
        return region(fixed, rows, cols)

    def rs_copy(phase, color, piece, sub=None):
        if phase < 2:
            coord, half, device = PAIRED[piece]
            rows = HALF[half]
        else:
            coord, device = DIRECT[piece]
            rows = ALL
        return remote(own.at[rs_region(phase, color, coord, rows, sub)], recvs[phase].at[rs_slot(phase, color, piece, sub)],
                      rs_send.at[phase], recv_sem(rs_recv, phase, color, piece, sub), device[ORDER[color][phase]])

    def rs_arrive(phase, color, pieces, sub=None):
        first = pieces[0]
        slot = rs_slot(phase, color, pl.ds(first, len(pieces)), sub)
        arrived(recvs[phase].at[slot], recv_sem(rs_recv, phase, color, first, sub))

    def rs_add(phase, color, coord, rows, pieces, sub=None):
        idx = rs_region(phase, color, coord, rows, sub)
        total = own[idx]
        for piece in pieces:
            total = total + recvs[phase][rs_slot(phase, color, piece, sub)]
        own[idx] = total

    def rs_mid(phase, color, sub=None):
        rs_arrive(phase, color, (0,), sub)
        rs_add(phase, color, right, LO, (0,), sub)
        rs_copy(phase, color, 4, sub).start()
        rs_arrive(phase, color, (1,), sub)
        rs_add(phase, color, left, HI, (1,), sub)
        rs_copy(phase, color, 5, sub).start()

    def rs_end(phase, color):
        rs_arrive(phase, color, (2, 3, 4, 5))
        rs_add(phase, color, pos, LO, (3, 4))
        rs_add(phase, color, pos, HI, (2, 5))

    with jax.named_scope('rs0_load'):
        for half in range(2):
            for color in range(3):
                chip_sum(color, half)
                for sub in range(2):
                    rs_copy(0, color, half, sub).start()
        for part in (2, 3):
            for color in range(3):
                chip_sum(color, part)
                rs_copy(0, color, part).start()
    with jax.named_scope('rs0_mid'):
        for sub in range(2):
            for color in range(3):
                rs_mid(0, color, sub)
        open_gate()
        for color in range(3):
            chip_sum(color, 4)
    with jax.named_scope('rs0_end'):
        for color in range(3):
            rs_end(0, color)
            for piece in range(4):
                rs_copy(1, color, piece).start()
    with jax.named_scope('rs1_mid'):
        for color in range(3):
            rs_mid(1, color)
    with jax.named_scope('rs1_end'):
        for color in range(3):
            rs_end(1, color)
            for piece in range(3):
                rs_copy(2, color, piece).start()
    with jax.named_scope('rs2'):
        for color in range(3):
            rs_arrive(2, color, (0, 1, 2))
            rs_add(2, color, pos, ALL, range(3))

    @pl.when(core == ATTN)
    def _():
        mom_from_expert()[0].wait_recv()
        keep_copies(ATTN)[0].wait()
        mom_pk[LO] = swap_attn[...]
        mom_pk[HI] = keep_attn[...]

    @pl.when(core == EXPERT)
    def _():
        for copy in mom_from_attn():
            copy.wait_recv()
        for copy in keep_copies(EXPERT):
            copy.wait()
        mom_pk[LO, WEST] = keep_up[...]
        mom_pk[HI, WEST] = swap_up[...]
        for first, cols in ((0, WEST), (8, EAST)):
            mom_pk[pl.ds(first, SIDE), EAST] = keep_down[:, cols]
            mom_pk[pl.ds(first + SIDE, SIDE), EAST] = swap_down[:, cols]

    mine = pos
    mom_new = MOMENTUM * mom_pk[...] + own[mine] * (1.0 / group_size)
    full[mine] = mom_new

    AG_SEND = ((pos, 0, right_dev), (pos, 1, left_dev), (pos, 1, right_dev), (pos, 0, left_dev), (left, 0, right_dev), (right, 1, left_dev))
    AG_LAND = ((left, 0), (right, 1), (left, 1), (right, 0), (far, 0), (far, 1))
    AG_DIRECT = (far, left, right)

    def ag_part(phase, color, coord, rows):
        axis, fixed, cols = ctx(phase, color)
        return place(full, {**fixed, axis: coord[axis]}, rows, cols)

    def ag_half(phase, color, coord, half, sub=None):
        if phase == 1:
            return ag_part(phase, color, coord, HALF[half])
        axis, second, _ = ORDER[color]
        span = pl.ds(2 * half, 2) if sub is None else pl.ds(2 * half + sub, 1)
        return place(x_all, {axis: coord[axis], second: span}, ALL, pl.ds(*COLS[color]))

    def ag_remote(part, phase, color, piece, device, sub=None):
        return remote(part, part, ag_send.at[phase], recv_sem(ag_recv, phase, color, piece, sub), device[ORDER[color][phase]])

    def ag_copy(phase, color, piece, sub=None):
        if phase < 2:
            coord, half, device = AG_SEND[piece]
            return ag_remote(ag_half(phase, color, coord, half, sub), phase, color, piece, device, sub)
        return ag_remote(ag_part(phase, color, pos, ALL), phase, color, piece, DIRECT[piece][1])

    def ag_arrive(phase, color, piece, sub=None):
        sem = recv_sem(ag_recv, phase, color, piece, sub)
        if phase == 2:
            arrived(ag_part(phase, color, [pl.ds(0, 3)] * 3, ALL), sem)
        elif piece < 2:
            coord, half = AG_LAND[piece]
            arrived(ag_half(phase, color, coord, half, sub), sem)
        elif phase == 1:
            arrived(ag_part(phase, color, [pl.ds(0, 2)] * 3, ALL), sem)
        else:
            arrived(place(x_all, {ORDER[color][0]: pl.ds(0, 2)}, ALL, pl.ds(*COLS[color])), sem)

    def drain_push():
        departed(peer, push_sem)

        @pl.when(core == ATTN)
        def _():
            for copy in mom_from_attn():
                copy.wait_send()

        @pl.when(core == EXPERT)
        def _():
            for copy in mom_from_expert():
                copy.wait_send()

    def rs_drain(phase):
        departed(recvs[phase], rs_send.at[phase])

    def ag_drain(phase):
        departed((x_all.at[pl.ds(0, 3)], full.at[0, pl.ds(0, 3)], full.at[0, 0, pl.ds(0, 3)])[phase], ag_send.at[phase])

    def ag_mid(phase, sub=None):
        for color in range(3):
            for piece in range(2):
                ag_arrive(phase, color, piece, sub)
                ag_copy(phase, color, piece + 4, sub).start()

    def norm_copy(level, color, piece):
        axis = ORDER[color][level]
        part = norms.at[level, color, pos[axis]]
        return remote(part, part, norm_send.at[level], norm_recv.at[level, color], DIRECT[piece][1][axis])

    def norm_sum(level, color):
        arrived(norms.at[level, color, pl.ds(0, 3)], norm_recv.at[level, color])
        return sum(norms[level, color, j] for j in range(SIDE))

    def norm_send_all(level, color):
        for piece in range(3):
            norm_copy(level, color, piece).start()

    def square_tile(line, cols):
        val = full[line + (ALL, cols)].reshape(8, 8, cols.size)
        val = jnp.sum(val * val, axis=0)
        return sum(val[:, k:k + 128] for k in range(0, cols.size, 128))

    def norm_start(color):
        first_axis, second_axis, _ = ORDER[color]
        line = region({first_axis: pos[first_axis], second_axis: pos[second_axis]}, ALL, ALL)[:3]
        first, width = COLS[color]
        west = max(0, min(NARROW - first, width))
        for side, (start, size) in enumerate(((first, west), (first + west, width - west))):
            val = square_tile(line, pl.ds(start, size)) if size else jnp.zeros((8, 128), F32)
            norms[1, color, pos[second_axis], side] = val
        norm_send_all(1, color)

    def result_copies(role, which):
        if role == ATTN:
            source = (full.at[mine], out_pk)[which]
            pairs = ((source.at[HI], source.at[LO], (mo_attn, got_attn)[which]),)
        else:
            first = pl.multiple_of(lax.rem(chip, 8) * CHIP_ROWS, CHIP_ROWS)
            ups = ((full.at[mine + (LO, WEST)], full.at[mine + (HI, WEST)]), (turn.at[pl.ds(first, 8)], turn.at[pl.ds(first + 8, 8)]))[which]
            pairs = (ups + ((mo_up, got_up)[which],), (stay_down.at[which], send_down.at[which], (mo_down, got_down)[which]))
        stay = [pltpu.make_async_copy(pair[0], pair[2], stay_sem.at[which, k]) for k, pair in enumerate(pairs)]
        away = [remote(pair[1], pair[2], back_send.at[which, k], back_recv.at[which, k], partner) for k, pair in enumerate(pairs)]
        return stay, away

    def result_start(role, which):
        stay, away = result_copies(role, which)
        for copy in away + stay:
            copy.start()

    with jax.named_scope('ag2'):
        for color in range(3):
            for piece in range(3):
                ag_copy(2, color, piece).start()
        drain_push()
        rs_drain(0)
        for color in range(3):
            ag_arrive(2, color, 0)
            norm_start(color)
            for piece in range(4):
                ag_copy(1, color, piece).start()

    with jax.named_scope('ag1_start'):
        @pl.when(core == ATTN)
        def _():
            result_start(ATTN, 0)

        @pl.when(core == EXPERT)
        def _():
            for rows, cols in ((LO, WEST), (HI, EAST)):
                down = full[mine + (rows, EAST)]
                send_down[0, :, cols] = down[SIDE:]
                stay_down[0, :, cols] = down[:SIDE]
            result_start(EXPERT, 0)
        rs_drain(1)
        ag_drain(2)
    with jax.named_scope('ag1_mid'):
        for color in range(3):
            norms[0, color, pos[ORDER[color][0]]] = norm_sum(1, color)
            norm_send_all(0, color)
        ag_mid(1)
        rs_drain(2)
    with jax.named_scope('ag1_end'):
        for color in range(3):
            ag_arrive(1, color, 2)
    with jax.named_scope('norm'):
        total = jnp.sum(norm_sum(0, 0) + norm_sum(0, 1) + norm_sum(0, 2), axis=(1, 2), keepdims=True)
        west, east = total[0], total[1]
        both = west + east
        west = jnp.where(core == ATTN, both, west)
        east = jnp.where(core == ATTN, both, east)
        lane = lax.broadcasted_iota(jnp.int32, (1, WIDE), 1)
        norm = jnp.sqrt(jnp.where(lane < NARROW, west, east))
        scales[...] = 1.0 / (norm + EPSILON)
    with jax.named_scope('ag0_start'):
        for color in range(3):
            axis, cols = ORDER[color][0], pl.ds(*COLS[color])
            idx = region({axis: pos[axis]}, ALL, cols)
            x_all[idx] = (full[idx] * scales[:, cols]).astype(BF16)
            for sub in range(2):
                for piece in range(2):
                    ag_copy(0, color, piece, sub).start()
            for piece in (2, 3):
                ag_copy(0, color, piece).start()
    with jax.named_scope('ag0_mid'):
        for sub in range(2):
            ag_mid(0, sub)
    with jax.named_scope('ag0_end'):
        for color in range(3):
            ag_arrive(0, color, 2)
    for level in range(2):
        departed(norms.at[level, :, pl.ds(0, 3)], norm_send.at[level])
    ag_drain(1)
    ag_drain(0)

    def weighted(a_val, q_val):
        return (COEF_B * a_val.astype(F32) + COEF_C * q_val.astype(BF16).astype(F32)).astype(BF16)

    def advance(x_val, y_val):
        return (COEF_A * x_val.astype(F32) + y_val.astype(BF16).astype(F32)).astype(BF16)

    def symmetric(out, base, size, block):
        for j in range(0, size, TILE):
            val = block(j)
            out[pl.ds(base + j, size - j), pl.ds(j, TILE)] = val
            if j + TILE < size:
                out[pl.ds(base + j, TILE), pl.ds(j + TILE, size - j - TILE)] = jnp.transpose(val[TILE:])

    def gram(base, size):
        def block(j):
            return lax.dot_general(x_mat[pl.ds(base + j, size - j), :], x_mat[pl.ds(base + j, TILE), :], (((1,), (1,)), ((), ())),
                                   preferred_element_type=F32).astype(BF16)
        symmetric(a_mat, base, size, block)

    def poly(base, size):
        def block(j):
            rows, cols = pl.ds(base + j, size - j), pl.ds(j, TILE)
            q_val = jnp.dot(a_mat[rows, pl.ds(0, size)], a_mat[pl.ds(base, size), cols], preferred_element_type=F32)
            return weighted(a_mat[rows, cols], q_val)
        symmetric(b_mat, base, size, block)

    def update(base, size):
        rows = pl.ds(base, size)
        y_val = jnp.dot(b_mat[rows, pl.ds(0, size)], x_mat[rows, :], preferred_element_type=F32)
        x_mat[rows, :] = advance(x_mat[rows, :], y_val)

    @pl.when(core == ATTN)
    def _():
        with jax.named_scope('fill'):
            x_mat[...] = x_all[...].reshape(WIDE, WIDE)

        def step(_, carry):
            gram(0, WIDE)
            poly(0, WIDE)
            update(0, WIDE)
            return carry
        with jax.named_scope('steps'):
            lax.fori_loop(0, NS_STEPS - 1, step, 0)
            gram(0, WIDE)
        with jax.named_scope('last'):
            rows = aligned(chip * CHIP_ROWS, CHIP_ROWS)
            a_val = a_mat[rows, :]
            b_val = weighted(a_val, jnp.dot(a_val, a_mat[...], preferred_element_type=F32))
            out = advance(x_mat[rows, :], jnp.dot(b_val, x_mat[...], preferred_element_type=F32)).astype(F32)
            out_pk[...] = out
            result_start(ATTN, 1)

    @pl.when(core == EXPERT)
    def _():
        with jax.named_scope('fill'):
            def fill_up(k, carry):
                val = x_all[k // 2, pl.ds(2 * lax.rem(k, 2), 2), :, :, WEST].reshape(128, NARROW)
                x_mat[WEST, aligned(k * 128, 128)] = jnp.transpose(val)
                return carry
            lax.fori_loop(0, 8, fill_up, 0)

            def fill_down(k, carry):
                z, y, x = coords_of(2 * k)
                val = x_all[z, y, pl.ds(x, 2), :, EAST].astype(F32)
                rows = aligned(NARROW + k * CHIP_ROWS, CHIP_ROWS)
                x_mat[rows, WEST] = val[:, :8].reshape(CHIP_ROWS, NARROW).astype(BF16)
                x_mat[rows, EAST] = val[:, 8:].reshape(CHIP_ROWS, NARROW).astype(BF16)
                return carry
            lax.fori_loop(0, 32, fill_down, 0)

        def step(_, carry):
            for stage in (gram, poly, update):
                stage(0, NARROW)
                stage(NARROW, NARROW)
            return carry
        with jax.named_scope('steps'):
            lax.fori_loop(0, NS_STEPS - 1, step, 0)
            gram(0, NARROW)
            gram(NARROW, NARROW)
        with jax.named_scope('last'):
            poly(0, NARROW)
            cols = aligned(chip // 8 * 128, 128)
            out_up = advance(x_mat[WEST, cols], jnp.dot(b_mat[WEST, WEST], x_mat[WEST, cols], preferred_element_type=F32))
            turn[...] = jnp.transpose(out_up.astype(F32))
            rows = aligned(NARROW + chip // 2 * CHIP_ROWS, CHIP_ROWS)
            a_val = a_mat[rows, WEST]
            b_val = weighted(a_val, jnp.dot(a_val, a_mat[EAST, WEST], preferred_element_type=F32))
            both = advance(x_mat[rows, :], jnp.dot(b_val, x_mat[EAST, :], preferred_element_type=F32)).astype(F32)
            out_down = jnp.where(lax.rem(chip, 2) == 0, both[:8], both[8:])
            send_down[1] = out_down[SIDE:]
            stay_down[1] = out_down[:SIDE]
            result_start(EXPERT, 1)

    with jax.named_scope('swap'):
        for role, other in ((ATTN, EXPERT), (EXPERT, ATTN)):
            @pl.when(core == role)
            def _(role=role, other=other):
                for which in range(2):
                    stay, away = result_copies(role, which)
                    for copy in stay:
                        copy.wait()
                    for copy in away:
                        copy.wait_send()
                    for copy in result_copies(other, which)[1]:
                        copy.wait_recv()


def finish(*refs):
    for k in range(3):
        mom, out, mas = refs[k], refs[3 + k], refs[6 + k]
        mom_out, mas_out, low_out = refs[9 + 3 * k:12 + 3 * k]
        old = mas[...]
        new = old - LEARN_RATE * (0.2 * math.sqrt(WIDE) * out[...] + WEIGHT_DECAY * old)
        mom_out[...] = mom[...]
        mas_out[...] = new
        low_out[...] = new.astype(BF16)


def solution(mesh):
    group_size = mesh.shape['data']
    grad_spec = P(('stage', 'data'), None, None, None)
    row_spec = P('stage', 'data', None)

    def step_local(grad_attn, mom_attn, mas_attn, grad_up, mom_up, mas_up, grad_down, mom_down, mas_down):
        vmem = pl.BlockSpec(memory_space=pltpu.VMEM)
        hbm = pl.BlockSpec(memory_space=pl.ANY)
        shapes = ((8, WIDE), (8, NARROW), (SIDE, WIDE))
        sem = pltpu.SemaphoreType.DMA
        scratch = [
            *[pltpu.VMEM(BLOCK, F32)] * 3,
            *[pltpu.VMEM((6,) + (SIDE,) * free + (8, WIDE), F32) for free in (2, 1)],
            pltpu.VMEM((3, CHIP_ROWS, WIDE), F32),
            pltpu.VMEM((CHIP_ROWS, WIDE), F32),
            *[pltpu.VMEM(shape, F32) for shape in shapes * 2],
            *[pltpu.VMEM((2, SIDE, WIDE), F32)] * 2,
            pltpu.VMEM((CHIP_ROWS, WIDE), F32),
            *[pltpu.VMEM((WIDE, WIDE), BF16)] * 3,
            pltpu.VMEM((128, NARROW), F32),
            pltpu.VMEM(BLOCK, BF16), pltpu.VMEM((2, 3, SIDE, 2, 8, 128), F32), pltpu.VMEM((1, WIDE), F32),
            sem((3, 5)), sem, sem((3, 5)),
            sem((3,)), sem((3, 3, 5)), sem((3,)), sem((3, 3, 5)),
            *[sem((2,))] * 2,
            *[sem((2, 2))] * 3,
            sem((2,)),
            sem((2,)), sem((2, 3)),
            pltpu.SemaphoreType.REGULAR,
        ]
        result = pl.pallas_call(
            functools.partial(kernel, group_size),
            out_shape=[jax.ShapeDtypeStruct(shape, F32) for shape in shapes * 2],
            in_specs=[hbm] * 6,
            out_specs=[hbm] * 6,
            scratch_shapes=scratch,
            compiler_params=pltpu.CompilerParams(collective_id=0, has_side_effects=True, vmem_limit_bytes=60 * 1024 * 1024),
            name='muon',
        )(grad_attn.reshape(BLOCK), grad_up.reshape(BLOCK[:4] + (NARROW,)), grad_down.reshape(BLOCK[:3] + (8, WIDE)),
          mom_attn[0], mom_up[0], mom_down[0])
        outs = [jax.ShapeDtypeStruct(shape, dtype) for shape in shapes for dtype in (F32, F32, BF16)]
        done = pl.pallas_call(finish, out_shape=outs, in_specs=[vmem] * 9, out_specs=[vmem] * 9, name='finish')(
            *result, mas_attn[0], mas_up[0], mas_down[0])
        return tuple(d[None] for d in done)

    return jax.shard_map(step_local, mesh=mesh, in_specs=(grad_spec, row_spec, row_spec) * 3, out_specs=(row_spec,) * 9,
                         check_vma=False)
```

```python
import functools
import math

import jax
import jax.numpy as jnp
from jax import lax
from jax.experimental import pallas as pl
from jax.experimental.pallas import tpu as pltpu
from jax.sharding import PartitionSpec as P

MOMENTUM = 0.95
LEARN_RATE = 0.25
WEIGHT_DECAY = 0.2
EPSILON = 1e-7
COEF_A = 3.4445
COEF_B = -4.7750
COEF_C = 2.0315
NS_STEPS = 5

F32 = jnp.float32
BF16 = jnp.bfloat16

COLS = ((0, 384), (384, 384), (768, 256))
ORDER = ((0, 1, 2), (1, 2, 0), (2, 0, 1))
ATTN = 1
EXPERT = 0
SIDE = 4
CHIP_ROWS = 16
WIDE = 1024
NARROW = 512
TILE = 256
BLOCK = (SIDE, SIDE, SIDE, CHIP_ROWS, WIDE)
ALL = slice(None)
LO = pl.ds(0, 8)
HI = pl.ds(8, 8)
HALF = (LO, HI)
WEST = pl.ds(0, NARROW)
EAST = pl.ds(NARROW, NARROW)
PIECES = (
    (('up', 0, 384, ALL, 0),),
    (('up', 384, 128, ALL, 384), ('down', 0, TILE, LO, NARROW), ('down', NARROW, TILE, HI, NARROW)),
    (('down', TILE, TILE, LO, 768), ('down', 768, TILE, HI, 768)),
)


def place(ref, fixed, rows, cols):
    return ref.at[region(fixed, rows, cols)]


def region(fixed, rows, cols):
    return tuple(fixed.get(axis, ALL) for axis in range(3)) + (rows, cols)


def coords_of(k):
    return k // (SIDE * SIDE), lax.rem(k // SIDE, SIDE), lax.rem(k, SIDE)


def aligned(start, size):
    return pl.ds(pl.multiple_of(start, size), size)


def kernel(group_size, grad_attn, grad_up, grad_down, mom_attn, mom_up, mom_down,
           mo_attn, mo_up, mo_down, got_attn, got_up, got_down,
           own, peer, full, recv0, recv1, recv2, mom_pk, swap_attn, swap_up, swap_down, keep_attn, keep_up, keep_down,
           send_down, stay_down, out_pk, x_mat, a_mat, b_mat, turn, x_all, norms, scales,
           load_sem, push_sem, pull_sem, rs_send, rs_recv, ag_send, ag_recv, ex_send, ex_recv, back_send, back_recv, stay_sem, keep_sem, norm_send, norm_recv, gate):
    me = lax.axis_index('data')
    core = lax.rem(me, 2)
    chip = me // 2
    pos = coords_of(chip)
    partner = me + 1 - 2 * core
    recvs = (recv0, recv1, recv2)

    def at_axis(axis, coord):
        coords = list(pos)
        coords[axis] = coord
        return ((coords[0] * SIDE + coords[1]) * SIDE + coords[2]) * 2 + core

    right = [lax.rem(p + 1, SIDE) for p in pos]
    left = [lax.rem(p + 3, SIDE) for p in pos]
    far = [lax.rem(p + 2, SIDE) for p in pos]
    right_dev = [at_axis(a, right[a]) for a in range(3)]
    left_dev = [at_axis(a, left[a]) for a in range(3)]
    far_dev = [at_axis(a, far[a]) for a in range(3)]

    def remote(src, dst, send_sem, recv_sem, device):
        return pltpu.make_async_remote_copy(src_ref=src, dst_ref=dst, send_sem=send_sem, recv_sem=recv_sem,
                                            device_id={'data': device}, device_id_type=pl.DeviceIdType.MESH)

    def arrived(part, sem):
        remote(part, part, sem, sem, partner).wait_recv()

    def departed(part, sem):
        remote(part, part, sem, sem, partner).wait_send()

    def turns(color):
        axis = ORDER[color][0]
        return axis, (far[axis], right[axis], left[axis], pos[axis])

    PARTS = ((0, 0, 0), (0, 1, 0), (0, 0, 1), (0, 1, 1), (1, None, None), (2, None, None), (3, None, None))

    def turn_fixed(color, turn_idx, sub):
        axis, coords = turns(color)
        fixed = {axis: coords[turn_idx]}
        if sub is not None:
            fixed[min(k for k in range(3) if k != axis)] = pl.ds(2 * sub, 2)
        return fixed

    def attn_copy(color, part):
        turn_idx, half, sub = PARTS[part]
        idx = region(turn_fixed(color, turn_idx, sub), ALL if half is None else HALF[half], pl.ds(*COLS[color]))
        return remote(grad_attn.at[idx], peer.at[idx], push_sem, pull_sem.at[color, part], partner)

    def expert_copies(color, part):
        turn_idx, half, sub = PARTS[part]
        fixed = turn_fixed(color, turn_idx, sub)
        copies = []
        for source, col, width, rows, packed in PIECES[color]:
            from_rows = ALL
            if half is not None and source == 'up':
                from_rows = rows = HALF[half]
            elif half is not None and rows is not HALF[half]:
                continue
            src = place(grad_up if source == 'up' else grad_down, fixed, from_rows, pl.ds(col, width))
            copies.append(remote(src, place(peer, fixed, rows, pl.ds(packed, width)), push_sem, pull_sem.at[color, part], partner))
        return copies

    def mom_from_attn():
        return [remote(mom_up, swap_up, ex_send.at[0], ex_recv.at[0], partner),
                remote(mom_down, swap_down, ex_send.at[1], ex_recv.at[1], partner)]

    def mom_from_expert():
        return [remote(mom_attn, swap_attn, ex_send.at[0], ex_recv.at[0], partner)]

    def keep_copies(role):
        pairs = ((mom_attn, keep_attn),) if role == ATTN else ((mom_up, keep_up), (mom_down, keep_down))
        return [pltpu.make_async_copy(src, dst, keep_sem.at[k]) for k, (src, dst) in enumerate(pairs)]

    barrier = pltpu.get_barrier_semaphore()
    for device in [partner] + right_dev + left_dev:
        pl.semaphore_signal(barrier, inc=1, device_id={'data': device}, device_id_type=pl.DeviceIdType.MESH)

    @pl.when(core == ATTN)
    def _():
        pltpu.make_async_copy(grad_attn, own, load_sem).start()
        for copy in keep_copies(ATTN):
            copy.start()

    with jax.named_scope('barrier'):
        pl.semaphore_wait(barrier, 7)

    @pl.when(core == ATTN)
    def _():
        for copy in mom_from_attn():
            copy.start()
        for part in range(len(PARTS)):
            for color in range(3):
                for copy in expert_copies(color, part):
                    copy.start()

    @pl.when(core == EXPERT)
    def _():
        for part in range(len(PARTS)):
            for color in range(3):
                attn_copy(color, part).start()
        for copy in mom_from_expert():
            copy.start()
        for copy in keep_copies(EXPERT):
            copy.start()
        for src, rows, cols in ((grad_up, ALL, WEST), (grad_down.at[:, :, :, :, WEST], LO, EAST), (grad_down.at[:, :, :, :, EAST], HI, EAST)):
            pltpu.make_async_copy(src, place(own, {}, rows, cols), load_sem).start()
        with jax.named_scope('gate'):
            pl.semaphore_wait(gate, 1)

    def open_gate():
        @pl.when(core == ATTN)
        def _():
            pl.semaphore_signal(gate, inc=1, device_id={'data': partner}, device_id_type=pl.DeviceIdType.MESH)

    def chip_sum(color, part):
        turn_idx, half, sub = PARTS[part]
        idx = region(turn_fixed(color, turn_idx, sub), ALL if half is None else HALF[half], pl.ds(*COLS[color]))
        arrived(peer.at[idx], pull_sem.at[color, part])
        own[idx] = own[idx] + peer[idx]

    PAIRED = ((far, 0, right_dev), (far, 1, left_dev), (right, 1, right_dev), (left, 0, left_dev), (right, 0, right_dev), (left, 1, left_dev))
    DIRECT = ((far, far_dev), (right, right_dev), (left, left_dev))

    def ctx(phase, color):
        order = ORDER[color]
        return order[phase], {order[k]: pos[order[k]] for k in range(phase)}, pl.ds(*COLS[color])

    def rs_slot(phase, color, piece, sub=None):
        free = [ALL] * (2 - phase)
        if sub is not None:
            free[0] = pl.ds(2 * sub, 2)
        return (piece, *free, ALL, pl.ds(*COLS[color]))

    def recv_sem(sems, phase, color, piece, sub):
        if phase == 2:
            return sems.at[color]
        if phase == 1:
            return sems.at[3 + 3 * color + min(piece, 2)]
        return sems.at[12 + 5 * color + (4 if piece > 1 else 2 * piece + sub)]

    def rs_region(phase, color, coord, rows, sub):
        axis, fixed, cols = ctx(phase, color)
        fixed = {**fixed, axis: coord[axis]}
        if sub is not None:
            fixed[min(k for k in range(3) if k != axis)] = pl.ds(2 * sub, 2)
        return region(fixed, rows, cols)

    def rs_copy(phase, color, piece, sub=None):
        if phase < 2:
            coord, half, device = PAIRED[piece]
            rows = HALF[half]
        else:
            coord, device = DIRECT[piece]
            rows = ALL
        return remote(own.at[rs_region(phase, color, coord, rows, sub)], recvs[phase].at[rs_slot(phase, color, piece, sub)],
                      rs_send.at[phase], recv_sem(rs_recv, phase, color, piece, sub), device[ORDER[color][phase]])

    def rs_arrive(phase, color, pieces, sub=None):
        first = pieces[0]
        slot = rs_slot(phase, color, pl.ds(first, len(pieces)), sub)
        arrived(recvs[phase].at[slot], recv_sem(rs_recv, phase, color, first, sub))

    def rs_add(phase, color, coord, rows, pieces, sub=None):
        idx = rs_region(phase, color, coord, rows, sub)
        total = own[idx]
        for piece in pieces:
            total = total + recvs[phase][rs_slot(phase, color, piece, sub)]
        own[idx] = total

    def rs_mid(phase, color, sub=None):
        rs_arrive(phase, color, (0,), sub)
        rs_add(phase, color, right, LO, (0,), sub)
        rs_copy(phase, color, 4, sub).start()
        rs_arrive(phase, color, (1,), sub)
        rs_add(phase, color, left, HI, (1,), sub)
        rs_copy(phase, color, 5, sub).start()

    def rs_end(phase, color):
        rs_arrive(phase, color, (2, 3, 4, 5))
        rs_add(phase, color, pos, LO, (3, 4))
        rs_add(phase, color, pos, HI, (2, 5))

    with jax.named_scope('rs0_load'):
        pltpu.make_async_copy(own, own, load_sem).wait()
        for part in range(4):
            for color in range(3):
                chip_sum(color, part)
                rs_copy(0, color, part % 2, part // 2).start()
        for part in (4, 5):
            for color in range(3):
                chip_sum(color, part)
                rs_copy(0, color, part - 2).start()
    with jax.named_scope('rs0_mid'):
        for sub in range(2):
            for color in range(3):
                rs_mid(0, color, sub)
        open_gate()
        for color in range(3):
            chip_sum(color, 6)
    with jax.named_scope('rs0_end'):
        for color in range(3):
            rs_end(0, color)
            for piece in range(4):
                rs_copy(1, color, piece).start()
    with jax.named_scope('rs1_mid'):
        for color in range(3):
            rs_mid(1, color)
    with jax.named_scope('rs1_end'):
        for color in range(3):
            rs_end(1, color)
            for piece in range(3):
                rs_copy(2, color, piece).start()
    with jax.named_scope('rs2'):
        for color in range(3):
            rs_arrive(2, color, (0, 1, 2))
            rs_add(2, color, pos, ALL, range(3))

    @pl.when(core == ATTN)
    def _():
        mom_from_expert()[0].wait_recv()
        keep_copies(ATTN)[0].wait()
        mom_pk[LO] = swap_attn[...]
        mom_pk[HI] = keep_attn[...]

    @pl.when(core == EXPERT)
    def _():
        for copy in mom_from_attn():
            copy.wait_recv()
        for copy in keep_copies(EXPERT):
            copy.wait()
        mom_pk[LO, WEST] = keep_up[...]
        mom_pk[HI, WEST] = swap_up[...]
        for first, cols in ((0, WEST), (8, EAST)):
            mom_pk[pl.ds(first, SIDE), EAST] = keep_down[:, cols]
            mom_pk[pl.ds(first + SIDE, SIDE), EAST] = swap_down[:, cols]

    mine = pos
    mom_new = MOMENTUM * mom_pk[...] + own[mine] * (1.0 / group_size)
    full[mine] = mom_new

    AG_SEND = ((pos, 0, right_dev), (pos, 1, left_dev), (pos, 1, right_dev), (pos, 0, left_dev), (left, 0, right_dev), (right, 1, left_dev))
    AG_LAND = ((left, 0), (right, 1), (left, 1), (right, 0), (far, 0), (far, 1))
    AG_DIRECT = (far, left, right)

    def ag_part(phase, color, coord, rows):
        axis, fixed, cols = ctx(phase, color)
        return place(full, {**fixed, axis: coord[axis]}, rows, cols)

    def ag_half(phase, color, coord, half, sub=None):
        if phase == 1:
            return ag_part(phase, color, coord, HALF[half])
        axis, second, _ = ORDER[color]
        span = pl.ds(2 * half, 2) if sub is None else pl.ds(2 * half + sub, 1)
        return place(x_all, {axis: coord[axis], second: span}, ALL, pl.ds(*COLS[color]))

    def ag_remote(part, phase, color, piece, device, sub=None):
        return remote(part, part, ag_send.at[phase], recv_sem(ag_recv, phase, color, piece, sub), device[ORDER[color][phase]])

    def ag_copy(phase, color, piece, sub=None):
        if phase < 2:
            coord, half, device = AG_SEND[piece]
            return ag_remote(ag_half(phase, color, coord, half, sub), phase, color, piece, device, sub)
        return ag_remote(ag_part(phase, color, pos, ALL), phase, color, piece, DIRECT[piece][1])

    def ag_arrive(phase, color, piece, sub=None):
        sem = recv_sem(ag_recv, phase, color, piece, sub)
        if phase == 2:
            arrived(ag_part(phase, color, [pl.ds(0, 3)] * 3, ALL), sem)
        elif piece < 2:
            coord, half = AG_LAND[piece]
            arrived(ag_half(phase, color, coord, half, sub), sem)
        elif phase == 1:
            arrived(ag_part(phase, color, [pl.ds(0, 2)] * 3, ALL), sem)
        else:
            arrived(place(x_all, {ORDER[color][0]: pl.ds(0, 2)}, ALL, pl.ds(*COLS[color])), sem)

    def drain_push():
        departed(peer, push_sem)

        @pl.when(core == ATTN)
        def _():
            for copy in mom_from_attn():
                copy.wait_send()

        @pl.when(core == EXPERT)
        def _():
            for copy in mom_from_expert():
                copy.wait_send()

    def rs_drain(phase):
        departed(recvs[phase], rs_send.at[phase])

    def ag_drain(phase):
        departed((x_all.at[pl.ds(0, 3)], full.at[0, pl.ds(0, 3)], full.at[0, 0, pl.ds(0, 3)])[phase], ag_send.at[phase])

    def ag_mid(phase, sub=None):
        for color in range(3):
            for piece in range(2):
                ag_arrive(phase, color, piece, sub)
                ag_copy(phase, color, piece + 4, sub).start()

    def norm_copy(level, color, piece):
        axis = ORDER[color][level]
        part = norms.at[level, color, pos[axis]]
        return remote(part, part, norm_send.at[level], norm_recv.at[level, color], DIRECT[piece][1][axis])

    def norm_sum(level, color):
        arrived(norms.at[level, color, pl.ds(0, 3)], norm_recv.at[level, color])
        return sum(norms[level, color, j] for j in range(SIDE))

    def norm_send_all(level, color):
        for piece in range(3):
            norm_copy(level, color, piece).start()

    def square_tile(line, cols):
        val = full[line + (ALL, cols)].reshape(8, 8, cols.size)
        val = jnp.sum(val * val, axis=0)
        return sum(val[:, k:k + 128] for k in range(0, cols.size, 128))

    def norm_start(color):
        first_axis, second_axis, _ = ORDER[color]
        line = region({first_axis: pos[first_axis], second_axis: pos[second_axis]}, ALL, ALL)[:3]
        first, width = COLS[color]
        west = max(0, min(NARROW - first, width))
        for side, (start, size) in enumerate(((first, west), (first + west, width - west))):
            val = square_tile(line, pl.ds(start, size)) if size else jnp.zeros((8, 128), F32)
            norms[1, color, pos[second_axis], side] = val
        norm_send_all(1, color)

    def result_copies(role, which):
        if role == ATTN:
            source = (full.at[mine], out_pk)[which]
            pairs = ((source.at[HI], source.at[LO], (mo_attn, got_attn)[which]),)
        else:
            first = pl.multiple_of(lax.rem(chip, 8) * CHIP_ROWS, CHIP_ROWS)
            ups = ((full.at[mine + (LO, WEST)], full.at[mine + (HI, WEST)]), (turn.at[pl.ds(first, 8)], turn.at[pl.ds(first + 8, 8)]))[which]
            pairs = (ups + ((mo_up, got_up)[which],), (stay_down.at[which], send_down.at[which], (mo_down, got_down)[which]))
        stay = [pltpu.make_async_copy(pair[0], pair[2], stay_sem.at[which, k]) for k, pair in enumerate(pairs)]
        away = [remote(pair[1], pair[2], back_send.at[which, k], back_recv.at[which, k], partner) for k, pair in enumerate(pairs)]
        return stay, away

    def result_start(role, which):
        stay, away = result_copies(role, which)
        for copy in away + stay:
            copy.start()

    with jax.named_scope('ag2'):
        for color in range(3):
            for piece in range(3):
                ag_copy(2, color, piece).start()
        drain_push()
        rs_drain(0)
        for color in range(3):
            ag_arrive(2, color, 0)
            norm_start(color)
            for piece in range(4):
                ag_copy(1, color, piece).start()

    with jax.named_scope('ag1_start'):
        @pl.when(core == ATTN)
        def _():
            result_start(ATTN, 0)

        @pl.when(core == EXPERT)
        def _():
            for rows, cols in ((LO, WEST), (HI, EAST)):
                down = full[mine + (rows, EAST)]
                send_down[0, :, cols] = down[SIDE:]
                stay_down[0, :, cols] = down[:SIDE]
            result_start(EXPERT, 0)
        rs_drain(1)
        ag_drain(2)
    with jax.named_scope('ag1_mid'):
        for color in range(3):
            norms[0, color, pos[ORDER[color][0]]] = norm_sum(1, color)
            norm_send_all(0, color)
        ag_mid(1)
        rs_drain(2)
    with jax.named_scope('ag1_end'):
        for color in range(3):
            ag_arrive(1, color, 2)
    with jax.named_scope('norm'):
        total = jnp.sum(norm_sum(0, 0) + norm_sum(0, 1) + norm_sum(0, 2), axis=(1, 2), keepdims=True)
        west, east = total[0], total[1]
        both = west + east
        west = jnp.where(core == ATTN, both, west)
        east = jnp.where(core == ATTN, both, east)
        lane = lax.broadcasted_iota(jnp.int32, (1, WIDE), 1)
        norm = jnp.sqrt(jnp.where(lane < NARROW, west, east))
        scales[...] = 1.0 / (norm + EPSILON)
    with jax.named_scope('ag0_start'):
        for color in range(3):
            axis, cols = ORDER[color][0], pl.ds(*COLS[color])
            idx = region({axis: pos[axis]}, ALL, cols)
            x_all[idx] = (full[idx] * scales[:, cols]).astype(BF16)
            for sub in range(2):
                for piece in range(2):
                    ag_copy(0, color, piece, sub).start()
            for piece in (2, 3):
                ag_copy(0, color, piece).start()
    with jax.named_scope('ag0_mid'):
        for sub in range(2):
            ag_mid(0, sub)
    with jax.named_scope('ag0_end'):
        for color in range(3):
            ag_arrive(0, color, 2)
    for level in range(2):
        departed(norms.at[level, :, pl.ds(0, 3)], norm_send.at[level])
    ag_drain(1)
    ag_drain(0)

    def weighted(a_val, q_val):
        return (COEF_B * a_val.astype(F32) + COEF_C * q_val.astype(BF16).astype(F32)).astype(BF16)

    def advance(x_val, y_val):
        return (COEF_A * x_val.astype(F32) + y_val.astype(BF16).astype(F32)).astype(BF16)

    def symmetric(out, base, size, block):
        for j in range(0, size, TILE):
            val = block(j)
            out[pl.ds(base + j, size - j), pl.ds(j, TILE)] = val
            if j + TILE < size:
                out[pl.ds(base + j, TILE), pl.ds(j + TILE, size - j - TILE)] = jnp.transpose(val[TILE:])

    def gram(base, size):
        def block(j):
            return lax.dot_general(x_mat[pl.ds(base + j, size - j), :], x_mat[pl.ds(base + j, TILE), :], (((1,), (1,)), ((), ())),
                                   preferred_element_type=F32).astype(BF16)
        symmetric(a_mat, base, size, block)

    def poly(base, size):
        def block(j):
            rows, cols = pl.ds(base + j, size - j), pl.ds(j, TILE)
            q_val = jnp.dot(a_mat[rows, pl.ds(0, size)], a_mat[pl.ds(base, size), cols], preferred_element_type=F32)
            return weighted(a_mat[rows, cols], q_val)
        symmetric(b_mat, base, size, block)

    def update(base, size):
        rows = pl.ds(base, size)
        y_val = jnp.dot(b_mat[rows, pl.ds(0, size)], x_mat[rows, :], preferred_element_type=F32)
        x_mat[rows, :] = advance(x_mat[rows, :], y_val)

    @pl.when(core == ATTN)
    def _():
        with jax.named_scope('fill'):
            x_mat[...] = x_all[...].reshape(WIDE, WIDE)

        def step(_, carry):
            gram(0, WIDE)
            poly(0, WIDE)
            update(0, WIDE)
            return carry
        with jax.named_scope('steps'):
            lax.fori_loop(0, NS_STEPS - 1, step, 0)
            gram(0, WIDE)
        with jax.named_scope('last'):
            rows = aligned(chip * CHIP_ROWS, CHIP_ROWS)
            a_val = a_mat[rows, :]
            b_val = weighted(a_val, jnp.dot(a_val, a_mat[...], preferred_element_type=F32))
            out = advance(x_mat[rows, :], jnp.dot(b_val, x_mat[...], preferred_element_type=F32)).astype(F32)
            out_pk[...] = out
            result_start(ATTN, 1)

    @pl.when(core == EXPERT)
    def _():
        with jax.named_scope('fill'):
            def fill(k, carry):
                val = x_all[k // 2, pl.ds(2 * lax.rem(k, 2), 2), :, :, WEST].reshape(128, NARROW)
                x_mat[WEST, aligned(k * 128, 128)] = jnp.transpose(val)
                val = x_all[k // 2, pl.ds(2 * lax.rem(k, 2), 2), :, :, EAST].astype(F32)
                rows = aligned(NARROW + k * 64, 64)
                x_mat[rows, WEST] = val[:, :, :8].reshape(64, NARROW).astype(BF16)
                x_mat[rows, EAST] = val[:, :, 8:].reshape(64, NARROW).astype(BF16)
                return carry
            lax.fori_loop(0, 8, fill, 0)

        def step(_, carry):
            for stage in (gram, poly, update):
                stage(0, NARROW)
                stage(NARROW, NARROW)
            return carry
        with jax.named_scope('steps'):
            lax.fori_loop(0, NS_STEPS - 1, step, 0)
            gram(0, NARROW)
            gram(NARROW, NARROW)
        with jax.named_scope('last'):
            poly(0, NARROW)
            cols = aligned(chip // 8 * 128, 128)
            out_up = advance(x_mat[WEST, cols], jnp.dot(b_mat[WEST, WEST], x_mat[WEST, cols], preferred_element_type=F32))
            turn[...] = jnp.transpose(out_up.astype(F32))
            rows = aligned(NARROW + chip // 2 * CHIP_ROWS, CHIP_ROWS)
            a_val = a_mat[rows, WEST]
            b_val = weighted(a_val, jnp.dot(a_val, a_mat[EAST, WEST], preferred_element_type=F32))
            both = advance(x_mat[rows, :], jnp.dot(b_val, x_mat[EAST, :], preferred_element_type=F32)).astype(F32)
            out_down = jnp.where(lax.rem(chip, 2) == 0, both[:8], both[8:])
            send_down[1] = out_down[SIDE:]
            stay_down[1] = out_down[:SIDE]
            result_start(EXPERT, 1)

    with jax.named_scope('swap'):
        for role, other in ((ATTN, EXPERT), (EXPERT, ATTN)):
            @pl.when(core == role)
            def _(role=role, other=other):
                for which in range(2):
                    stay, away = result_copies(role, which)
                    for copy in stay:
                        copy.wait()
                    for copy in away:
                        copy.wait_send()
                    for copy in result_copies(other, which)[1]:
                        copy.wait_recv()


def finish(*refs):
    for k in range(3):
        mom, out, mas = refs[k], refs[3 + k], refs[6 + k]
        mom_out, mas_out, low_out = refs[9 + 3 * k:12 + 3 * k]
        old = mas[...]
        new = old - LEARN_RATE * (0.2 * math.sqrt(WIDE) * out[...] + WEIGHT_DECAY * old)
        mom_out[...] = mom[...]
        mas_out[...] = new
        low_out[...] = new.astype(BF16)


def solution(mesh):
    group_size = mesh.shape['data']
    grad_spec = P(('stage', 'data'), None, None, None)
    row_spec = P('stage', 'data', None)

    def step_local(grad_attn, mom_attn, mas_attn, grad_up, mom_up, mas_up, grad_down, mom_down, mas_down):
        vmem = pl.BlockSpec(memory_space=pltpu.VMEM)
        hbm = pl.BlockSpec(memory_space=pltpu.HBM)
        any_space = pl.BlockSpec(memory_space=pl.ANY)
        shapes = ((8, WIDE), (8, NARROW), (SIDE, WIDE))
        sem = pltpu.SemaphoreType.DMA
        scratch = [
            *[pltpu.VMEM(BLOCK, F32)] * 3,
            *[pltpu.VMEM((6,) + (SIDE,) * free + (8, WIDE), F32) for free in (2, 1)],
            pltpu.VMEM((3, CHIP_ROWS, WIDE), F32),
            pltpu.VMEM((CHIP_ROWS, WIDE), F32),
            *[pltpu.VMEM(shape, F32) for shape in shapes * 2],
            *[pltpu.VMEM((2, SIDE, WIDE), F32)] * 2,
            pltpu.VMEM((CHIP_ROWS, WIDE), F32),
            *[pltpu.VMEM((WIDE, WIDE), BF16)] * 3,
            pltpu.VMEM((128, NARROW), F32),
            pltpu.VMEM(BLOCK, BF16), pltpu.VMEM((2, 3, SIDE, 2, 8, 128), F32), pltpu.VMEM((1, WIDE), F32),
            sem, sem, sem((3, 7)),
            sem((3,)), sem((27,)), sem((3,)), sem((27,)),
            *[sem((2,))] * 2,
            *[sem((2, 2))] * 3,
            sem((2,)),
            sem((2,)), sem((2, 3)),
            pltpu.SemaphoreType.REGULAR,
        ]
        result = pl.pallas_call(
            functools.partial(kernel, group_size),
            out_shape=[jax.ShapeDtypeStruct(shape, F32) for shape in shapes * 2],
            in_specs=[hbm] * 6,
            out_specs=[any_space] * 6,
            scratch_shapes=scratch,
            compiler_params=pltpu.CompilerParams(collective_id=0, has_side_effects=True, vmem_limit_bytes=36 * 1024 * 1024),
            name='muon',
        )(*(pltpu.with_memory_space_constraint(v, pltpu.HBM) for v in (grad_attn.reshape(BLOCK), grad_up.reshape(BLOCK[:4] + (NARROW,)), grad_down.reshape(BLOCK[:3] + (8, WIDE)))),
          *(pltpu.with_memory_space_constraint(v[0], pltpu.HBM) for v in (mom_attn, mom_up, mom_down)))
        outs = [jax.ShapeDtypeStruct(shape, dtype) for shape in shapes for dtype in (F32, F32, BF16)]
        done = pl.pallas_call(finish, out_shape=outs, in_specs=[vmem] * 9, out_specs=[vmem] * 9, name='finish',
                              compiler_params=pltpu.CompilerParams(vmem_limit_bytes=4 * 1024 * 1024))(
            *result, mas_attn[0], mas_up[0], mas_down[0])
        return tuple(d[None] for d in done)

    return jax.shard_map(step_local, mesh=mesh, in_specs=(grad_spec, row_spec, row_spec) * 3, out_specs=(row_spec,) * 9,
                         check_vma=False)
```

```python
import functools
import math

import jax
import jax.numpy as jnp
from jax import lax
from jax.experimental import pallas as pl
from jax.experimental.pallas import tpu as pltpu
from jax.sharding import PartitionSpec as P

MOMENTUM = 0.95
LEARN_RATE = 0.25
WEIGHT_DECAY = 0.2
EPSILON = 1e-7
COEF_A = 3.4445
COEF_B = -4.7750
COEF_C = 2.0315
NS_STEPS = 5

F32 = jnp.float32
BF16 = jnp.bfloat16

COLS = ((0, 384), (384, 384), (768, 256))
ORDER = ((0, 1, 2), (1, 2, 0), (2, 0, 1))
ATTN = 1
EXPERT = 0
SIDE = 4
CHIP_ROWS = 16
WIDE = 1024
NARROW = 512
TILE = 256
BLOCK = (SIDE, SIDE, SIDE, CHIP_ROWS, WIDE)
ALL = slice(None)
LO = pl.ds(0, 8)
HI = pl.ds(8, 8)
HALF = (LO, HI)
WEST = pl.ds(0, NARROW)
EAST = pl.ds(NARROW, NARROW)
PIECES = (
    (('up', 0, 384, ALL, 0),),
    (('up', 384, 128, ALL, 384), ('down', 0, TILE, LO, NARROW), ('down', NARROW, TILE, HI, NARROW)),
    (('down', TILE, TILE, LO, 768), ('down', 768, TILE, HI, 768)),
)


def place(ref, fixed, rows, cols):
    return ref.at[region(fixed, rows, cols)]


def region(fixed, rows, cols):
    return tuple(fixed.get(axis, ALL) for axis in range(3)) + (rows, cols)


def coords_of(k):
    return k // (SIDE * SIDE), lax.rem(k // SIDE, SIDE), lax.rem(k, SIDE)


def aligned(start, size):
    return pl.ds(pl.multiple_of(start, size), size)


def kernel(group_size, grad_attn, grad_up, grad_down, mom_attn, mom_up, mom_down,
           mo_attn, mo_up, mo_down, got_attn, got_up, got_down,
           own, peer, full, recv0, recv1, recv2, mom_pk, swap_attn, swap_up, swap_down, keep_attn, keep_up, keep_down,
           send_down, stay_down, out_pk, x_mat, a_mat, b_mat, turn, x_all, norms, scales,
           load_sem, push_sem, pull_sem, rs_send, rs_recv, ag_send, ag_recv, ex_send, ex_recv, back_send, back_recv, stay_sem, keep_sem, norm_send, norm_recv, gate):
    me = lax.axis_index('data')
    core = lax.rem(me, 2)
    chip = me // 2
    pos = coords_of(chip)
    partner = me + 1 - 2 * core
    recvs = (recv0, recv1, recv2)

    def at_axis(axis, coord):
        coords = list(pos)
        coords[axis] = coord
        return ((coords[0] * SIDE + coords[1]) * SIDE + coords[2]) * 2 + core

    right = [lax.rem(p + 1, SIDE) for p in pos]
    left = [lax.rem(p + 3, SIDE) for p in pos]
    far = [lax.rem(p + 2, SIDE) for p in pos]
    right_dev = [at_axis(a, right[a]) for a in range(3)]
    left_dev = [at_axis(a, left[a]) for a in range(3)]
    far_dev = [at_axis(a, far[a]) for a in range(3)]

    def remote(src, dst, send_sem, recv_sem, device):
        return pltpu.make_async_remote_copy(src_ref=src, dst_ref=dst, send_sem=send_sem, recv_sem=recv_sem,
                                            device_id={'data': device}, device_id_type=pl.DeviceIdType.MESH)

    def arrived(part, sem):
        remote(part, part, sem, sem, partner).wait_recv()

    def departed(part, sem):
        remote(part, part, sem, sem, partner).wait_send()

    def turns(color):
        axis = ORDER[color][0]
        return axis, (far[axis], right[axis], left[axis], pos[axis])

    PARTS = ((0, 0, 0), (0, 1, 0), (0, 0, 1), (0, 1, 1), (1, None, None), (2, None, None), (3, None, None))

    def turn_fixed(color, turn_idx, sub):
        axis, coords = turns(color)
        fixed = {axis: coords[turn_idx]}
        if sub is not None:
            fixed[min(k for k in range(3) if k != axis)] = pl.ds(2 * sub, 2)
        return fixed

    def pull_of(color, part):
        return pull_sem.at[3 * part + color if part < 4 else 8 + part]

    def attn_copy(color, part):
        turn_idx, half, sub = PARTS[part]
        idx = region(turn_fixed(color, turn_idx, sub), ALL if half is None else HALF[half], pl.ds(*COLS[color]))
        return remote(grad_attn.at[idx], peer.at[idx], push_sem, pull_of(color, part), partner)

    def expert_copies(color, part):
        turn_idx, half, sub = PARTS[part]
        fixed = turn_fixed(color, turn_idx, sub)
        copies = []
        for source, col, width, rows, packed in PIECES[color]:
            from_rows = ALL
            if half is not None and source == 'up':
                from_rows = rows = HALF[half]
            elif half is not None and rows is not HALF[half]:
                continue
            src = place(grad_up if source == 'up' else grad_down, fixed, from_rows, pl.ds(col, width))
            copies.append(remote(src, place(peer, fixed, rows, pl.ds(packed, width)), push_sem, pull_of(color, part), partner))
        return copies

    def mom_from_attn():
        return [remote(mom_up, swap_up, ex_send, ex_recv, partner), remote(mom_down, swap_down, ex_send, ex_recv, partner)]

    def mom_from_expert():
        return [remote(mom_attn, swap_attn, ex_send, ex_recv, partner)]

    def keep_copies(role):
        pairs = ((mom_attn, keep_attn),) if role == ATTN else ((mom_up, keep_up), (mom_down, keep_down))
        return [pltpu.make_async_copy(src, dst, keep_sem) for src, dst in pairs]

    barrier = pltpu.get_barrier_semaphore()
    for device in [partner] + right_dev + left_dev:
        pl.semaphore_signal(barrier, inc=1, device_id={'data': device}, device_id_type=pl.DeviceIdType.MESH)

    @pl.when(core == ATTN)
    def _():
        pltpu.make_async_copy(grad_attn, own, load_sem).start()
        for copy in keep_copies(ATTN):
            copy.start()

    with jax.named_scope('barrier'):
        pl.semaphore_wait(barrier, 7)

    @pl.when(core == ATTN)
    def _():
        for copy in mom_from_attn():
            copy.start()
        for part in range(len(PARTS)):
            for color in range(3):
                for copy in expert_copies(color, part):
                    copy.start()

    @pl.when(core == EXPERT)
    def _():
        for part in range(len(PARTS)):
            for color in range(3):
                attn_copy(color, part).start()
        for copy in mom_from_expert():
            copy.start()
        for copy in keep_copies(EXPERT):
            copy.start()
        for src, rows, cols in ((grad_up, ALL, WEST), (grad_down.at[:, :, :, :, WEST], LO, EAST), (grad_down.at[:, :, :, :, EAST], HI, EAST)):
            pltpu.make_async_copy(src, place(own, {}, rows, cols), load_sem).start()
        with jax.named_scope('gate'):
            pl.semaphore_wait(gate, 1)

    def open_gate():
        @pl.when(core == ATTN)
        def _():
            pl.semaphore_signal(gate, inc=1, device_id={'data': partner}, device_id_type=pl.DeviceIdType.MESH)

    def chip_sum(color, part):
        turn_idx, half, sub = PARTS[part]
        idx = region(turn_fixed(color, turn_idx, sub), ALL if half is None else HALF[half], pl.ds(*COLS[color]))
        if part < 4:
            arrived(peer.at[idx], pull_of(color, part))
        elif color == 0:
            arrived(peer.at[0], pull_of(color, part))
        own[idx] = own[idx] + peer[idx]

    PAIRED = ((far, 0, right_dev), (far, 1, left_dev), (right, 1, right_dev), (left, 0, left_dev), (right, 0, right_dev), (left, 1, left_dev))
    DIRECT = ((far, far_dev), (right, right_dev), (left, left_dev))

    def ctx(phase, color):
        order = ORDER[color]
        return order[phase], {order[k]: pos[order[k]] for k in range(phase)}, pl.ds(*COLS[color])

    def rs_slot(phase, color, piece, sub=None):
        free = [ALL] * (2 - phase)
        if sub is not None:
            free[0] = pl.ds(2 * sub, 2)
        return (piece, *free, ALL, pl.ds(*COLS[color]))

    def recv_sem(sems, phase, color, piece, sub):
        if phase == 2:
            return sems.at[color]
        if phase == 1:
            return sems.at[3 + 3 * color + min(piece, 2)]
        return sems.at[12 + 5 * color + (4 if piece > 1 else 2 * piece + sub)]

    def rs_region(phase, color, coord, rows, sub):
        axis, fixed, cols = ctx(phase, color)
        fixed = {**fixed, axis: coord[axis]}
        if sub is not None:
            fixed[min(k for k in range(3) if k != axis)] = pl.ds(2 * sub, 2)
        return region(fixed, rows, cols)

    def rs_copy(phase, color, piece, sub=None):
        if phase < 2:
            coord, half, device = PAIRED[piece]
            rows = HALF[half]
        else:
            coord, device = DIRECT[piece]
            rows = ALL
        return remote(own.at[rs_region(phase, color, coord, rows, sub)], recvs[phase].at[rs_slot(phase, color, piece, sub)],
                      rs_send.at[phase], recv_sem(rs_recv, phase, color, piece, sub), device[ORDER[color][phase]])

    def rs_arrive(phase, color, pieces, sub=None):
        first = pieces[0]
        slot = rs_slot(phase, color, pl.ds(first, len(pieces)), sub)
        arrived(recvs[phase].at[slot], recv_sem(rs_recv, phase, color, first, sub))

    def rs_add(phase, color, coord, rows, pieces, sub=None):
        idx = rs_region(phase, color, coord, rows, sub)
        total = own[idx]
        for piece in pieces:
            total = total + recvs[phase][rs_slot(phase, color, piece, sub)]
        own[idx] = total

    def rs_mid(phase, color, sub=None):
        rs_arrive(phase, color, (0,), sub)
        rs_add(phase, color, right, LO, (0,), sub)
        rs_copy(phase, color, 4, sub).start()
        rs_arrive(phase, color, (1,), sub)
        rs_add(phase, color, left, HI, (1,), sub)
        rs_copy(phase, color, 5, sub).start()

    def rs_end(phase, color):
        rs_arrive(phase, color, (2, 3, 4, 5))
        rs_add(phase, color, pos, LO, (3, 4))
        rs_add(phase, color, pos, HI, (2, 5))

    with jax.named_scope('rs0_load'):
        pltpu.make_async_copy(own, own, load_sem).wait()
        for part in range(4):
            for color in range(3):
                chip_sum(color, part)
                rs_copy(0, color, part % 2, part // 2).start()
        for part in (4, 5):
            for color in range(3):
                chip_sum(color, part)
                rs_copy(0, color, part - 2).start()
    with jax.named_scope('rs0_mid'):
        for sub in range(2):
            for color in range(3):
                rs_mid(0, color, sub)
        for color in range(3):
            chip_sum(color, 6)
    open_gate()
    with jax.named_scope('rs0_end'):
        for color in range(3):
            rs_end(0, color)
            for piece in range(4):
                rs_copy(1, color, piece).start()
    with jax.named_scope('rs1_mid'):
        for color in range(3):
            rs_mid(1, color)
    with jax.named_scope('rs1_end'):
        for color in range(3):
            rs_end(1, color)
            for piece in range(3):
                rs_copy(2, color, piece).start()
    with jax.named_scope('rs2'):
        for color in range(3):
            rs_arrive(2, color, (0, 1, 2))
            rs_add(2, color, pos, ALL, range(3))

    arrived(swap_attn, ex_recv)
    pltpu.make_async_copy(keep_attn, keep_attn, keep_sem).wait()

    @pl.when(core == ATTN)
    def _():
        mom_pk[LO] = swap_attn[...]
        mom_pk[HI] = keep_attn[...]

    @pl.when(core == EXPERT)
    def _():
        mom_pk[LO, WEST] = keep_up[...]
        mom_pk[HI, WEST] = swap_up[...]
        for first, cols in ((0, WEST), (8, EAST)):
            mom_pk[pl.ds(first, SIDE), EAST] = keep_down[:, cols]
            mom_pk[pl.ds(first + SIDE, SIDE), EAST] = swap_down[:, cols]

    mine = pos
    mom_new = MOMENTUM * mom_pk[...] + own[mine] * (1.0 / group_size)
    full[mine] = mom_new

    AG_SEND = ((pos, 0, right_dev), (pos, 1, left_dev), (pos, 1, right_dev), (pos, 0, left_dev), (left, 0, right_dev), (right, 1, left_dev))
    AG_LAND = ((left, 0), (right, 1), (left, 1), (right, 0), (far, 0), (far, 1))
    AG_DIRECT = (far, left, right)

    def ag_part(phase, color, coord, rows):
        axis, fixed, cols = ctx(phase, color)
        return place(full, {**fixed, axis: coord[axis]}, rows, cols)

    def ag_half(phase, color, coord, half, sub=None):
        if phase == 1:
            return ag_part(phase, color, coord, HALF[half])
        axis, second, _ = ORDER[color]
        span = pl.ds(2 * half, 2) if sub is None else pl.ds(2 * half + sub, 1)
        return place(x_all, {axis: coord[axis], second: span}, ALL, pl.ds(*COLS[color]))

    def ag_remote(part, phase, color, piece, device, sub=None):
        return remote(part, part, ag_send.at[phase], recv_sem(ag_recv, phase, color, piece, sub), device[ORDER[color][phase]])

    def ag_copy(phase, color, piece, sub=None):
        if phase < 2:
            coord, half, device = AG_SEND[piece]
            return ag_remote(ag_half(phase, color, coord, half, sub), phase, color, piece, device, sub)
        return ag_remote(ag_part(phase, color, pos, ALL), phase, color, piece, DIRECT[piece][1])

    def ag_arrive(phase, color, piece, sub=None):
        sem = recv_sem(ag_recv, phase, color, piece, sub)
        if phase == 2:
            arrived(ag_part(phase, color, [pl.ds(0, 3)] * 3, ALL), sem)
        elif piece < 2:
            coord, half = AG_LAND[piece]
            arrived(ag_half(phase, color, coord, half, sub), sem)
        elif phase == 1:
            arrived(ag_part(phase, color, [pl.ds(0, 2)] * 3, ALL), sem)
        else:
            arrived(place(x_all, {ORDER[color][0]: pl.ds(0, 2)}, ALL, pl.ds(*COLS[color])), sem)

    def drain_push():
        departed(peer, push_sem)
        departed(swap_attn, ex_send)

    def rs_drain(phase):
        departed(recvs[phase], rs_send.at[phase])

    def ag_drain(phase):
        departed((x_all.at[pl.ds(0, 3)], full.at[0, pl.ds(0, 3)], full.at[0, 0, pl.ds(0, 3)])[phase], ag_send.at[phase])

    def ag_mid(phase, sub=None):
        for color in range(3):
            for piece in range(2):
                ag_arrive(phase, color, piece, sub)
                ag_copy(phase, color, piece + 4, sub).start()

    def norm_copy(level, color, piece):
        axis = ORDER[color][level]
        part = norms.at[level, color, pos[axis]]
        return remote(part, part, norm_send.at[level], norm_recv.at[level], DIRECT[piece][1][axis])

    def norm_sum(level, color):
        return sum(norms[level, color, j] for j in range(SIDE))

    def norm_arrive(level):
        arrived(norms.at[level, :, pl.ds(0, 3)], norm_recv.at[level])

    def norm_send_all(level, color):
        for piece in range(3):
            norm_copy(level, color, piece).start()

    def square_tile(line, cols):
        val = full[line + (ALL, cols)].reshape(8, 8, cols.size)
        val = jnp.sum(val * val, axis=0)
        return sum(val[:, k:k + 128] for k in range(0, cols.size, 128))

    def norm_start(color):
        first_axis, second_axis, _ = ORDER[color]
        line = region({first_axis: pos[first_axis], second_axis: pos[second_axis]}, ALL, ALL)[:3]
        first, width = COLS[color]
        west = max(0, min(NARROW - first, width))
        for side, (start, size) in enumerate(((first, west), (first + west, width - west))):
            val = square_tile(line, pl.ds(start, size)) if size else jnp.zeros((8, 128), F32)
            norms[1, color, pos[second_axis], side] = val
        norm_send_all(1, color)

    def result_copies(role, which):
        if role == ATTN:
            source = (full.at[mine], out_pk)[which]
            pairs = ((source.at[HI], source.at[LO], (mo_attn, got_attn)[which]),)
        else:
            first = pl.multiple_of(lax.rem(chip, 8) * CHIP_ROWS, CHIP_ROWS)
            ups = ((full.at[mine + (LO, WEST)], full.at[mine + (HI, WEST)]), (turn.at[pl.ds(first, 8)], turn.at[pl.ds(first + 8, 8)]))[which]
            pairs = (ups + ((mo_up, got_up)[which],), (stay_down.at[which], send_down.at[which], (mo_down, got_down)[which]))
        stay = [pltpu.make_async_copy(pair[0], pair[2], stay_sem) for pair in pairs]
        away = [remote(pair[1], pair[2], back_send, back_recv, partner) for pair in pairs]
        return stay, away

    def result_start(role, which):
        stay, away = result_copies(role, which)
        for copy in away + stay:
            copy.start()

    with jax.named_scope('ag2'):
        for color in range(3):
            for piece in range(3):
                ag_copy(2, color, piece).start()
        drain_push()
        rs_drain(0)
        for color in range(3):
            ag_arrive(2, color, 0)
            norm_start(color)
            for piece in range(4):
                ag_copy(1, color, piece).start()

    with jax.named_scope('ag1_start'):
        @pl.when(core == ATTN)
        def _():
            result_start(ATTN, 0)

        @pl.when(core == EXPERT)
        def _():
            for rows, cols in ((LO, WEST), (HI, EAST)):
                down = full[mine + (rows, EAST)]
                send_down[0, :, cols] = down[SIDE:]
                stay_down[0, :, cols] = down[:SIDE]
            result_start(EXPERT, 0)
        rs_drain(1)
        ag_drain(2)
    with jax.named_scope('ag1_mid'):
        norm_arrive(1)
        for color in range(3):
            norms[0, color, pos[ORDER[color][0]]] = norm_sum(1, color)
            norm_send_all(0, color)
        ag_mid(1)
        rs_drain(2)
    with jax.named_scope('ag1_end'):
        for color in range(3):
            ag_arrive(1, color, 2)
    with jax.named_scope('norm'):
        norm_arrive(0)
        total = jnp.sum(norm_sum(0, 0) + norm_sum(0, 1) + norm_sum(0, 2), axis=(1, 2), keepdims=True)
        west, east = total[0], total[1]
        both = west + east
        west = jnp.where(core == ATTN, both, west)
        east = jnp.where(core == ATTN, both, east)
        lane = lax.broadcasted_iota(jnp.int32, (1, WIDE), 1)
        norm = jnp.sqrt(jnp.where(lane < NARROW, west, east))
        scales[...] = 1.0 / (norm + EPSILON)
    with jax.named_scope('ag0_start'):
        for color in range(3):
            axis, cols = ORDER[color][0], pl.ds(*COLS[color])
            idx = region({axis: pos[axis]}, ALL, cols)
            x_all[idx] = (full[idx] * scales[:, cols]).astype(BF16)
            for sub in range(2):
                for piece in range(2):
                    ag_copy(0, color, piece, sub).start()
            for piece in (2, 3):
                ag_copy(0, color, piece).start()
    with jax.named_scope('ag0_mid'):
        for sub in range(2):
            ag_mid(0, sub)
    with jax.named_scope('ag0_end'):
        for color in range(3):
            ag_arrive(0, color, 2)
    for level in range(2):
        departed(norms.at[level, :, pl.ds(0, 3)], norm_send.at[level])
    ag_drain(1)
    ag_drain(0)

    def weighted(a_val, q_val):
        return (COEF_B * a_val.astype(F32) + COEF_C * q_val.astype(BF16).astype(F32)).astype(BF16)

    def advance(x_val, y_val):
        return (COEF_A * x_val.astype(F32) + y_val.astype(BF16).astype(F32)).astype(BF16)

    def symmetric(out, base, size, block):
        for j in range(0, size, TILE):
            val = block(j)
            out[pl.ds(base + j, size - j), pl.ds(j, TILE)] = val
            if j + TILE < size:
                out[pl.ds(base + j, TILE), pl.ds(j + TILE, size - j - TILE)] = jnp.transpose(val[TILE:])

    def gram(base, size):
        def block(j):
            return lax.dot_general(x_mat[pl.ds(base + j, size - j), :], x_mat[pl.ds(base + j, TILE), :], (((1,), (1,)), ((), ())),
                                   preferred_element_type=F32).astype(BF16)
        symmetric(a_mat, base, size, block)

    def poly(base, size):
        def block(j):
            rows, cols = pl.ds(base + j, size - j), pl.ds(j, TILE)
            q_val = jnp.dot(a_mat[rows, pl.ds(0, size)], a_mat[pl.ds(base, size), cols], preferred_element_type=F32)
            return weighted(a_mat[rows, cols], q_val)
        symmetric(b_mat, base, size, block)

    def update(base, size):
        rows = pl.ds(base, size)
        y_val = jnp.dot(b_mat[rows, pl.ds(0, size)], x_mat[rows, :], preferred_element_type=F32)
        x_mat[rows, :] = advance(x_mat[rows, :], y_val)

    @pl.when(core == ATTN)
    def _():
        with jax.named_scope('fill'):
            x_mat[...] = x_all[...].reshape(WIDE, WIDE)

        with jax.named_scope('steps'):
            for _ in range(NS_STEPS - 1):
                gram(0, WIDE)
                poly(0, WIDE)
                update(0, WIDE)
            gram(0, WIDE)
        with jax.named_scope('last'):
            rows = aligned(chip * CHIP_ROWS, CHIP_ROWS)
            a_val = a_mat[rows, :]
            b_val = weighted(a_val, jnp.dot(a_val, a_mat[...], preferred_element_type=F32))
            out = advance(x_mat[rows, :], jnp.dot(b_val, x_mat[...], preferred_element_type=F32)).astype(F32)
            out_pk[...] = out
            result_start(ATTN, 1)

    @pl.when(core == EXPERT)
    def _():
        with jax.named_scope('fill'):
            def fill(k, carry):
                val = x_all[k // 2, pl.ds(2 * lax.rem(k, 2), 2), :, :, WEST].reshape(128, NARROW)
                x_mat[WEST, aligned(k * 128, 128)] = jnp.transpose(val)
                val = x_all[k // 2, pl.ds(2 * lax.rem(k, 2), 2), :, :, EAST].astype(F32)
                rows = aligned(NARROW + k * 64, 64)
                x_mat[rows, WEST] = val[:, :, :8].reshape(64, NARROW).astype(BF16)
                x_mat[rows, EAST] = val[:, :, 8:].reshape(64, NARROW).astype(BF16)
                return carry
            lax.fori_loop(0, 8, fill, 0)

        with jax.named_scope('steps'):
            for _ in range(NS_STEPS - 1):
                for stage in (gram, poly, update):
                    stage(0, NARROW)
                    stage(NARROW, NARROW)
            gram(0, NARROW)
            gram(NARROW, NARROW)
        with jax.named_scope('last'):
            poly(0, NARROW)
            cols = aligned(chip // 8 * 128, 128)
            out_up = advance(x_mat[WEST, cols], jnp.dot(b_mat[WEST, WEST], x_mat[WEST, cols], preferred_element_type=F32))
            turn[...] = jnp.transpose(out_up.astype(F32))
            rows = aligned(NARROW + chip // 2 * CHIP_ROWS, CHIP_ROWS)
            a_val = a_mat[rows, WEST]
            b_val = weighted(a_val, jnp.dot(a_val, a_mat[EAST, WEST], preferred_element_type=F32))
            both = advance(x_mat[rows, :], jnp.dot(b_val, x_mat[EAST, :], preferred_element_type=F32)).astype(F32)
            out_down = jnp.where(lax.rem(chip, 2) == 0, both[:8], both[8:])
            send_down[1] = out_down[SIDE:]
            stay_down[1] = out_down[:SIDE]
            result_start(EXPERT, 1)

    with jax.named_scope('swap'):
        pltpu.make_async_copy(out_pk, out_pk, stay_sem).wait()
        departed(out_pk, back_send)
        arrived(out_pk, back_recv)


def finish(*refs):
    for k in range(3):
        mom, out, mas = refs[k], refs[3 + k], refs[6 + k]
        mom_out, mas_out, low_out = refs[9 + 3 * k:12 + 3 * k]
        old = mas[...]
        new = old - LEARN_RATE * (0.2 * math.sqrt(WIDE) * out[...] + WEIGHT_DECAY * old)
        mom_out[...] = mom[...]
        mas_out[...] = new
        low_out[...] = new.astype(BF16)


def solution(mesh):
    group_size = mesh.shape['data']
    grad_spec = P(('stage', 'data'), None, None, None)
    row_spec = P('stage', 'data', None)

    def step_local(grad_attn, mom_attn, mas_attn, grad_up, mom_up, mas_up, grad_down, mom_down, mas_down):
        vmem = pl.BlockSpec(memory_space=pltpu.VMEM)
        hbm = pl.BlockSpec(memory_space=pltpu.HBM)
        any_space = pl.BlockSpec(memory_space=pl.ANY)
        shapes = ((8, WIDE), (8, NARROW), (SIDE, WIDE))
        sem = pltpu.SemaphoreType.DMA
        scratch = [
            *[pltpu.VMEM(BLOCK, F32)] * 3,
            *[pltpu.VMEM((6,) + (SIDE,) * free + (8, WIDE), F32) for free in (2, 1)],
            pltpu.VMEM((3, CHIP_ROWS, WIDE), F32),
            pltpu.VMEM((CHIP_ROWS, WIDE), F32),
            *[pltpu.VMEM(shape, F32) for shape in shapes * 2],
            *[pltpu.VMEM((2, SIDE, WIDE), F32)] * 2,
            pltpu.VMEM((CHIP_ROWS, WIDE), F32),
            *[pltpu.VMEM((WIDE, WIDE), BF16)] * 3,
            pltpu.VMEM((128, NARROW), F32),
            pltpu.VMEM(BLOCK, BF16), pltpu.VMEM((2, 3, SIDE, 2, 8, 128), F32), pltpu.VMEM((1, WIDE), F32),
            sem, sem, sem((15,)),
            sem((3,)), sem((27,)), sem((3,)), sem((27,)),
            *[sem] * 6,
            sem((2,)), sem((2,)),
            pltpu.SemaphoreType.REGULAR,
        ]
        result = pl.pallas_call(
            functools.partial(kernel, group_size),
            out_shape=[jax.ShapeDtypeStruct(shape, F32) for shape in shapes * 2],
            in_specs=[hbm] * 6,
            out_specs=[any_space] * 6,
            scratch_shapes=scratch,
            compiler_params=pltpu.CompilerParams(collective_id=0, has_side_effects=True, vmem_limit_bytes=36 * 1024 * 1024),
            name='muon',
        )(*(pltpu.with_memory_space_constraint(v, pltpu.HBM) for v in (grad_attn.reshape(BLOCK), grad_up.reshape(BLOCK[:4] + (NARROW,)), grad_down.reshape(BLOCK[:3] + (8, WIDE)))),
          *(pltpu.with_memory_space_constraint(v[0], pltpu.HBM) for v in (mom_attn, mom_up, mom_down)))
        outs = [jax.ShapeDtypeStruct(shape, dtype) for shape in shapes for dtype in (F32, F32, BF16)]
        done = pl.pallas_call(finish, out_shape=outs, in_specs=[vmem] * 9, out_specs=[vmem] * 9, name='finish',
                              compiler_params=pltpu.CompilerParams(vmem_limit_bytes=4 * 1024 * 1024))(
            *result, mas_attn[0], mas_up[0], mas_down[0])
        return tuple(d[None] for d in done)

    return jax.shard_map(step_local, mesh=mesh, in_specs=(grad_spec, row_spec, row_spec) * 3, out_specs=(row_spec,) * 9,
                         check_vma=False)
```

```python
import functools
import math

import jax
import jax.numpy as jnp
from jax import lax
from jax.experimental import pallas as pl
from jax.experimental.pallas import tpu as pltpu
from jax.sharding import PartitionSpec as P

MOMENTUM = 0.95
LEARN_RATE = 0.25
WEIGHT_DECAY = 0.2
EPSILON = 1e-7
COEF_A = 3.4445
COEF_B = -4.7750
COEF_C = 2.0315
NS_STEPS = 5

F32 = jnp.float32
BF16 = jnp.bfloat16

COLS = ((0, 384), (384, 384), (768, 256))
ORDER = ((0, 1, 2), (1, 2, 0), (2, 0, 1))
ATTN = 1
EXPERT = 0
SIDE = 4
CHIP_ROWS = 16
WIDE = 1024
NARROW = 512
TILE = 256
BLOCK = (SIDE, SIDE, SIDE, CHIP_ROWS, WIDE)
ALL = slice(None)
LO = pl.ds(0, 8)
HI = pl.ds(8, 8)
HALF = (LO, HI)
WEST = pl.ds(0, NARROW)
EAST = pl.ds(NARROW, NARROW)
PIECES = (
    (('up', 0, 384, ALL, 0),),
    (('up', 384, 128, ALL, 384), ('down', 0, TILE, LO, NARROW), ('down', NARROW, TILE, HI, NARROW)),
    (('down', TILE, TILE, LO, 768), ('down', 768, TILE, HI, 768)),
)


def place(ref, fixed, rows, cols):
    return ref.at[region(fixed, rows, cols)]


def region(fixed, rows, cols):
    return tuple(fixed.get(axis, ALL) for axis in range(3)) + (rows, cols)


def coords_of(k):
    return k // (SIDE * SIDE), lax.rem(k // SIDE, SIDE), lax.rem(k, SIDE)


def aligned(start, size):
    return pl.ds(pl.multiple_of(start, size), size)


def kernel(group_size, grad_attn, grad_up, grad_down, mom_attn, mom_up, mom_down,
           mo_attn, mo_up, mo_down, got_attn, got_up, got_down,
           own, peer, full, recv0, recv1, recv2, mom_pk, swap_attn, swap_up, swap_down, keep_attn, keep_up, keep_down,
           send_down, stay_down, out_pk, x_mat, a_mat, b_mat, turn, x_all, norms, scales,
           load_sem, push_sem, pull_sem, rs_send, rs_recv, ag_send, ag_recv, ex_send, ex_recv, back_send, back_recv, stay_sem, keep_sem, norm_send, norm_recv, gate):
    me = lax.axis_index('data')
    core = lax.rem(me, 2)
    chip = me // 2
    pos = coords_of(chip)
    partner = me + 1 - 2 * core
    recvs = (recv0, recv1, recv2)

    def at_axis(axis, coord):
        coords = list(pos)
        coords[axis] = coord
        return ((coords[0] * SIDE + coords[1]) * SIDE + coords[2]) * 2 + core

    right = [lax.rem(p + 1, SIDE) for p in pos]
    left = [lax.rem(p + 3, SIDE) for p in pos]
    far = [lax.rem(p + 2, SIDE) for p in pos]
    right_dev = [at_axis(a, right[a]) for a in range(3)]
    left_dev = [at_axis(a, left[a]) for a in range(3)]
    far_dev = [at_axis(a, far[a]) for a in range(3)]

    def remote(src, dst, send_sem, recv_sem, device):
        return pltpu.make_async_remote_copy(src_ref=src, dst_ref=dst, send_sem=send_sem, recv_sem=recv_sem,
                                            device_id={'data': device}, device_id_type=pl.DeviceIdType.MESH)

    def arrived(part, sem):
        remote(part, part, sem, sem, partner).wait_recv()

    def departed(part, sem):
        remote(part, part, sem, sem, partner).wait_send()

    def turns(color):
        axis = ORDER[color][0]
        return axis, (far[axis], right[axis], left[axis], pos[axis])

    PARTS = ((0, 0, 0), (0, 1, 0), (0, 0, 1), (0, 1, 1), (1, None, None), (2, None, None), (3, None, None))

    def turn_fixed(color, turn_idx, sub):
        axis, coords = turns(color)
        fixed = {axis: coords[turn_idx]}
        if sub is not None:
            fixed[min(k for k in range(3) if k != axis)] = pl.ds(2 * sub, 2)
        return fixed

    def pull_of(color, part):
        return pull_sem.at[3 * part + color if part < 4 else 8 + part]

    def attn_copy(color, part):
        turn_idx, half, sub = PARTS[part]
        idx = region(turn_fixed(color, turn_idx, sub), ALL if half is None else HALF[half], pl.ds(*COLS[color]))
        return remote(grad_attn.at[idx], peer.at[idx], push_sem, pull_of(color, part), partner)

    def expert_copies(color, part):
        turn_idx, half, sub = PARTS[part]
        fixed = turn_fixed(color, turn_idx, sub)
        copies = []
        for source, col, width, rows, packed in PIECES[color]:
            from_rows = ALL
            if half is not None and source == 'up':
                from_rows = rows = HALF[half]
            elif half is not None and rows is not HALF[half]:
                continue
            src = place(grad_up if source == 'up' else grad_down, fixed, from_rows, pl.ds(col, width))
            copies.append(remote(src, place(peer, fixed, rows, pl.ds(packed, width)), push_sem, pull_of(color, part), partner))
        return copies

    def mom_from_attn():
        return [remote(mom_up, swap_up, ex_send, ex_recv, partner), remote(mom_down, swap_down, ex_send, ex_recv, partner)]

    def mom_from_expert():
        return [remote(mom_attn, swap_attn, ex_send, ex_recv, partner)]

    def keep_copies(role):
        pairs = ((mom_attn, keep_attn),) if role == ATTN else ((mom_up, keep_up), (mom_down, keep_down))
        return [pltpu.make_async_copy(src, dst, keep_sem) for src, dst in pairs]

    barrier = pltpu.get_barrier_semaphore()
    for device in [partner] + right_dev + left_dev:
        pl.semaphore_signal(barrier, inc=1, device_id={'data': device}, device_id_type=pl.DeviceIdType.MESH)

    @pl.when(core == ATTN)
    def _():
        pltpu.make_async_copy(grad_attn, own, load_sem).start()
        for copy in keep_copies(ATTN):
            copy.start()

    with jax.named_scope('barrier'):
        pl.semaphore_wait(barrier, 7)

    @pl.when(core == ATTN)
    def _():
        for copy in mom_from_attn():
            copy.start()
        for part in range(len(PARTS)):
            for color in range(3):
                for copy in expert_copies(color, part):
                    copy.start()

    @pl.when(core == EXPERT)
    def _():
        for part in range(len(PARTS)):
            for color in range(3):
                attn_copy(color, part).start()
        for copy in mom_from_expert():
            copy.start()
        for copy in keep_copies(EXPERT):
            copy.start()
        for src, rows, cols in ((grad_up, ALL, WEST), (grad_down.at[:, :, :, :, WEST], LO, EAST), (grad_down.at[:, :, :, :, EAST], HI, EAST)):
            pltpu.make_async_copy(src, place(own, {}, rows, cols), load_sem).start()

    def open_gate():
        @pl.when(core == ATTN)
        def _():
            pl.semaphore_signal(gate, inc=1, device_id={'data': partner}, device_id_type=pl.DeviceIdType.MESH)

    def chip_sum(color, part):
        turn_idx, half, sub = PARTS[part]
        idx = region(turn_fixed(color, turn_idx, sub), ALL if half is None else HALF[half], pl.ds(*COLS[color]))
        if part < 4:
            arrived(peer.at[idx], pull_of(color, part))
        elif color == 0:
            arrived(peer.at[0], pull_of(color, part))
        own[idx] = own[idx] + peer[idx]

    PAIRED = ((far, 0, right_dev), (far, 1, left_dev), (right, 1, right_dev), (left, 0, left_dev), (right, 0, right_dev), (left, 1, left_dev))
    DIRECT = ((far, far_dev), (right, right_dev), (left, left_dev))

    def ctx(phase, color):
        order = ORDER[color]
        return order[phase], {order[k]: pos[order[k]] for k in range(phase)}, pl.ds(*COLS[color])

    def rs_slot(phase, color, piece, sub=None):
        free = [ALL] * (2 - phase)
        if sub is not None:
            free[0] = pl.ds(2 * sub, 2)
        return (piece, *free, ALL, pl.ds(*COLS[color]))

    def recv_sem(sems, phase, color, piece, sub):
        if phase == 2:
            return sems.at[color]
        if phase == 1:
            return sems.at[3 + 3 * color + min(piece, 2)]
        return sems.at[12 + 5 * color + (4 if piece > 1 else 2 * piece + sub)]

    def rs_region(phase, color, coord, rows, sub):
        axis, fixed, cols = ctx(phase, color)
        fixed = {**fixed, axis: coord[axis]}
        if sub is not None:
            fixed[min(k for k in range(3) if k != axis)] = pl.ds(2 * sub, 2)
        return region(fixed, rows, cols)

    def rs_copy(phase, color, piece, sub=None):
        if phase < 2:
            coord, half, device = PAIRED[piece]
            rows = HALF[half]
        else:
            coord, device = DIRECT[piece]
            rows = ALL
        return remote(own.at[rs_region(phase, color, coord, rows, sub)], recvs[phase].at[rs_slot(phase, color, piece, sub)],
                      rs_send.at[phase], recv_sem(rs_recv, phase, color, piece, sub), device[ORDER[color][phase]])

    def rs_arrive(phase, color, pieces, sub=None):
        first = pieces[0]
        slot = rs_slot(phase, color, pl.ds(first, len(pieces)), sub)
        arrived(recvs[phase].at[slot], recv_sem(rs_recv, phase, color, first, sub))

    def rs_add(phase, color, coord, rows, pieces, sub=None):
        idx = rs_region(phase, color, coord, rows, sub)
        total = own[idx]
        for piece in pieces:
            total = total + recvs[phase][rs_slot(phase, color, piece, sub)]
        own[idx] = total

    def rs_mid(phase, color, sub=None):
        rs_arrive(phase, color, (0,), sub)
        rs_add(phase, color, right, LO, (0,), sub)
        rs_copy(phase, color, 4, sub).start()
        rs_arrive(phase, color, (1,), sub)
        rs_add(phase, color, left, HI, (1,), sub)
        rs_copy(phase, color, 5, sub).start()

    def rs_end(phase, color):
        rs_arrive(phase, color, (2, 3, 4, 5))
        rs_add(phase, color, pos, LO, (3, 4))
        rs_add(phase, color, pos, HI, (2, 5))

    def attn_sum(color, part):
        @pl.when(core == ATTN)
        def _():
            chip_sum(color, part)

    with jax.named_scope('rs0_load'):
        pltpu.make_async_copy(own, own, load_sem).wait()

        @pl.when(core == EXPERT)
        def _():
            with jax.named_scope('gate'):
                pl.semaphore_wait(gate, 1)
            for part in range(len(PARTS)):
                for color in range(3):
                    chip_sum(color, part)

        for part in range(4):
            for color in range(3):
                attn_sum(color, part)
                rs_copy(0, color, part % 2, part // 2).start()
        for part in (4, 5):
            for color in range(3):
                attn_sum(color, part)
                rs_copy(0, color, part - 2).start()
    with jax.named_scope('rs0_mid'):
        for sub in range(2):
            for color in range(3):
                rs_mid(0, color, sub)
        for color in range(3):
            attn_sum(color, 6)
    open_gate()
    with jax.named_scope('rs0_end'):
        for color in range(3):
            rs_end(0, color)
            for piece in range(4):
                rs_copy(1, color, piece).start()
    with jax.named_scope('rs1_mid'):
        for color in range(3):
            rs_mid(1, color)
    with jax.named_scope('rs1_end'):
        for color in range(3):
            rs_end(1, color)
            for piece in range(3):
                rs_copy(2, color, piece).start()
    with jax.named_scope('rs2'):
        for color in range(3):
            rs_arrive(2, color, (0, 1, 2))
            rs_add(2, color, pos, ALL, range(3))

    arrived(swap_attn, ex_recv)
    pltpu.make_async_copy(keep_attn, keep_attn, keep_sem).wait()

    @pl.when(core == ATTN)
    def _():
        mom_pk[LO] = swap_attn[...]
        mom_pk[HI] = keep_attn[...]

    @pl.when(core == EXPERT)
    def _():
        mom_pk[LO, WEST] = keep_up[...]
        mom_pk[HI, WEST] = swap_up[...]
        for first, cols in ((0, WEST), (8, EAST)):
            mom_pk[pl.ds(first, SIDE), EAST] = keep_down[:, cols]
            mom_pk[pl.ds(first + SIDE, SIDE), EAST] = swap_down[:, cols]

    mine = pos
    mom_new = MOMENTUM * mom_pk[...] + own[mine] * (1.0 / group_size)
    full[mine] = mom_new

    AG_SEND = ((pos, 0, right_dev), (pos, 1, left_dev), (pos, 1, right_dev), (pos, 0, left_dev), (left, 0, right_dev), (right, 1, left_dev))
    AG_LAND = ((left, 0), (right, 1), (left, 1), (right, 0), (far, 0), (far, 1))
    AG_DIRECT = (far, left, right)

    def ag_part(phase, color, coord, rows):
        axis, fixed, cols = ctx(phase, color)
        return place(full, {**fixed, axis: coord[axis]}, rows, cols)

    def ag_half(phase, color, coord, half, sub=None):
        if phase == 1:
            return ag_part(phase, color, coord, HALF[half])
        axis, second, _ = ORDER[color]
        span = pl.ds(2 * half, 2) if sub is None else pl.ds(2 * half + sub, 1)
        return place(x_all, {axis: coord[axis], second: span}, ALL, pl.ds(*COLS[color]))

    def ag_remote(part, phase, color, piece, device, sub=None):
        return remote(part, part, ag_send.at[phase], recv_sem(ag_recv, phase, color, piece, sub), device[ORDER[color][phase]])

    def ag_copy(phase, color, piece, sub=None):
        if phase < 2:
            coord, half, device = AG_SEND[piece]
            return ag_remote(ag_half(phase, color, coord, half, sub), phase, color, piece, device, sub)
        return ag_remote(ag_part(phase, color, pos, ALL), phase, color, piece, DIRECT[piece][1])

    def ag_arrive(phase, color, piece, sub=None):
        sem = recv_sem(ag_recv, phase, color, piece, sub)
        if phase == 2:
            arrived(ag_part(phase, color, [pl.ds(0, 3)] * 3, ALL), sem)
        elif piece < 2:
            coord, half = AG_LAND[piece]
            arrived(ag_half(phase, color, coord, half, sub), sem)
        elif phase == 1:
            arrived(ag_part(phase, color, [pl.ds(0, 2)] * 3, ALL), sem)
        else:
            arrived(place(x_all, {ORDER[color][0]: pl.ds(0, 2)}, ALL, pl.ds(*COLS[color])), sem)

    def drain_push():
        departed(peer, push_sem)
        departed(swap_attn, ex_send)

    def rs_drain(phase):
        departed(recvs[phase], rs_send.at[phase])

    def ag_drain(phase):
        departed((x_all.at[pl.ds(0, 3)], full.at[0, pl.ds(0, 3)], full.at[0, 0, pl.ds(0, 3)])[phase], ag_send.at[phase])

    def ag_mid(phase, sub=None):
        for color in range(3):
            for piece in range(2):
                ag_arrive(phase, color, piece, sub)
                ag_copy(phase, color, piece + 4, sub).start()

    def norm_copy(level, color, piece):
        axis = ORDER[color][level]
        part = norms.at[level, color, pos[axis]]
        return remote(part, part, norm_send.at[level], norm_recv.at[level], DIRECT[piece][1][axis])

    def norm_sum(level, color):
        return sum(norms[level, color, j] for j in range(SIDE))

    def norm_arrive(level):
        arrived(norms.at[level, :, pl.ds(0, 3)], norm_recv.at[level])

    def norm_send_all(level, color):
        for piece in range(3):
            norm_copy(level, color, piece).start()

    def square_tile(line, cols):
        val = full[line + (ALL, cols)].reshape(8, 8, cols.size)
        val = jnp.sum(val * val, axis=0)
        return sum(val[:, k:k + 128] for k in range(0, cols.size, 128))

    def norm_start(color):
        first_axis, second_axis, _ = ORDER[color]
        line = region({first_axis: pos[first_axis], second_axis: pos[second_axis]}, ALL, ALL)[:3]
        first, width = COLS[color]
        west = max(0, min(NARROW - first, width))
        for side, (start, size) in enumerate(((first, west), (first + west, width - west))):
            val = square_tile(line, pl.ds(start, size)) if size else jnp.zeros((8, 128), F32)
            norms[1, color, pos[second_axis], side] = val
        norm_send_all(1, color)

    def result_copies(role, which):
        if role == ATTN:
            source = (full.at[mine], out_pk)[which]
            pairs = ((source.at[HI], source.at[LO], (mo_attn, got_attn)[which]),)
        else:
            first = pl.multiple_of(lax.rem(chip, 8) * CHIP_ROWS, CHIP_ROWS)
            ups = ((full.at[mine + (LO, WEST)], full.at[mine + (HI, WEST)]), (turn.at[pl.ds(first, 8)], turn.at[pl.ds(first + 8, 8)]))[which]
            pairs = (ups + ((mo_up, got_up)[which],), (stay_down.at[which], send_down.at[which], (mo_down, got_down)[which]))
        stay = [pltpu.make_async_copy(pair[0], pair[2], stay_sem) for pair in pairs]
        away = [remote(pair[1], pair[2], back_send, back_recv, partner) for pair in pairs]
        return stay, away

    def result_start(role, which):
        stay, away = result_copies(role, which)
        for copy in away + stay:
            copy.start()

    with jax.named_scope('ag2'):
        for color in range(3):
            for piece in range(3):
                ag_copy(2, color, piece).start()
        drain_push()
        rs_drain(0)
        for color in range(3):
            ag_arrive(2, color, 0)
            norm_start(color)
            for piece in range(4):
                ag_copy(1, color, piece).start()

    with jax.named_scope('ag1_start'):
        @pl.when(core == ATTN)
        def _():
            result_start(ATTN, 0)

        @pl.when(core == EXPERT)
        def _():
            for rows, cols in ((LO, WEST), (HI, EAST)):
                down = full[mine + (rows, EAST)]
                send_down[0, :, cols] = down[SIDE:]
                stay_down[0, :, cols] = down[:SIDE]
            result_start(EXPERT, 0)
        rs_drain(1)
        ag_drain(2)
    with jax.named_scope('ag1_mid'):
        norm_arrive(1)
        for color in range(3):
            norms[0, color, pos[ORDER[color][0]]] = norm_sum(1, color)
            norm_send_all(0, color)
        ag_mid(1)
        rs_drain(2)
    with jax.named_scope('ag1_end'):
        for color in range(3):
            ag_arrive(1, color, 2)
    with jax.named_scope('norm'):
        norm_arrive(0)
        total = jnp.sum(norm_sum(0, 0) + norm_sum(0, 1) + norm_sum(0, 2), axis=(1, 2), keepdims=True)
        west, east = total[0], total[1]
        both = west + east
        west = jnp.where(core == ATTN, both, west)
        east = jnp.where(core == ATTN, both, east)
        lane = lax.broadcasted_iota(jnp.int32, (1, WIDE), 1)
        norm = jnp.sqrt(jnp.where(lane < NARROW, west, east))
        scales[...] = 1.0 / (norm + EPSILON)
    with jax.named_scope('ag0_start'):
        for color in range(3):
            axis, cols = ORDER[color][0], pl.ds(*COLS[color])
            idx = region({axis: pos[axis]}, ALL, cols)
            x_all[idx] = (full[idx] * scales[:, cols]).astype(BF16)
            for sub in range(2):
                for piece in range(2):
                    ag_copy(0, color, piece, sub).start()
            for piece in (2, 3):
                ag_copy(0, color, piece).start()
    with jax.named_scope('ag0_mid'):
        for sub in range(2):
            ag_mid(0, sub)
    with jax.named_scope('ag0_end'):
        for color in range(3):
            ag_arrive(0, color, 2)
    for level in range(2):
        departed(norms.at[level, :, pl.ds(0, 3)], norm_send.at[level])
    ag_drain(1)
    ag_drain(0)

    def weighted(a_val, q_val):
        return (COEF_B * a_val.astype(F32) + COEF_C * q_val.astype(BF16).astype(F32)).astype(BF16)

    def advance(x_val, y_val):
        return (COEF_A * x_val.astype(F32) + y_val.astype(BF16).astype(F32)).astype(BF16)

    def symmetric(out, base, size, block):
        for j in range(0, size, TILE):
            val = block(j)
            out[pl.ds(base + j, size - j), pl.ds(j, TILE)] = val
            if j + TILE < size:
                out[pl.ds(base + j, TILE), pl.ds(j + TILE, size - j - TILE)] = jnp.transpose(val[TILE:])

    def gram(base, size):
        def block(j):
            return lax.dot_general(x_mat[pl.ds(base + j, size - j), :], x_mat[pl.ds(base + j, TILE), :], (((1,), (1,)), ((), ())),
                                   preferred_element_type=F32).astype(BF16)
        symmetric(a_mat, base, size, block)

    def poly(base, size):
        def block(j):
            rows, cols = pl.ds(base + j, size - j), pl.ds(j, TILE)
            q_val = jnp.dot(a_mat[rows, pl.ds(0, size)], a_mat[pl.ds(base, size), cols], preferred_element_type=F32)
            return weighted(a_mat[rows, cols], q_val)
        symmetric(b_mat, base, size, block)

    def update(base, size):
        rows = pl.ds(base, size)
        y_val = jnp.dot(b_mat[rows, pl.ds(0, size)], x_mat[rows, :], preferred_element_type=F32)
        x_mat[rows, :] = advance(x_mat[rows, :], y_val)

    @pl.when(core == ATTN)
    def _():
        with jax.named_scope('fill'):
            x_mat[...] = x_all[...].reshape(WIDE, WIDE)

        with jax.named_scope('steps'):
            for _ in range(NS_STEPS - 1):
                gram(0, WIDE)
                poly(0, WIDE)
                update(0, WIDE)
            gram(0, WIDE)
        with jax.named_scope('last'):
            rows = aligned(chip * CHIP_ROWS, CHIP_ROWS)
            a_val = a_mat[rows, :]
            b_val = weighted(a_val, jnp.dot(a_val, a_mat[...], preferred_element_type=F32))
            out = advance(x_mat[rows, :], jnp.dot(b_val, x_mat[...], preferred_element_type=F32)).astype(F32)
            out_pk[...] = out
            result_start(ATTN, 1)

    @pl.when(core == EXPERT)
    def _():
        with jax.named_scope('fill'):
            def fill(k, carry):
                val = x_all[k // 2, pl.ds(2 * lax.rem(k, 2), 2), :, :, WEST].reshape(128, NARROW)
                x_mat[WEST, aligned(k * 128, 128)] = jnp.transpose(val)
                val = x_all[k // 2, pl.ds(2 * lax.rem(k, 2), 2), :, :, EAST].astype(F32)
                rows = aligned(NARROW + k * 64, 64)
                x_mat[rows, WEST] = val[:, :, :8].reshape(64, NARROW).astype(BF16)
                x_mat[rows, EAST] = val[:, :, 8:].reshape(64, NARROW).astype(BF16)
                return carry
            lax.fori_loop(0, 8, fill, 0, unroll=True)

        with jax.named_scope('steps'):
            for _ in range(NS_STEPS - 1):
                for stage in (gram, poly, update):
                    stage(0, NARROW)
                    stage(NARROW, NARROW)
            gram(0, NARROW)
            gram(NARROW, NARROW)
        with jax.named_scope('last'):
            poly(0, NARROW)
            cols = aligned(chip // 8 * 128, 128)
            out_up = advance(x_mat[WEST, cols], jnp.dot(b_mat[WEST, WEST], x_mat[WEST, cols], preferred_element_type=F32))
            turn[...] = jnp.transpose(out_up.astype(F32))
            rows = aligned(NARROW + chip // 2 * CHIP_ROWS, CHIP_ROWS)
            a_val = a_mat[rows, WEST]
            b_val = weighted(a_val, jnp.dot(a_val, a_mat[EAST, WEST], preferred_element_type=F32))
            both = advance(x_mat[rows, :], jnp.dot(b_val, x_mat[EAST, :], preferred_element_type=F32)).astype(F32)
            out_down = jnp.where(lax.rem(chip, 2) == 0, both[:8], both[8:])
            send_down[1] = out_down[SIDE:]
            stay_down[1] = out_down[:SIDE]
            result_start(EXPERT, 1)

    with jax.named_scope('swap'):
        pltpu.make_async_copy(out_pk, out_pk, stay_sem).wait()
        departed(out_pk, back_send)
        arrived(out_pk, back_recv)


def finish(*refs):
    for k in range(3):
        mom, out, mas = refs[k], refs[3 + k], refs[6 + k]
        mom_out, mas_out, low_out = refs[9 + 3 * k:12 + 3 * k]
        old = mas[...]
        new = old - LEARN_RATE * (0.2 * math.sqrt(WIDE) * out[...] + WEIGHT_DECAY * old)
        mom_out[...] = mom[...]
        mas_out[...] = new
        low_out[...] = new.astype(BF16)


def solution(mesh):
    group_size = mesh.shape['data']
    grad_spec = P(('stage', 'data'), None, None, None)
    row_spec = P('stage', 'data', None)

    def step_local(grad_attn, mom_attn, mas_attn, grad_up, mom_up, mas_up, grad_down, mom_down, mas_down):
        vmem = pl.BlockSpec(memory_space=pltpu.VMEM)
        hbm = pl.BlockSpec(memory_space=pltpu.HBM)
        any_space = pl.BlockSpec(memory_space=pl.ANY)
        shapes = ((8, WIDE), (8, NARROW), (SIDE, WIDE))
        sem = pltpu.SemaphoreType.DMA
        scratch = [
            *[pltpu.VMEM(BLOCK, F32)] * 3,
            *[pltpu.VMEM((6,) + (SIDE,) * free + (8, WIDE), F32) for free in (2, 1)],
            pltpu.VMEM((3, CHIP_ROWS, WIDE), F32),
            pltpu.VMEM((CHIP_ROWS, WIDE), F32),
            *[pltpu.VMEM(shape, F32) for shape in shapes * 2],
            *[pltpu.VMEM((2, SIDE, WIDE), F32)] * 2,
            pltpu.VMEM((CHIP_ROWS, WIDE), F32),
            *[pltpu.VMEM((WIDE, WIDE), BF16)] * 3,
            pltpu.VMEM((128, NARROW), F32),
            pltpu.VMEM(BLOCK, BF16), pltpu.VMEM((2, 3, SIDE, 2, 8, 128), F32), pltpu.VMEM((1, WIDE), F32),
            sem, sem, sem((15,)),
            sem((3,)), sem((27,)), sem((3,)), sem((27,)),
            *[sem] * 6,
            sem((2,)), sem((2,)),
            pltpu.SemaphoreType.REGULAR,
        ]
        result = pl.pallas_call(
            functools.partial(kernel, group_size),
            out_shape=[jax.ShapeDtypeStruct(shape, F32) for shape in shapes * 2],
            in_specs=[hbm] * 6,
            out_specs=[any_space] * 6,
            scratch_shapes=scratch,
            compiler_params=pltpu.CompilerParams(collective_id=0, has_side_effects=True, vmem_limit_bytes=36 * 1024 * 1024),
            name='muon',
        )(*(pltpu.with_memory_space_constraint(v, pltpu.HBM) for v in (grad_attn.reshape(BLOCK), grad_up.reshape(BLOCK[:4] + (NARROW,)), grad_down.reshape(BLOCK[:3] + (8, WIDE)))),
          *(pltpu.with_memory_space_constraint(v[0], pltpu.HBM) for v in (mom_attn, mom_up, mom_down)))
        outs = [jax.ShapeDtypeStruct(shape, dtype) for shape in shapes for dtype in (F32, F32, BF16)]
        done = pl.pallas_call(finish, out_shape=outs, in_specs=[vmem] * 9, out_specs=[vmem] * 9, name='finish',
                              compiler_params=pltpu.CompilerParams(vmem_limit_bytes=4 * 1024 * 1024))(
            *result, mas_attn[0], mas_up[0], mas_down[0])
        return tuple(d[None] for d in done)

    return jax.shard_map(step_local, mesh=mesh, in_specs=(grad_spec, row_spec, row_spec) * 3, out_specs=(row_spec,) * 9,
                         check_vma=False)
```
